32 devices in a mesh: data: 1 (over z), model: 4 (over y), stage: 8 (over x, core).
Axes of the slice: x: 4, y: 4, z: 1, core: 2. Of those that a mesh axis runs over, the one named last changes fastest.
The devices are a block of a 4x4x8 slice.
Arguments:
- x_in: bfloat16 [1, 1024, 1536], P('data')
- y_target: bfloat16 [1, 1024, 1536], P('data')
- w_qkv: bfloat16 [8, 1536, 3, 12, 128], P('stage', None, None, 'model')
- w_out: bfloat16 [8, 12, 128, 1536], P('stage', 'model')
- w_up: bfloat16 [8, 1536, 6144], P('stage', None, 'model')
- w_down: bfloat16 [8, 6144, 1536], P('stage', 'model')
- norm_gain: bfloat16 [8, 2, 1536], P('stage')
Outputs:
- output 1: float32 [1], P('data')
- output 2: float32 [8, 1536, 3, 12, 128], P(('data', 'stage'), None, None, 'model')
- output 3: float32 [8, 12, 128, 1536], P(('data', 'stage'), 'model')
- output 4: float32 [8, 1536, 6144], P(('data', 'stage'), None, 'model')
- output 5: float32 [8, 6144, 1536], P(('data', 'stage'), 'model')
- output 6: float32 [8, 2, 1536], P(('data', 'stage'))
All inputs are finite; a program needn't handle non-finite values.
Results may differ from the reference program's by a relative error of at most 0.00889341.
Values are sent between devices in bfloat16 or wider.
A program may use at most 768 MiB of HBM per device.

```python
import jax
import jax.numpy as jnp
from jax import lax

BATCH = 1
SEQ = 1024
D = 1536
HEADS = 12
LAYERS = 8

HEAD = D // HEADS
FF = 4 * D
QUERY_BLOCK = min(SEQ, 256)
NORM_EPS = 1e-6
NEG_BIG = -1e30


def setup_inputs(seed: int = 0, part: int = 0) -> dict:
    part_key = jax.random.fold_in(jax.random.key(seed), part)
    key_x, key_y = jax.random.split(part_key, 2)
    key_qkv, key_out, key_up, key_down, key_gain = jax.random.split(jax.random.key(seed + 1), 5)
    x_in = jax.random.normal(key_x, (BATCH, SEQ, D), jnp.float32)
    y_target = jax.random.normal(key_y, (BATCH, SEQ, D), jnp.float32)
    w_qkv = jax.random.normal(key_qkv, (LAYERS, D, 3, HEADS, HEAD), jnp.float32) * D ** -0.5
    w_out = jax.random.normal(key_out, (LAYERS, HEADS, HEAD, D), jnp.float32) * D ** -0.5
    w_up = jax.random.normal(key_up, (LAYERS, D, FF), jnp.float32) * D ** -0.5
    w_down = jax.random.normal(key_down, (LAYERS, FF, D), jnp.float32) * FF ** -0.5
    norm_gain = 1.0 + 0.3 * jax.random.normal(key_gain, (LAYERS, 2, D), jnp.float32)
    return {
        "x_in": x_in.astype(jnp.bfloat16),
        "y_target": y_target.astype(jnp.bfloat16),
        "w_qkv": w_qkv.astype(jnp.bfloat16),
        "w_out": w_out.astype(jnp.bfloat16),
        "w_up": w_up.astype(jnp.bfloat16),
        "w_down": w_down.astype(jnp.bfloat16),
        "norm_gain": norm_gain.astype(jnp.bfloat16),
    }


def rms_scale(hid32, gain32):
    inv_rms = lax.rsqrt(jnp.mean(hid32 * hid32, axis=-1, keepdims=True) + NORM_EPS)
    return (hid32 * inv_rms * gain32).astype(jnp.bfloat16)


def attend_sequence(qkv_seq):
    q_seq = qkv_seq[:, 0].astype(jnp.float32)
    k_seq = qkv_seq[:, 1].astype(jnp.float32)
    v_seq = qkv_seq[:, 2].astype(jnp.float32)
    key_pos = jnp.arange(SEQ)

    def query_block(block_start):
        q_blk = lax.dynamic_slice_in_dim(q_seq, block_start, QUERY_BLOCK, 0)
        scores = jnp.einsum("qhe,khe->hqk", q_blk, k_seq) * HEAD ** -0.5
        q_pos = block_start + jnp.arange(QUERY_BLOCK)
        scores = jnp.where(key_pos[None, None, :] <= q_pos[None, :, None], scores, NEG_BIG)
        attn_probs = jax.nn.softmax(scores, axis=-1).astype(jnp.bfloat16)
        return jnp.einsum("hqk,khe->qhe", attn_probs.astype(jnp.float32), v_seq).astype(jnp.bfloat16)

    blocks = lax.map(jax.checkpoint(query_block), jnp.arange(SEQ // QUERY_BLOCK) * QUERY_BLOCK)
    return blocks.reshape(SEQ, HEADS, HEAD)


def layer_forward(hid, layer_w):
    w_qkv_l, w_out_l, w_up_l, w_down_l, gain_l = layer_w
    hid32 = hid.reshape(BATCH * SEQ, D).astype(jnp.float32)
    norm_a = rms_scale(hid32, gain_l[0])
    qkv_act = jnp.dot(norm_a, w_qkv_l.reshape(D, 3 * D), preferred_element_type=jnp.float32).astype(jnp.bfloat16)
    attn_act = lax.map(attend_sequence, qkv_act.reshape(BATCH, SEQ, 3, HEADS, HEAD))
    mid_hid = hid32 + jnp.dot(attn_act.reshape(BATCH * SEQ, D), w_out_l.reshape(D, D), preferred_element_type=jnp.float32)
    norm_b = rms_scale(mid_hid, gain_l[1])
    up_act = jnp.dot(norm_b, w_up_l, preferred_element_type=jnp.float32)
    gelu_act = jax.nn.gelu(up_act, approximate=True).astype(jnp.bfloat16)
    new_hid = mid_hid + jnp.dot(gelu_act, w_down_l, preferred_element_type=jnp.float32)
    return new_hid.astype(jnp.bfloat16).reshape(BATCH, SEQ, D)


def total_loss(weights, x_in, y_target):
    def layer_step(hid, layer_w):
        return jax.checkpoint(layer_forward)(hid, layer_w), None

    final_hid = lax.scan(layer_step, x_in, weights)[0]
    loss_diff = final_hid.astype(jnp.float32) - y_target.astype(jnp.float32)
    return 0.5 * jnp.mean(loss_diff * loss_diff)


def reference(x_in, y_target, w_qkv, w_out, w_up, w_down, norm_gain):
    weights = (w_qkv, w_out, w_up, w_down, norm_gain.astype(jnp.float32))
    loss_val, grads = jax.value_and_grad(total_loss)(weights, x_in, y_target)
    return (
        loss_val.reshape(1),
        grads[0].astype(jnp.float32),
        grads[1].astype(jnp.float32),
        grads[2].astype(jnp.float32),
        grads[3].astype(jnp.float32),
        grads[4].astype(jnp.float32),
    )
```

```python
import functools
import math

import jax
import jax.numpy as jnp
from jax import lax
from jax.experimental import pallas as pl
from jax.experimental.pallas import tpu as pltpu
from jax.sharding import PartitionSpec as P

NORM_EPS = 1e-6
NEG_BIG = -1e30
CHUNK = 128
F32 = jnp.float32
BF16 = jnp.bfloat16
MESH_ID = pl.DeviceIdType.MESH
GELU_A = math.sqrt(2.0 / math.pi)
GELU_B = 0.044715
VMEM_BYTES = 67043328


def dot_nn(a, b):
    return lax.dot_general(a, b, (((1,), (0,)), ((), ())), preferred_element_type=F32)


def dot_nt(a, b):
    return lax.dot_general(a, b, (((1,), (1,)), ((), ())), preferred_element_type=F32)


def dot_tn(a, b):
    return lax.dot_general(a, b, (((0,), (0,)), ((), ())), preferred_element_type=F32)


def rms_inverse(v):
    return lax.rsqrt(jnp.mean(v * v, axis=-1, keepdims=True) + NORM_EPS)


def gelu_tanh(u):
    return u * (0.5 * (1.0 + jnp.tanh(GELU_A * (u + GELU_B * (u * u * u)))))


def gelu_slope(u):
    t = jnp.tanh(GELU_A * (u + GELU_B * (u * u * u)))
    return 0.5 * (1.0 + t) + (0.5 * u) * (1.0 - t * t) * (GELU_A * (1.0 + (3.0 * GELU_B) * (u * u)))


def tile_of(width, top=512):
    for tile in (top, 384, 256, 128):
        if width % tile == 0:
            return tile
    return width


def fold_rows(v):
    total = v[0:8]
    for r in range(8, v.shape[0], 8):
        total = total + v[r : r + 8]
    return total


def step_kernel(cfg, *refs):
    n, t, tq, n_model, n_stage = cfg["n"], cfg["t"], cfg["tq"], cfg["n_model"], cfg["n_stage"]
    seq, d_model, heads, hd, ff = cfg["seq"], cfg["d_model"], cfg["heads"], cfg["hd"], cfg["ff"]
    hw = heads * hd
    elem_count = cfg["elem_count"]
    scale = hd**-0.5
    (
        x_hbm, y_hbm, wqkv_hbm, wout_hbm, wup_hbm, wdown_hbm, gain_ref,
        na_hbm, nb_hbm, at_hbm, z_hbm, dqkv_hbm, dmid_hbm, dup_hbm, dout_hbm, small_ref,
        wqkv, wout, wup, wdown, hbuf, nbbuf, doutbuf, dmidbuf, qkvbuf, upbuf, midq, yq, dkacc, dvacc,
        rs_r, rs_s, na_st, z_st, at_st, dup_st, dqkv_st, hsend, dsend, dmidq,
        lossacc, gacc, lossbuf, fin_s, fin_r,
        w_sem, x_sem, y_sem, h_rsem, h_ssem, d_rsem, d_ssem, rs_rsem, rs_ssem, ag_rsem, ag_ssem,
        out_sem, full_sem, loss_sem, fin_rsem, fin_ssem,
    ) = refs
    me = lax.axis_index("model")
    stage = lax.axis_index("stage")
    last = n_stage - 1
    order = [d for d in (2, 1, 3) if d < n_model] if n_model > 2 else list(range(1, n_model))

    def remote(src, dst, ssem, rsem, where):
        return pltpu.make_async_remote_copy(
            src_ref=src, dst_ref=dst, send_sem=ssem, recv_sem=rsem, device_id=where, device_id_type=MESH_ID
        )

    def rows_of(c):
        return pl.ds(pl.multiple_of(c * t, t), t)

    def quarter(c, m):
        return pl.ds(pl.multiple_of(c * t + m * tq, tq), tq)

    own = pl.ds(pl.multiple_of(me * tq, tq), tq)

    def weight_copy(k):
        src = (wqkv_hbm, wout_hbm, wup_hbm, wdown_hbm)[k]
        dst = (wqkv, wout, wup, wdown)[k]
        return pltpu.make_async_copy(src, dst, w_sem.at[k])

    def x_copy(c):
        return pltpu.make_async_copy(x_hbm.at[rows_of(c)], hbuf.at[rows_of(c)], x_sem.at[c])

    def y_copy(c):
        return pltpu.make_async_copy(y_hbm.at[quarter(c, me)], yq.at[c], y_sem.at[c])

    @pl.when(stage == 0)
    def _():
        x_copy(0).start()

    for k in range(4):
        weight_copy(k).start()

    @pl.when(stage == 0)
    def _():
        for c in range(1, n):
            x_copy(c).start()

    @pl.when(stage == last)
    def _():
        for c in range(n):
            y_copy(c).start()

    barrier = pltpu.get_barrier_semaphore()
    up_stage = lax.rem(stage + 1, n_stage)
    down_stage = lax.rem(stage + n_stage - 1, n_stage)
    greet = [{"model": lax.rem(me + d, n_model)} for d in range(1, n_model)]
    greet += [{"stage": up_stage, "model": m} for m in range(n_model)]
    if n_stage > 2:
        greet += [{"stage": down_stage, "model": m} for m in range(n_model)]
    for where in greet:
        pl.semaphore_signal(barrier, inc=1, device_id=where, device_id_type=MESH_ID)

    qkvbuf[...] = jnp.zeros_like(qkvbuf)
    dkacc[...] = jnp.zeros_like(dkacc)
    dvacc[...] = jnp.zeros_like(dvacc)
    lossacc[...] = jnp.zeros_like(lossacc)
    gacc[...] = jnp.zeros_like(gacc)
    pl.semaphore_wait(barrier, len(greet))

    gain_a = gain_ref[0:1, :]
    gain_b = gain_ref[1:2, :]

    def rs_copy(p, c, d, peer):
        return remote(
            rs_s.at[p, pl.ds(pl.multiple_of(peer * tq, tq), tq)], rs_r.at[p, c, d - 1],
            rs_ssem.at[p, d - 1], rs_rsem.at[p, c, d - 1], {"model": peer},
        )

    def rs_start(p, c):
        for d in order:
            rs_copy(p, c, d, lax.rem(me + d, n_model)).start()

    def rs_drain(p):
        for d in order:
            rs_copy(p, 0, d, 0).wait_send()

    def rs_sum(p, c):
        for d in order:
            rs_copy(p, c, d, 0).wait_recv()
        total = rs_s[p, own, :].astype(F32)
        for d in range(1, n_model):
            total = total + rs_r[p, c, d - 1].astype(F32)
        return total

    def ag_copy(p, buf, c, d, peer, owner):
        return remote(
            buf.at[quarter(c, owner)], buf.at[quarter(c, owner)],
            ag_ssem.at[p, d - 1], ag_rsem.at[p, c, d - 1], {"model": peer},
        )

    def ag_start(p, buf, c):
        for d in order:
            ag_copy(p, buf, c, d, lax.rem(me + d, n_model), me).start()

    def ag_drain(p, buf):
        for d in order:
            ag_copy(p, buf, 0, d, 0, 0).wait_send()

    def ag_wait(p, buf, c):
        for d in order:
            ag_copy(p, buf, c, d, 0, lax.rem(me + n_model - d, n_model)).wait_recv()

    def h_copy(c, m, sender):
        return remote(
            hsend, hbuf.at[quarter(c, sender)], h_ssem.at[m], h_rsem.at[c, sender], {"stage": up_stage, "model": m}
        )

    def d_copy(c, m, sender):
        return remote(
            dsend, doutbuf.at[quarter(c, sender)], d_ssem.at[m], d_rsem.at[c, sender],
            {"stage": down_stage, "model": m},
        )

    def peer_d_copy(c, d, peer, sender):
        return remote(
            doutbuf.at[quarter(c, sender)], doutbuf.at[quarter(c, sender)], d_ssem.at[d], d_rsem.at[c, sender],
            {"model": peer},
        )

    def staged_out(k, c):
        src = (na_st, z_st, at_st, dup_st, dqkv_st)[k]
        dst = (na_hbm, z_hbm, at_hbm, dup_hbm, dqkv_hbm)[k]
        return pltpu.make_async_copy(src, dst.at[rows_of(c)], out_sem.at[k])

    def full_out(k, c):
        src = (nbbuf, dmidbuf, doutbuf)[k]
        dst = (nb_hbm, dmid_hbm, dout_hbm)[k]
        return pltpu.make_async_copy(src.at[rows_of(c)], dst.at[rows_of(c)], full_sem.at[k, c])

    def causal(c):
        q_pos = c * t + lax.broadcasted_iota(jnp.int32, (t, seq), 0)
        k_pos = lax.broadcasted_iota(jnp.int32, (t, seq), 1)
        return k_pos <= q_pos

    def probs(c, i, mask):
        q = qkvbuf[rows_of(c), i * hd : (i + 1) * hd]
        k = qkvbuf[:, hw + i * hd : hw + (i + 1) * hd]
        s = jnp.where(mask, dot_nt(q, k) * scale, NEG_BIG)
        e = jnp.exp(s - jnp.max(s, axis=-1, keepdims=True))
        return e / jnp.sum(e, axis=-1, keepdims=True)

    def fwd_attn(c, first):
        @pl.when(stage == 0)
        def _():
            x_copy(c).wait()

        @pl.when(stage > 0)
        def _():
            for m in range(n_model):
                h_copy(c, 0, m).wait_recv()

        @pl.when(first)
        def _():
            weight_copy(0).wait()
            weight_copy(1).wait()

        @pl.when(jnp.logical_not(first))
        def _():
            staged_out(0, c).wait()
            staged_out(2, c).wait()
            rs_drain(0)

        h32 = hbuf[rows_of(c), :].astype(F32)
        na_st[...] = (h32 * rms_inverse(h32) * gain_a).astype(BF16)
        staged_out(0, c).start()
        wide = 3 * hw
        tile = tile_of(wide, 384)
        for j in range(wide // tile):
            cols = slice(j * tile, (j + 1) * tile)
            qkvbuf[rows_of(c), cols] = dot_nn(na_st[...], wqkv[:, cols]).astype(BF16)
        mask = causal(c)
        for i in range(heads):
            p16 = probs(c, i, mask).astype(BF16)
            v = qkvbuf[:, 2 * hw + i * hd : 2 * hw + (i + 1) * hd]
            at_st[:, i * hd : (i + 1) * hd] = dot_nn(p16, v).astype(BF16)
        staged_out(2, c).start()
        tile = tile_of(d_model)
        for j in range(d_model // tile):
            cols = slice(j * tile, (j + 1) * tile)
            rs_s[0, :, cols] = dot_nn(at_st[...], wout[:, cols]).astype(BF16)
        rs_start(0, c)

    def fwd_mid(c, first):
        @pl.when(jnp.logical_not(first))
        def _():
            ag_drain(0, nbbuf)

        mid = rs_sum(0, c) + hbuf[quarter(c, me), :].astype(F32)
        midq[c] = mid
        nbbuf[quarter(c, me), :] = (mid * rms_inverse(mid) * gain_b).astype(BF16)
        ag_start(0, nbbuf, c)

    def fwd_mlp(c, first):
        @pl.when(first)
        def _():
            weight_copy(2).wait()
            weight_copy(3).wait()

        @pl.when(jnp.logical_not(first))
        def _():
            staged_out(1, c).wait()
            rs_drain(1)

        ag_wait(0, nbbuf, c)
        full_out(0, c).start()
        tile = tile_of(ff)
        for j in range(ff // tile):
            cols = slice(j * tile, (j + 1) * tile)
            u = dot_nn(nbbuf[rows_of(c), :], wup[:, cols])
            upbuf[rows_of(c), cols] = u
            z_st[:, cols] = gelu_tanh(u).astype(BF16)
        staged_out(1, c).start()
        tile = tile_of(d_model)
        for j in range(d_model // tile):
            cols = slice(j * tile, (j + 1) * tile)
            rs_s[1, :, cols] = dot_nn(z_st[...], wdown[:, cols]).astype(BF16)
        rs_start(1, c)

    def fwd_end(c, first):
        h_out = (midq[c] + rs_sum(1, c)).astype(BF16)

        @pl.when(stage < last)
        def _():
            @pl.when(jnp.logical_not(first))
            def _():
                for m in range(n_model):
                    h_copy(c, m, me).wait_send()

            hsend[...] = h_out
            for m in range(n_model):
                h_copy(c, m, me).start()

        @pl.when(stage == last)
        def _():
            y_copy(c).wait()

            @pl.when(jnp.logical_not(first))
            def _():
                for d in order:
                    peer_d_copy(c, d, 0, me).wait_send()

            diff = h_out.astype(F32) - yq[c].astype(F32)
            lossacc[...] += fold_rows(diff * diff)
            doutbuf[quarter(c, me), :] = (diff * (1.0 / elem_count)).astype(BF16)
            for d in order:
                peer_d_copy(c, d, lax.rem(me + d, n_model), me).start()

    def fwd_body(i, carry):
        first = i == 0
        second = i == 1

        @pl.when(i < n)
        def _():
            fwd_attn(i, first)

        @pl.when(i >= 1)
        def _():
            fwd_mlp(i - 1, second)

        @pl.when(i < n)
        def _():
            fwd_mid(i, first)

        @pl.when(i >= 1)
        def _():
            fwd_end(i - 1, second)

        return carry

    lax.fori_loop(0, n + 1, fwd_body, 0)

    rs_drain(0)
    rs_drain(1)
    ag_drain(0, nbbuf)
    staged_out(0, 0).wait()
    staged_out(1, 0).wait()
    staged_out(2, 0).wait()

    @pl.when(stage < last)
    def _():
        for m in range(n_model):
            h_copy(0, m, me).wait_send()

    @pl.when(stage == last)
    def _():
        for d in order:
            peer_d_copy(0, d, 0, me).wait_send()
        total = lossacc[:, 0:128]
        for j in range(1, d_model // 128):
            total = total + lossacc[:, j * 128 : (j + 1) * 128]
        lossbuf[...] = total

    def rms_backward(v, gain, d_norm, k):
        inv = rms_inverse(v)
        normed = v * inv
        gacc[k] += fold_rows(d_norm * normed)
        d_normed = d_norm * gain
        return inv * (d_normed - normed * jnp.mean(d_normed * normed, axis=-1, keepdims=True))

    def bwd_mlp(c, first):
        @pl.when(stage < last)
        def _():
            for m in range(n_model):
                d_copy(c, 0, m).wait_recv()

        @pl.when(stage == last)
        def _():
            for d in order:
                peer_d_copy(c, d, 0, lax.rem(me + n_model - d, n_model)).wait_recv()

        full_out(2, c).start()

        @pl.when(jnp.logical_not(first))
        def _():
            staged_out(3, c).wait()
            rs_drain(2)

        tile = tile_of(ff)
        for j in range(ff // tile):
            cols = slice(j * tile, (j + 1) * tile)
            d_gelu = dot_nt(doutbuf[rows_of(c), :], wdown[cols, :])
            dup_st[:, cols] = (d_gelu * gelu_slope(upbuf[rows_of(c), cols])).astype(BF16)
        staged_out(3, c).start()
        tile = tile_of(d_model)
        for j in range(d_model // tile):
            cols = slice(j * tile, (j + 1) * tile)
            rs_s[2, :, cols] = dot_nt(dup_st[...], wup[cols, :]).astype(BF16)
        rs_start(2, c)

    def bwd_mid(c, first, slot):
        @pl.when(jnp.logical_not(first))
        def _():
            ag_drain(1, dmidbuf)

        d_norm = rs_sum(2, c)
        d_mid = doutbuf[quarter(c, me), :].astype(F32) + rms_backward(midq[c], gain_b, d_norm, 1)
        dmidq[slot] = d_mid
        dmidbuf[quarter(c, me), :] = d_mid.astype(BF16)
        ag_start(1, dmidbuf, c)

    def bwd_attn(c, first):
        ag_wait(1, dmidbuf, c)
        full_out(1, c).start()

        @pl.when(jnp.logical_not(first))
        def _():
            staged_out(4, c).wait()
            rs_drain(3)

        d_attn = dot_nt(dmidbuf[rows_of(c), :], wout[...]).astype(BF16)
        mask = causal(c)
        for i in range(heads):
            qc = slice(i * hd, (i + 1) * hd)
            kc = slice(hw + i * hd, hw + (i + 1) * hd)
            vc = slice(2 * hw + i * hd, 2 * hw + (i + 1) * hd)
            da = d_attn[:, qc]
            p = probs(c, i, mask)
            dp = dot_nt(da, qkvbuf[:, vc])
            ds = (p * (dp - jnp.sum(p * dp, axis=-1, keepdims=True)) * scale).astype(BF16)
            dqkv_st[:, qc] = dot_nn(ds, qkvbuf[:, kc]).astype(BF16)
            dkacc[:, qc] += dot_tn(ds, qkvbuf[rows_of(c), qc])
            dvacc[:, qc] += dot_tn(p.astype(BF16), da)
        dqkv_st[:, hw : 2 * hw] = dkacc[rows_of(c), :].astype(BF16)
        dqkv_st[:, 2 * hw : 3 * hw] = dvacc[rows_of(c), :].astype(BF16)
        staged_out(4, c).start()
        tile = tile_of(d_model)
        for j in range(d_model // tile):
            cols = slice(j * tile, (j + 1) * tile)
            rs_s[3, :, cols] = dot_nt(dqkv_st[...], wqkv[cols, :]).astype(BF16)
        rs_start(3, c)

    def loss_copy():
        return remote(lossbuf, lossbuf, loss_sem.at[0], loss_sem.at[1], {"stage": down_stage})

    def bwd_end(c, first, slot):
        h32 = hbuf[quarter(c, me), :].astype(F32)
        d_in = dmidq[slot] + rms_backward(h32, gain_a, rs_sum(3, c), 0)

        @pl.when(stage > 0)
        def _():
            @pl.when(jnp.logical_not(first))
            def _():
                for m in range(n_model):
                    d_copy(c, m, me).wait_send()

            dsend[...] = d_in.astype(BF16)
            for m in range(n_model):
                d_copy(c, m, me).start()

        @pl.when(first)
        def _():
            @pl.when(stage < last)
            def _():
                loss_copy().wait_recv()

            @pl.when(stage > 0)
            def _():
                loss_copy().start()

    def bwd_body(i, carry):
        first = i == 0
        second = i == 1
        c = n - 1 - i

        @pl.when(i < n)
        def _():
            bwd_mlp(c, first)

        @pl.when(i >= 1)
        def _():
            bwd_attn(c + 1, second)

        @pl.when(i < n)
        def _():
            bwd_mid(c, first, lax.rem(i, 2))

        @pl.when(i >= 1)
        def _():
            bwd_end(c + 1, second, lax.rem(i + 1, 2))

        return carry

    lax.fori_loop(0, n + 1, bwd_body, 0)

    fin_s[...] = jnp.zeros_like(fin_s)
    fin_s[0:1, :] = jnp.sum(gacc[0], axis=0, keepdims=True)
    fin_s[1:2, :] = jnp.sum(gacc[1], axis=0, keepdims=True)
    fin_s[2:3, 0:128] = jnp.sum(lossbuf[...], axis=0, keepdims=True)

    def fin_copy(d, peer):
        return remote(fin_s, fin_r.at[d - 1], fin_ssem.at[d - 1], fin_rsem.at[d - 1], {"model": peer})

    for d in order:
        fin_copy(d, lax.rem(me + d, n_model)).start()

    rs_drain(2)
    rs_drain(3)
    ag_drain(1, dmidbuf)
    staged_out(3, 0).wait()
    staged_out(4, 0).wait()
    for k in range(3):
        for c in range(n):
            full_out(k, c).wait()

    @pl.when(stage > 0)
    def _():
        for m in range(n_model):
            d_copy(0, m, me).wait_send()
        loss_copy().wait_send()

    for d in order:
        fin_copy(d, 0).wait_recv()
    parts = [jnp.where(me == 0, fin_s[...], 0.0)]
    for m in range(n_model):
        term = jnp.where(me == m, fin_s[...], 0.0)
        for d in range(1, n_model):
            term = term + jnp.where(lax.rem(m + d, n_model) == me, fin_r[d - 1], 0.0)
        parts.append(term)
    total = parts[1]
    for m in range(1, n_model):
        total = total + parts[m + 1]
    small_ref[0:2, :] = total[0:2, :]
    loss = jnp.sum(total[2:3, :], axis=-1, keepdims=True) * (0.5 / elem_count)
    small_ref[2:8, :] = jnp.broadcast_to(loss, (6, d_model))
    for d in order:
        fin_copy(d, 0).wait_send()


def run_step(cfg, x, y, wqkv, wout, wup, wdown, gain):
    n, t, tq, n_model, seq = cfg["n"], cfg["t"], cfg["tq"], cfg["n_model"], cfg["seq"]
    d_model, ff, hw = cfg["d_model"], cfg["ff"], cfg["heads"] * cfg["hd"]
    dma = pltpu.SemaphoreType.DMA
    near = max(n_model - 1, 1)
    act = lambda width: jax.ShapeDtypeStruct((seq, width), BF16)
    any_spec = pl.BlockSpec(memory_space=pl.ANY)
    vmem_spec = pl.BlockSpec(memory_space=pltpu.VMEM)
    scratch = [
        pltpu.VMEM((d_model, 3 * hw), BF16),
        pltpu.VMEM((hw, d_model), BF16),
        pltpu.VMEM((d_model, ff), BF16),
        pltpu.VMEM((ff, d_model), BF16),
        pltpu.VMEM((seq, d_model), BF16),
        pltpu.VMEM((seq, d_model), BF16),
        pltpu.VMEM((seq, d_model), BF16),
        pltpu.VMEM((seq, d_model), BF16),
        pltpu.VMEM((seq, 3 * hw), BF16),
        pltpu.VMEM((seq, ff), F32),
        pltpu.VMEM((n, tq, d_model), F32),
        pltpu.VMEM((n, tq, d_model), BF16),
        pltpu.VMEM((seq, hw), F32),
        pltpu.VMEM((seq, hw), F32),
        pltpu.VMEM((4, n, near, tq, d_model), BF16),
        pltpu.VMEM((4, t, d_model), BF16),
        pltpu.VMEM((t, d_model), BF16),
        pltpu.VMEM((t, ff), BF16),
        pltpu.VMEM((t, hw), BF16),
        pltpu.VMEM((t, ff), BF16),
        pltpu.VMEM((t, 3 * hw), BF16),
        pltpu.VMEM((tq, d_model), BF16),
        pltpu.VMEM((tq, d_model), BF16),
        pltpu.VMEM((2, tq, d_model), F32),
        pltpu.VMEM((8, d_model), F32),
        pltpu.VMEM((2, 8, d_model), F32),
        pltpu.VMEM((8, 128), F32),
        pltpu.VMEM((8, d_model), F32),
        pltpu.VMEM((near, 8, d_model), F32),
        dma((4,)),
        dma((n,)),
        dma((n,)),
        dma((n, n_model)),
        dma((n_model,)),
        dma((n, n_model)),
        dma((n_model,)),
        dma((4, n, near)),
        dma((4, near)),
        dma((2, n, near)),
        dma((2, near)),
        dma((5,)),
        dma((3, n)),
        dma((2,)),
        dma((near,)),
        dma((near,)),
    ]
    return pl.pallas_call(
        functools.partial(step_kernel, cfg),
        name="pipeline_step",
        out_shape=(
            act(d_model), act(d_model), act(hw), act(ff), act(3 * hw), act(d_model), act(ff), act(d_model),
            jax.ShapeDtypeStruct((8, d_model), F32),
        ),
        in_specs=[any_spec] * 6 + [vmem_spec],
        out_specs=[any_spec] * 8 + [vmem_spec],
        scratch_shapes=scratch,
        compiler_params=pltpu.CompilerParams(
            collective_id=0, has_side_effects=True, vmem_limit_bytes=VMEM_BYTES
        ),
    )(x, y, wqkv, wout, wup, wdown, gain)


def solution(mesh):
    n_stage = mesh.shape["stage"]
    n_model = mesh.shape["model"]

    def device_fn(x_in, y_target, w_qkv, w_out, w_up, w_down, norm_gain):
        n_batch, seq_len, d_model = x_in.shape
        heads, hd, ff = w_qkv.shape[3], w_qkv.shape[4], w_up.shape[2]
        t = min(CHUNK, seq_len)
        cfg = dict(
            n=seq_len // t, t=t, tq=t // n_model, n_model=n_model, n_stage=n_stage, seq=seq_len, d_model=d_model,
            heads=heads, hd=hd, ff=ff, elem_count=n_batch * seq_len * d_model,
        )
        na, nb, at, z, dqkv, dmid, dup, dout, small = run_step(
            cfg, x_in[0], y_target[0], w_qkv[0].reshape(d_model, 3 * heads * hd), w_out[0].reshape(heads * hd, d_model),
            w_up[0], w_down[0], norm_gain[0].astype(F32),
        )
        grad_qkv = dot_tn(na, dqkv).reshape(1, d_model, 3, heads, hd)
        grad_out = dot_tn(at, dmid).reshape(1, heads, hd, d_model)
        grad_up = dot_tn(nb, dup)[None]
        grad_down = dot_tn(z, dout)[None]
        return small[2:3, 0], grad_qkv, grad_out, grad_up, grad_down, small[None, 0:2]

    act_spec = P("data", None, None)
    weight_specs = (
        P("stage", None, None, "model", None),
        P("stage", "model", None, None),
        P("stage", None, "model"),
        P("stage", "model", None),
        P("stage", None, None),
    )
    grad_specs = (
        P(("data", "stage"), None, None, "model", None),
        P(("data", "stage"), "model", None, None),
        P(("data", "stage"), None, "model"),
        P(("data", "stage"), "model", None),
        P(("data", "stage"), None, None),
    )
    return jax.shard_map(
        device_fn,
        mesh=mesh,
        in_specs=(act_spec, act_spec) + weight_specs,
        out_specs=(P("data"),) + grad_specs,
        check_vma=False,
    )
```

```python
import functools
import math

import jax
import jax.numpy as jnp
from jax import lax
from jax.experimental import pallas as pl
from jax.experimental.pallas import tpu as pltpu
from jax.sharding import PartitionSpec as P

NORM_EPS = 1e-6
NEG_BIG = -1e30
CHUNK = 64
KEY_STEP = 256
GRAD_ROWS = 768
LOG2E = 1.4426950408889634
F32 = jnp.float32
BF16 = jnp.bfloat16
MESH_ID = pl.DeviceIdType.MESH
GELU_A = math.sqrt(2.0 / math.pi)
GELU_B = 0.044715
VMEM_BYTES = 67043328


def dot_nn(a, b):
    return lax.dot_general(a, b, (((1,), (0,)), ((), ())), preferred_element_type=F32)


def dot_nt(a, b):
    return lax.dot_general(a, b, (((1,), (1,)), ((), ())), preferred_element_type=F32)


def dot_tn(a, b):
    return lax.dot_general(a, b, (((0,), (0,)), ((), ())), preferred_element_type=F32)


def rms_inverse(v):
    return lax.rsqrt(jnp.mean(v * v, axis=-1, keepdims=True) + NORM_EPS)


def gelu_tanh(u):
    return u * (0.5 * (1.0 + jnp.tanh(GELU_A * (u + GELU_B * (u * u * u)))))


def gelu_slope(u):
    t = jnp.tanh(GELU_A * (u + GELU_B * (u * u * u)))
    return 0.5 * (1.0 + t) + (0.5 * u) * (1.0 - t * t) * (GELU_A * (1.0 + (3.0 * GELU_B) * (u * u)))


def tile_of(width, top=512):
    for tile in (top, 512, 384, 256, 128):
        if width % tile == 0:
            return tile
    return width


def fold_rows(v):
    total = v[0:8]
    for r in range(8, v.shape[0], 8):
        total = total + v[r : r + 8]
    return total


def step_kernel(cfg, *refs):
    n, t, tq, n_model, n_stage = cfg["n"], cfg["t"], cfg["tq"], cfg["n_model"], cfg["n_stage"]
    seq, d_model, heads, hd, ff = cfg["seq"], cfg["d_model"], cfg["heads"], cfg["hd"], cfg["ff"]
    hw = heads * hd
    elem_count = cfg["elem_count"]
    scale = hd**-0.5
    (
        x_hbm, y_hbm, wqkv_hbm, wout_hbm, wup_hbm, wdown_hbm, gain_ref,
        na_hbm, nb_hbm, at_hbm, z_hbm, dqkv_hbm, dmid_hbm, dup_hbm, dout_hbm, small_ref,
        wqkv, wout, wup, wdown, wqkv_t, wout_t, wup_t, wdown_t, hbuf, nbbuf, doutbuf, dmidbuf, qkvbuf, upbuf, midq, yq, dkacc, dvacc,
        rs_r, rs_s, na_st, z_st, at_st, dup_st, dqkv_st, hsend, dsend, dmidq,
        lossacc, gacc, lossbuf, fin_s, fin_r,
        w_sem, x_sem, y_sem, h_rsem, h_ssem, d_rsem, d_ssem, rs_rsem, rs_ssem, ag_rsem, ag_ssem,
        out_sem, full_sem, loss_sem, fin_rsem, fin_ssem,
    ) = refs
    me = lax.axis_index("model")
    stage = lax.axis_index("stage")
    last = n_stage - 1
    order = [d for d in (2, 1, 3) if d < n_model] if n_model > 2 else list(range(1, n_model))

    def remote(src, dst, ssem, rsem, where):
        return pltpu.make_async_remote_copy(
            src_ref=src, dst_ref=dst, send_sem=ssem, recv_sem=rsem, device_id=where, device_id_type=MESH_ID
        )

    def rows_of(c):
        return pl.ds(pl.multiple_of(c * t, t), t)

    def quarter(c, m):
        return pl.ds(pl.multiple_of(c * t + m * tq, tq), tq)

    own = pl.ds(pl.multiple_of(me * tq, tq), tq)

    slabs = 3 * heads

    def weight_copy(k):
        if k < slabs:
            return pltpu.make_async_copy(wqkv_hbm.at[k], wqkv.at[:, pl.ds(k * hd, hd)], w_sem.at[k])
        src = (wout_hbm, wup_hbm, wdown_hbm)[k - slabs]
        dst = (wout, wup, wdown)[k - slabs]
        return pltpu.make_async_copy(src, dst, w_sem.at[k])

    def x_copy(c):
        return pltpu.make_async_copy(x_hbm.at[rows_of(c)], hbuf.at[rows_of(c)], x_sem.at[c])

    def y_copy(c):
        return pltpu.make_async_copy(y_hbm.at[quarter(c, me)], yq.at[c], y_sem.at[c])

    @pl.when(stage == 0)
    def _():
        x_copy(0).start()

    for k in range(slabs + 3):
        weight_copy(k).start()

    @pl.when(stage == 0)
    def _():
        for c in range(1, n):
            x_copy(c).start()

    @pl.when(stage == last)
    def _():
        for c in range(n):
            y_copy(c).start()

    barrier = pltpu.get_barrier_semaphore()
    up_stage = lax.rem(stage + 1, n_stage)
    down_stage = lax.rem(stage + n_stage - 1, n_stage)
    greet = [{"model": lax.rem(me + d, n_model)} for d in range(1, n_model)]
    greet += [{"stage": up_stage, "model": m} for m in range(n_model)]
    if n_stage > 2:
        greet += [{"stage": down_stage, "model": m} for m in range(n_model)]
    for where in greet:
        pl.semaphore_signal(barrier, inc=1, device_id=where, device_id_type=MESH_ID)

    qkvbuf[:, 2 * hw : 3 * hw] = jnp.zeros((seq, hw), BF16)
    lossacc[...] = jnp.zeros_like(lossacc)
    gacc[...] = jnp.zeros_like(gacc)
    pl.semaphore_wait(barrier, len(greet))

    gains = gain_ref[...].astype(F32)
    gain_a = gains[0:1, :]
    gain_b = gains[1:2, :]

    def rs_copy(p, c, d, peer):
        slot = lax.rem(c, 2)
        return remote(
            rs_s.at[p, slot, pl.ds(pl.multiple_of(peer * tq, tq), tq)], rs_r.at[p % 2, c, d - 1],
            rs_ssem.at[p, slot, d - 1], rs_rsem.at[p, c, d - 1], {"model": peer},
        )

    def rs_start(p, c):
        for d in order:
            rs_copy(p, c, d, lax.rem(me + d, n_model)).start()

    def rs_drain(p, c):
        for d in order:
            rs_copy(p, c, d, 0).wait_send()

    def rs_sum(p, c):
        with jax.named_scope(f"rs_wait{p}"):
            for d in order:
                rs_copy(p, c, d, 0).wait_recv()
        total = rs_s[p, lax.rem(c, 2), own, :].astype(F32)
        for d in range(1, n_model):
            total = total + rs_r[p % 2, c, d - 1].astype(F32)
        return total

    def ag_copy(p, buf, c, d, peer, owner):
        return remote(
            buf.at[quarter(c, owner)], buf.at[quarter(c, owner)],
            ag_ssem.at[p, d - 1], ag_rsem.at[p, c, d - 1], {"model": peer},
        )

    def ag_start(p, buf, c):
        for d in order:
            ag_copy(p, buf, c, d, lax.rem(me + d, n_model), me).start()

    def ag_drain(p, buf):
        for d in order:
            ag_copy(p, buf, 0, d, 0, 0).wait_send()

    def ag_wait(p, buf, c):
        with jax.named_scope(f"ag_wait{p}"):
            for d in order:
                ag_copy(p, buf, c, d, 0, lax.rem(me + n_model - d, n_model)).wait_recv()

    def h_copy(c, m, sender):
        return remote(
            hsend, hbuf.at[quarter(c, sender)], h_ssem.at[m], h_rsem.at[c, sender], {"stage": up_stage, "model": m}
        )

    def d_copy(c, m, sender):
        return remote(
            dsend, doutbuf.at[quarter(c, sender)], d_ssem.at[m], d_rsem.at[c, sender],
            {"stage": down_stage, "model": m},
        )

    def peer_d_copy(c, d, peer, sender):
        return remote(
            doutbuf.at[quarter(c, sender)], doutbuf.at[quarter(c, sender)], d_ssem.at[d], d_rsem.at[c, sender],
            {"model": peer},
        )

    def staged_out(k, c):
        src = (na_st, z_st, at_st, dup_st, dqkv_st)[k]
        dst = (na_hbm, z_hbm, at_hbm, dup_hbm, dqkv_hbm)[k]
        return pltpu.make_async_copy(src, dst.at[rows_of(c)], out_sem.at[k])

    def full_out(k, c):
        src = (nbbuf, dmidbuf, doutbuf)[k]
        dst = (nb_hbm, dmid_hbm, dout_hbm)[k]
        return pltpu.make_async_copy(src.at[rows_of(c)], dst.at[rows_of(c)], full_sem.at[k, c])

    key_step = min(KEY_STEP, seq)

    def by_prefix(c, body):
        need = lax.div(c * t + t - 1, key_step)
        for k in range(seq // key_step):

            @pl.when(need == k)
            def _():
                body((k + 1) * key_step)

    def scores(c, keys):
        return [
            dot_nt(qkvbuf[rows_of(c), i * hd : (i + 1) * hd], qkvbuf[0:keys, hw + i * hd : hw + (i + 1) * hd])
            for i in range(heads)
        ]

    def causal_softmax(c, keys, raw):
        q_pos = c * t + lax.broadcasted_iota(jnp.int32, (t, keys), 0)
        k_pos = lax.broadcasted_iota(jnp.int32, (t, keys), 1)
        s = jnp.where(k_pos <= q_pos, raw, NEG_BIG / scale)
        e = jnp.exp2((s - jnp.max(s, axis=-1, keepdims=True)) * (scale * LOG2E))
        return e * (1.0 / jnp.sum(e, axis=-1, keepdims=True))

    def fwd_attn(c, first):
        @pl.when(stage == 0)
        def _():
            x_copy(c).wait()

        @pl.when(stage > 0)
        def _():
            with jax.named_scope("h_wait"):
                for m in range(n_model):
                    h_copy(c, 0, m).wait_recv()

        @pl.when(first & (stage == 0))
        def _():
            for k in range(slabs + 1):
                weight_copy(k).wait()

        @pl.when(jnp.logical_not(first))
        def _():
            staged_out(0, c).wait()
            staged_out(2, c).wait()

        @pl.when(c >= 2)
        def _():
            rs_drain(0, c)

        slot = lax.rem(c, 2)

        h32 = hbuf[rows_of(c), :].astype(F32)
        na_st[...] = (h32 * rms_inverse(h32) * gain_a).astype(BF16)
        staged_out(0, c).start()
        wide = 3 * hw
        tile = tile_of(wide, 384)
        for j in range(wide // tile):
            cols = slice(j * tile, (j + 1) * tile)
            qkvbuf[rows_of(c), cols] = dot_nn(na_st[...], wqkv[:, cols]).astype(BF16)

        def attend(keys):
            probs = [causal_softmax(c, keys, raw).astype(BF16) for raw in scores(c, keys)]
            for i in range(heads):
                v = qkvbuf[0:keys, 2 * hw + i * hd : 2 * hw + (i + 1) * hd]
                at_st[:, i * hd : (i + 1) * hd] = dot_nn(probs[i], v).astype(BF16)

        by_prefix(c, attend)
        staged_out(2, c).start()
        tile = tile_of(d_model)
        for j in range(d_model // tile):
            cols = slice(j * tile, (j + 1) * tile)
            rs_s[0, slot, :, cols] = dot_nn(at_st[...], wout[:, cols]).astype(BF16)
        rs_start(0, c)

    def fwd_mid(c, first):
        @pl.when(jnp.logical_not(first))
        def _():
            ag_drain(0, nbbuf)

        mid = rs_sum(0, c) + hbuf[quarter(c, me), :].astype(F32)
        midq[c] = mid
        nbbuf[quarter(c, me), :] = (mid * rms_inverse(mid) * gain_b).astype(BF16)
        ag_start(0, nbbuf, c)

    def fwd_mlp(c, first):
        @pl.when(first & (stage == 0))
        def _():
            weight_copy(slabs + 1).wait()
            weight_copy(slabs + 2).wait()

        @pl.when(jnp.logical_not(first))
        def _():
            staged_out(1, c).wait()

        @pl.when(c >= 2)
        def _():
            rs_drain(1, c)

        slot = lax.rem(c, 2)

        ag_wait(0, nbbuf, c)
        full_out(0, c).start()
        tile = tile_of(ff)
        for j in range(ff // tile):
            cols = slice(j * tile, (j + 1) * tile)
            u = dot_nn(nbbuf[rows_of(c), :], wup[:, cols])
            upbuf[rows_of(c), cols] = u
            z_st[:, cols] = gelu_tanh(u).astype(BF16)
        staged_out(1, c).start()
        tile = tile_of(d_model)
        for j in range(d_model // tile):
            cols = slice(j * tile, (j + 1) * tile)
            rs_s[1, slot, :, cols] = dot_nn(z_st[...], wdown[:, cols]).astype(BF16)
        rs_start(1, c)

    def fwd_end(c, first):
        h_out = (midq[c] + rs_sum(1, c)).astype(BF16)

        @pl.when(stage < last)
        def _():
            @pl.when(jnp.logical_not(first))
            def _():
                for m in range(n_model):
                    h_copy(c, m, me).wait_send()

            hsend[...] = h_out
            for m in range(n_model):
                h_copy(c, m, me).start()

        @pl.when(stage == last)
        def _():
            y_copy(c).wait()

            @pl.when(jnp.logical_not(first))
            def _():
                for d in order:
                    peer_d_copy(c, d, 0, me).wait_send()

            diff = h_out.astype(F32) - yq[c].astype(F32)
            lossacc[...] += fold_rows(diff * diff)
            doutbuf[quarter(c, me), :] = (diff * (1.0 / elem_count)).astype(BF16)
            for d in order:
                peer_d_copy(c, d, lax.rem(me + d, n_model), me).start()

    def pipeline(phases, chunk_of):
        deepest = max(lag for _, lag, _ in phases)

        def body(i, carry):
            for phase, lag, name in phases:
                j = i - lag

                @pl.when((j >= 0) & (j < n))
                def _():
                    with jax.named_scope(name):
                        phase(chunk_of(j), j == 0)

            return carry

        lax.fori_loop(0, n + deepest, body, 0)

    def flip_weights():
        for w, w_t in ((wdown, wdown_t), (wup, wup_t), (wout, wout_t), (wqkv, wqkv_t)):
            depth = tile_of(w.shape[0], 256)
            for r in range(w.shape[0] // depth):
                w_t[:, r * depth : (r + 1) * depth] = w[r * depth : (r + 1) * depth, :].T

    @pl.when(stage > 0)
    def _():
        for k in range(slabs + 3):
            weight_copy(k).wait()
        flip_weights()

    pipeline(
        [(fwd_attn, 0, "fwd_attn"), (fwd_mlp, 1, "fwd_mlp"), (fwd_mid, 0, "fwd_mid"), (fwd_end, 1, "fwd_end")],
        lambda j: j,
    )

    @pl.when(stage == 0)
    def _():
        flip_weights()

    dkacc[...] = jnp.zeros_like(dkacc)
    dvacc[...] = jnp.zeros_like(dvacc)

    for c in range(min(n, 2)):
        rs_drain(0, c)
        rs_drain(1, c)
    ag_drain(0, nbbuf)
    staged_out(0, 0).wait()
    staged_out(1, 0).wait()
    staged_out(2, 0).wait()

    @pl.when(stage < last)
    def _():
        for m in range(n_model):
            h_copy(0, m, me).wait_send()

    @pl.when(stage == last)
    def _():
        for d in order:
            peer_d_copy(0, d, 0, me).wait_send()
        total = lossacc[:, 0:128]
        for j in range(1, d_model // 128):
            total = total + lossacc[:, j * 128 : (j + 1) * 128]
        lossbuf[...] = total

    def rms_backward(v, gain, d_norm, k):
        inv = rms_inverse(v)
        normed = v * inv
        gacc[k] += fold_rows(d_norm * normed)
        d_normed = d_norm * gain
        return inv * (d_normed - normed * jnp.mean(d_normed * normed, axis=-1, keepdims=True))

    def bwd_mlp(c, first):
        @pl.when(stage < last)
        def _():
            with jax.named_scope("d_wait"):
                for m in range(n_model):
                    d_copy(c, 0, m).wait_recv()

        @pl.when(stage == last)
        def _():
            for d in order:
                peer_d_copy(c, d, 0, lax.rem(me + n_model - d, n_model)).wait_recv()

        full_out(2, c).start()

        @pl.when(jnp.logical_not(first))
        def _():
            staged_out(3, c).wait()

        @pl.when(c < n - 2)
        def _():
            rs_drain(2, c)

        slot = lax.rem(c, 2)

        tile = tile_of(ff)
        for j in range(ff // tile):
            cols = slice(j * tile, (j + 1) * tile)
            d_gelu = dot_nn(doutbuf[rows_of(c), :], wdown_t[:, cols])
            dup_st[:, cols] = (d_gelu * gelu_slope(upbuf[rows_of(c), cols])).astype(BF16)
        staged_out(3, c).start()
        tile = tile_of(d_model)
        for j in range(d_model // tile):
            cols = slice(j * tile, (j + 1) * tile)
            rs_s[2, slot, :, cols] = dot_nn(dup_st[...], wup_t[:, cols]).astype(BF16)
        rs_start(2, c)

    def bwd_mid(c, first):
        @pl.when(jnp.logical_not(first))
        def _():
            ag_drain(1, dmidbuf)

        d_norm = rs_sum(2, c)
        d_mid = doutbuf[quarter(c, me), :].astype(F32) + rms_backward(midq[c], gain_b, d_norm, 1)
        dmidq[lax.rem(c, 4)] = d_mid
        dmidbuf[quarter(c, me), :] = d_mid.astype(BF16)
        ag_start(1, dmidbuf, c)

    def bwd_attn(c, first):
        ag_wait(1, dmidbuf, c)
        full_out(1, c).start()

        @pl.when(jnp.logical_not(first))
        def _():
            staged_out(4, c).wait()

        @pl.when(c < n - 2)
        def _():
            rs_drain(3, c)

        slot = lax.rem(c, 2)

        d_attn = dot_nn(dmidbuf[rows_of(c), :], wout_t[...]).astype(BF16)
        at_st[...] = d_attn

        def attend(keys):
            raws = scores(c, keys)
            d_probs = [
                dot_nt(at_st[:, i * hd : (i + 1) * hd], qkvbuf[0:keys, 2 * hw + i * hd : 2 * hw + (i + 1) * hd])
                for i in range(heads)
            ]
            probs, d_scores = [], []
            for raw, dp in zip(raws, d_probs):
                p = causal_softmax(c, keys, raw)
                probs.append(p.astype(BF16))
                d_scores.append((p * (dp - jnp.sum(p * dp, axis=-1, keepdims=True)) * scale).astype(BF16))
            for i in range(heads):
                cols = slice(i * hd, (i + 1) * hd)
                dqkv_st[:, cols] = dot_nn(d_scores[i], qkvbuf[0:keys, hw + i * hd : hw + (i + 1) * hd]).astype(BF16)
            for i in range(heads):
                cols = slice(i * hd, (i + 1) * hd)
                dkacc[0:keys, cols] += dot_tn(d_scores[i], qkvbuf[rows_of(c), cols])
                dvacc[0:keys, cols] += dot_tn(probs[i], at_st[:, cols])

        by_prefix(c, attend)
        dqkv_st[:, hw : 2 * hw] = dkacc[rows_of(c), :].astype(BF16)
        dqkv_st[:, 2 * hw : 3 * hw] = dvacc[rows_of(c), :].astype(BF16)
        staged_out(4, c).start()
        tile = tile_of(d_model)
        for j in range(d_model // tile):
            cols = slice(j * tile, (j + 1) * tile)
            rs_s[3, slot, :, cols] = dot_nn(dqkv_st[...], wqkv_t[:, cols]).astype(BF16)
        rs_start(3, c)

    def loss_copy():
        return remote(lossbuf, lossbuf, loss_sem.at[0], loss_sem.at[1], {"stage": down_stage})

    def bwd_end(c, first):
        h32 = hbuf[quarter(c, me), :].astype(F32)
        d_in = dmidq[lax.rem(c, 4)] + rms_backward(h32, gain_a, rs_sum(3, c), 0)

        @pl.when(stage > 0)
        def _():
            @pl.when(jnp.logical_not(first))
            def _():
                for m in range(n_model):
                    d_copy(c, m, me).wait_send()

            dsend[...] = d_in.astype(BF16)
            for m in range(n_model):
                d_copy(c, m, me).start()

        @pl.when(first)
        def _():
            @pl.when(stage < last)
            def _():
                loss_copy().wait_recv()

            @pl.when(stage > 0)
            def _():
                loss_copy().start()

    pipeline(
        [(bwd_mlp, 0, "bwd_mlp"), (bwd_attn, 1, "bwd_attn"), (bwd_mid, 0, "bwd_mid"), (bwd_end, 1, "bwd_end")],
        lambda j: n - 1 - j,
    )

    fin_s[...] = jnp.zeros_like(fin_s)
    fin_s[0:1, :] = jnp.sum(gacc[0], axis=0, keepdims=True)
    fin_s[1:2, :] = jnp.sum(gacc[1], axis=0, keepdims=True)
    fin_s[2:3, 0:128] = jnp.sum(lossbuf[...], axis=0, keepdims=True)

    def fin_copy(d, peer):
        return remote(fin_s, fin_r.at[d - 1], fin_ssem.at[d - 1], fin_rsem.at[d - 1], {"model": peer})

    for d in order:
        fin_copy(d, lax.rem(me + d, n_model)).start()

    for c in range(min(n, 2)):
        rs_drain(2, c)
        rs_drain(3, c)
    ag_drain(1, dmidbuf)
    staged_out(3, 0).wait()
    staged_out(4, 0).wait()
    for k in range(3):
        for c in range(n):
            full_out(k, c).wait()

    @pl.when(stage > 0)
    def _():
        for m in range(n_model):
            d_copy(0, m, me).wait_send()
        loss_copy().wait_send()

    for d in order:
        fin_copy(d, 0).wait_recv()
    parts = [jnp.where(me == 0, fin_s[...], 0.0)]
    for m in range(n_model):
        term = jnp.where(me == m, fin_s[...], 0.0)
        for d in range(1, n_model):
            term = term + jnp.where(lax.rem(m + d, n_model) == me, fin_r[d - 1], 0.0)
        parts.append(term)
    total = parts[1]
    for m in range(1, n_model):
        total = total + parts[m + 1]
    small_ref[0:2, :] = total[0:2, :]
    loss = jnp.sum(total[2:3, :], axis=-1, keepdims=True) * (0.5 / elem_count)
    small_ref[2:8, :] = jnp.broadcast_to(loss, (6, d_model))
    for d in order:
        fin_copy(d, 0).wait_send()


def run_step(cfg, x, y, wqkv, wout, wup, wdown, gain):
    n, t, tq, n_model, seq = cfg["n"], cfg["t"], cfg["tq"], cfg["n_model"], cfg["seq"]
    d_model, ff, hw = cfg["d_model"], cfg["ff"], cfg["heads"] * cfg["hd"]
    dma = pltpu.SemaphoreType.DMA
    near = max(n_model - 1, 1)
    act = lambda width: jax.ShapeDtypeStruct((seq, width), BF16)
    any_spec = pl.BlockSpec(memory_space=pl.ANY)
    vmem_spec = pl.BlockSpec(memory_space=pltpu.VMEM)
    scratch = [
        pltpu.VMEM((d_model, 3 * hw), BF16),
        pltpu.VMEM((hw, d_model), BF16),
        pltpu.VMEM((d_model, ff), BF16),
        pltpu.VMEM((ff, d_model), BF16),
        pltpu.VMEM((3 * hw, d_model), BF16),
        pltpu.VMEM((d_model, hw), BF16),
        pltpu.VMEM((ff, d_model), BF16),
        pltpu.VMEM((d_model, ff), BF16),
        pltpu.VMEM((seq, d_model), BF16),
        pltpu.VMEM((seq, d_model), BF16),
        pltpu.VMEM((seq, d_model), BF16),
        pltpu.VMEM((seq, d_model), BF16),
        pltpu.VMEM((seq, 3 * hw), BF16),
        pltpu.VMEM((seq, ff), F32),
        pltpu.VMEM((n, tq, d_model), F32),
        pltpu.VMEM((n, tq, d_model), BF16),
        pltpu.VMEM((seq, hw), F32),
        pltpu.VMEM((seq, hw), F32),
        pltpu.VMEM((2, n, near, tq, d_model), BF16),
        pltpu.VMEM((4, 2, t, d_model), BF16),
        pltpu.VMEM((t, d_model), BF16),
        pltpu.VMEM((t, ff), BF16),
        pltpu.VMEM((t, hw), BF16),
        pltpu.VMEM((t, ff), BF16),
        pltpu.VMEM((t, 3 * hw), BF16),
        pltpu.VMEM((tq, d_model), BF16),
        pltpu.VMEM((tq, d_model), BF16),
        pltpu.VMEM((4, tq, d_model), F32),
        pltpu.VMEM((8, d_model), F32),
        pltpu.VMEM((2, 8, d_model), F32),
        pltpu.VMEM((8, 128), F32),
        pltpu.VMEM((8, d_model), F32),
        pltpu.VMEM((near, 8, d_model), F32),
        dma((3 * cfg["heads"] + 3,)),
        dma((n,)),
        dma((n,)),
        dma((n, n_model)),
        dma((n_model,)),
        dma((n, n_model)),
        dma((n_model,)),
        dma((4, n, near)),
        dma((4, 2, near)),
        dma((2, n, near)),
        dma((2, near)),
        dma((5,)),
        dma((3, n)),
        dma((2,)),
        dma((near,)),
        dma((near,)),
    ]
    return pl.pallas_call(
        functools.partial(step_kernel, cfg),
        name="pipeline_step",
        out_shape=(
            act(d_model), act(d_model), act(hw), act(ff), act(3 * hw), act(d_model), act(ff), act(d_model),
            jax.ShapeDtypeStruct((8, d_model), F32),
        ),
        in_specs=[any_spec] * 6 + [vmem_spec],
        out_specs=[any_spec] * 8 + [vmem_spec],
        scratch_shapes=scratch,
        compiler_params=pltpu.CompilerParams(
            collective_id=0, has_side_effects=True, vmem_limit_bytes=VMEM_BYTES
        ),
    )(x, y, wqkv, wout, wup, wdown, gain)


def grads_kernel(nj, bm, *refs):
    ins, small = refs[: 2 * nj], refs[2 * nj]
    outs, loss_ref, gain_ref = refs[2 * nj + 1 : 3 * nj + 1], refs[3 * nj + 1], refs[3 * nj + 2]
    scratch = refs[3 * nj + 3 :]
    bufs, stages, in_sem, out_sem = scratch[: 2 * nj], scratch[2 * nj : 3 * nj], scratch[-2], scratch[-1]

    def load(k):
        return pltpu.make_async_copy(ins[k], bufs[k], in_sem.at[k])

    for k in range(2 * nj):
        load(k).start()
    loss_ref[...] = small[2:3, 0:1]
    gain_ref[...] = small[0:2, :]
    for j in range(nj):
        load(2 * j).wait()
        load(2 * j + 1).wait()
        a, b, out, stage = bufs[2 * j], bufs[2 * j + 1], outs[j], stages[j]
        rows = a.shape[1]
        step = min(bm, rows)
        blocks = rows // step

        def put(i, slot):
            where = pl.ds(pl.multiple_of(i * step, step), step)
            dst = out.at[:, where] if len(out.shape) == 3 else out.at[where]
            return pltpu.make_async_copy(stage.at[slot], dst, out_sem.at[j, slot])

        def block(i, carry):
            slot = lax.rem(i, 2)

            @pl.when(i >= 2)
            def _():
                put(i, slot).wait()

            acc = dot_tn(a[:, pl.ds(pl.multiple_of(i * step, step), step)], b[...])
            if len(out.shape) == 3:
                lanes = out.shape[2]
                for s in range(out.shape[0]):
                    stage[slot, s] = acc[:, s * lanes : (s + 1) * lanes]
            else:
                stage[slot] = acc
            put(i, slot).start()
            return carry

        lax.fori_loop(0, blocks, block, 0)
    for j in range(nj):
        rows = bufs[2 * j].shape[1]
        step = min(bm, rows)
        for slot in range(min(2, rows // step)):
            out, stage = outs[j], stages[j]
            dst = out.at[:, 0:step] if len(out.shape) == 3 else out.at[0:step]
            pltpu.make_async_copy(stage.at[slot], dst, out_sem.at[j, slot]).wait()


def weight_grads(pairs, out_shapes, small, bm):
    nj = len(pairs)
    flat = [x for pair in pairs for x in pair]
    any_spec = pl.BlockSpec(memory_space=pl.ANY)
    vmem_spec = pl.BlockSpec(memory_space=pltpu.VMEM)
    stages = []
    for (a, _), out in zip(pairs, out_shapes):
        step = min(bm, a.shape[1])
        stages.append(pltpu.VMEM((2,) + out[:-2] + (step, out[-1]), F32))
    outs = [jax.ShapeDtypeStruct(out, F32) for out in out_shapes]
    outs += [jax.ShapeDtypeStruct((1, 1), F32), jax.ShapeDtypeStruct((2, small.shape[1]), F32)]
    return pl.pallas_call(
        functools.partial(grads_kernel, nj, bm),
        name="weight_grads",
        out_shape=outs,
        in_specs=[any_spec] * (2 * nj) + [vmem_spec],
        out_specs=[any_spec] * nj + [vmem_spec] * 2,
        scratch_shapes=[pltpu.VMEM(x.shape, x.dtype) for x in flat]
        + stages
        + [pltpu.SemaphoreType.DMA((2 * nj,)), pltpu.SemaphoreType.DMA((nj, 2))],
        compiler_params=pltpu.CompilerParams(vmem_limit_bytes=VMEM_BYTES),
    )(*flat, small)


def solution(mesh):
    n_stage = mesh.shape["stage"]
    n_model = mesh.shape["model"]

    def device_fn(x_in, y_target, w_qkv, w_out, w_up, w_down, norm_gain):
        n_batch, seq_len, d_model = x_in.shape
        heads, hd, ff = w_qkv.shape[3], w_qkv.shape[4], w_up.shape[2]
        t = min(CHUNK, seq_len)
        cfg = dict(
            n=seq_len // t, t=t, tq=t // n_model, n_model=n_model, n_stage=n_stage, seq=seq_len, d_model=d_model,
            heads=heads, hd=hd, ff=ff, elem_count=n_batch * seq_len * d_model,
        )
        na, nb, at, z, dqkv, dmid, dup, dout, small = run_step(
            cfg, x_in[0], y_target[0], w_qkv[0].transpose(1, 2, 0, 3).reshape(3 * heads, d_model, hd), w_out[0].reshape(heads * hd, d_model),
            w_up[0], w_down[0], norm_gain[0],
        )
        g_out, g_up, g_down, g_qkv, loss, g_gain = weight_grads(
            [(at, dmid), (nb, dup), (z, dout), (na, dqkv)],
            [(heads * hd, d_model), (d_model, ff), (ff, d_model), (3 * heads, d_model, hd)],
            small,
            tile_of(d_model, GRAD_ROWS),
        )
        grad_qkv = g_qkv.reshape(3, heads, d_model, hd).transpose(2, 0, 1, 3)[None]
        return loss.reshape(1), grad_qkv, g_out.reshape(1, heads, hd, d_model), g_up[None], g_down[None], g_gain[None]

    act_spec = P("data", None, None)
    weight_specs = (
        P("stage", None, None, "model", None),
        P("stage", "model", None, None),
        P("stage", None, "model"),
        P("stage", "model", None),
        P("stage", None, None),
    )
    grad_specs = (
        P(("data", "stage"), None, None, "model", None),
        P(("data", "stage"), "model", None, None),
        P(("data", "stage"), None, "model"),
        P(("data", "stage"), "model", None),
        P(("data", "stage"), None, None),
    )
    return jax.shard_map(
        device_fn,
        mesh=mesh,
        in_specs=(act_spec, act_spec) + weight_specs,
        out_specs=(P("data"),) + grad_specs,
        check_vma=False,
    )
```

```python
import functools
import math

import jax
import jax.numpy as jnp
from jax import lax
from jax.experimental import pallas as pl
from jax.experimental.pallas import tpu as pltpu
from jax.sharding import PartitionSpec as P

NORM_EPS = 1e-6
NEG_BIG = -1e30
CHUNK = 64
KEY_STEP = 256
GRAD_ROWS = 768
LOG2E = 1.4426950408889634
F32 = jnp.float32
BF16 = jnp.bfloat16
MESH_ID = pl.DeviceIdType.MESH
GELU_A = math.sqrt(2.0 / math.pi)
GELU_B = 0.044715
VMEM_BYTES = 67043328


def dot_nn(a, b):
    return lax.dot_general(a, b, (((1,), (0,)), ((), ())), preferred_element_type=F32)


def dot_nt(a, b):
    return lax.dot_general(a, b, (((1,), (1,)), ((), ())), preferred_element_type=F32)


def dot_tn(a, b):
    return lax.dot_general(a, b, (((0,), (0,)), ((), ())), preferred_element_type=F32)


def rms_inverse(v):
    return lax.rsqrt(jnp.mean(v * v, axis=-1, keepdims=True) + NORM_EPS)


def gelu_tanh(u):
    return u * (0.5 * (1.0 + jnp.tanh(GELU_A * (u + GELU_B * (u * u * u)))))


def gelu_slope(u):
    t = jnp.tanh(GELU_A * (u + GELU_B * (u * u * u)))
    return 0.5 * (1.0 + t) + (0.5 * u) * (1.0 - t * t) * (GELU_A * (1.0 + (3.0 * GELU_B) * (u * u)))


def tile_of(width, top=512):
    for tile in (top, 512, 384, 256, 128):
        if width % tile == 0:
            return tile
    return width


def fold_rows(v):
    total = v[0:8]
    for r in range(8, v.shape[0], 8):
        total = total + v[r : r + 8]
    return total


def step_kernel(cfg, *refs):
    n, t, tq, n_model, n_stage = cfg["n"], cfg["t"], cfg["tq"], cfg["n_model"], cfg["n_stage"]
    seq, d_model, heads, hd, ff = cfg["seq"], cfg["d_model"], cfg["heads"], cfg["hd"], cfg["ff"]
    hw = heads * hd
    elem_count = cfg["elem_count"]
    scale = hd**-0.5
    (
        x_hbm, y_hbm, wqkv_hbm, wout_hbm, wup_hbm, wdown_hbm, gain_ref,
        na_hbm, nb_hbm, at_hbm, z_hbm, dqkv_hbm, dmid_hbm, dup_hbm, dout_hbm, small_ref,
        wqkv, wout, wup, wdown, wqkv_t, wout_t, wup_t, wdown_t, hbuf, nbbuf, doutbuf, dmidbuf, qkvbuf, upbuf, midq, yq, dkacc, dvacc,
        rs_r, rs_s, na_st, z_st, at_st, dup_st, dqkv_st, ds_st, pr_st, hsend, dsend, dmidq,
        lossacc, gacc, lossbuf, fin_s, fin_r,
        w_sem, x_sem, y_sem, h_rsem, h_ssem, d_rsem, d_ssem, rs_rsem, rs_ssem, ag_rsem, ag_ssem,
        out_sem, full_sem, loss_sem, fin_rsem, fin_ssem,
    ) = refs
    me = lax.axis_index("model")
    stage = lax.axis_index("stage")
    last = n_stage - 1
    order = [d for d in (2, 1, 3) if d < n_model] if n_model > 2 else list(range(1, n_model))

    odd = lax.rem(me, 2)
    send_order = [2, 3 - 2 * odd, 1 + 2 * odd] if n_model == 4 else order

    far_first = [2, 3 - 2 * odd, 1 + 2 * odd, 0] if n_model == 4 else list(range(n_model))

    def remote(src, dst, ssem, rsem, where):
        return pltpu.make_async_remote_copy(
            src_ref=src, dst_ref=dst, send_sem=ssem, recv_sem=rsem, device_id=where, device_id_type=MESH_ID
        )

    def rows_of(c):
        return pl.ds(pl.multiple_of(c * t, t), t)

    def quarter(c, m):
        return pl.ds(pl.multiple_of(c * t + m * tq, tq), tq)

    own = pl.ds(pl.multiple_of(me * tq, tq), tq)

    slabs = 3 * heads

    def weight_copy(k):
        if k < slabs:
            return pltpu.make_async_copy(wqkv_hbm.at[k], wqkv.at[:, pl.ds(k * hd, hd)], w_sem.at[k])
        src = (wout_hbm, wup_hbm, wdown_hbm)[k - slabs]
        dst = (wout, wup, wdown)[k - slabs]
        return pltpu.make_async_copy(src, dst, w_sem.at[k])

    def x_copy(k):
        rows = pl.ds(0, t) if k == 0 else pl.ds(t, seq - t)
        return pltpu.make_async_copy(x_hbm.at[rows], hbuf.at[rows], x_sem.at[k])

    def y_copy(c):
        return pltpu.make_async_copy(y_hbm.at[quarter(c, me)], yq.at[pl.ds(c * tq, tq)], y_sem.at[0])

    def y_all():
        return pltpu.make_async_copy(y_hbm.at[pl.ds(0, n * tq)], yq, y_sem.at[0])

    @pl.when(stage == 0)
    def _():
        x_copy(0).start()

    for k in range(slabs + 3):
        weight_copy(k).start()

    @pl.when(stage == 0)
    def _():
        x_copy(1).start()

    @pl.when(stage == last)
    def _():
        for c in range(n):
            y_copy(c).start()

    barrier = pltpu.get_barrier_semaphore()
    up_stage = lax.rem(stage + 1, n_stage)
    down_stage = lax.rem(stage + n_stage - 1, n_stage)
    greet = [{"model": lax.rem(me + d, n_model)} for d in range(1, n_model)]
    greet += [{"stage": up_stage, "model": m} for m in range(n_model)]
    if n_stage > 2:
        greet += [{"stage": down_stage, "model": m} for m in range(n_model)]
    for where in greet:
        pl.semaphore_signal(barrier, inc=1, device_id=where, device_id_type=MESH_ID)

    qkvbuf[:, 2 * hw : 3 * hw] = jnp.zeros((seq, hw), BF16)
    lossacc[...] = jnp.zeros_like(lossacc)
    gacc[...] = jnp.zeros_like(gacc)
    pl.semaphore_wait(barrier, len(greet))

    gains = gain_ref[...].astype(F32)
    gain_a = gains[0:1, :]
    gain_b = gains[1:2, :]

    others = n_model - 1

    def rs_copy(p, c, d, peer):
        slot = lax.rem(c, 2)
        return remote(
            rs_s.at[p, slot, pl.ds(pl.multiple_of(peer * tq, tq), tq)], rs_r.at[p, slot, d - 1],
            rs_ssem.at[p, slot], rs_rsem.at[p, slot], {"model": peer},
        )

    def rs_all(p, c):
        slot = lax.rem(c, 2)
        return remote(rs_r.at[p, slot], rs_r.at[p, slot], rs_ssem.at[p, slot], rs_rsem.at[p, slot], {"model": 0})

    def rs_start(p, c):
        for d in send_order:
            rs_copy(p, c, d, lax.rem(me + d, n_model)).start()

    def rs_drain(p, c):
        rs_all(p, c).wait_send()

    def rs_sum(p, c):
        with jax.named_scope(f"rs_wait{p}"):
            rs_all(p, c).wait_recv()
        total = rs_s[p, lax.rem(c, 2), own, :].astype(F32)
        for d in range(1, n_model):
            total = total + rs_r[p, lax.rem(c, 2), d - 1].astype(F32)
        return total

    def ag_copy(p, buf, c, peer):
        slot = lax.rem(c, 2)
        return remote(
            buf.at[quarter(c, me)], buf.at[quarter(c, me)], ag_ssem.at[p], ag_rsem.at[p, slot], {"model": peer}
        )

    def ag_all(p, buf, c):
        rows = pl.ds(0, others * tq)
        return remote(buf.at[rows], buf.at[rows], ag_ssem.at[p], ag_rsem.at[p, lax.rem(c, 2)], {"model": 0})

    def ag_start(p, buf, c):
        for d in send_order:
            ag_copy(p, buf, c, lax.rem(me + d, n_model)).start()

    def ag_drain(p, buf):
        ag_all(p, buf, 0).wait_send()

    def ag_wait(p, buf, c):
        with jax.named_scope(f"ag_wait{p}"):
            ag_all(p, buf, c).wait_recv()

    def h_copy(c, m):
        return remote(
            hsend, hbuf.at[quarter(c, me)], h_ssem.at[0], h_rsem.at[c], {"stage": up_stage, "model": m}
        )

    def h_all(c):
        return remote(hbuf.at[rows_of(c)], hbuf.at[rows_of(c)], h_ssem.at[0], h_rsem.at[c], {"model": 0})

    def d_copy(c, m):
        return remote(
            dsend, doutbuf.at[quarter(c, me)], d_ssem.at[0], d_rsem.at[c], {"stage": down_stage, "model": m}
        )

    def d_all(c):
        return remote(doutbuf.at[rows_of(c)], doutbuf.at[rows_of(c)], d_ssem.at[0], d_rsem.at[c], {"model": 0})

    def peer_d_copy(c, peer):
        return remote(
            doutbuf.at[quarter(c, me)], doutbuf.at[quarter(c, me)], d_ssem.at[0], d_rsem.at[c], {"model": peer}
        )

    def peer_d_all(c):
        rows = pl.ds(0, others * tq)
        return remote(doutbuf.at[rows], doutbuf.at[rows], d_ssem.at[0], d_rsem.at[c], {"model": 0})

    def staged_out(k, c):
        src = (na_st, z_st, at_st, dup_st, dqkv_st)[k]
        dst = (na_hbm, z_hbm, at_hbm, dup_hbm, dqkv_hbm)[k]
        return pltpu.make_async_copy(src, dst.at[rows_of(c)], out_sem.at[k])

    def full_out(k, c):
        src = (nbbuf, dmidbuf, doutbuf)[k]
        dst = (nb_hbm, dmid_hbm, dout_hbm)[k]
        return pltpu.make_async_copy(src.at[rows_of(c)], dst.at[rows_of(c)], full_sem.at[k])

    def full_all(k):
        return pltpu.make_async_copy((nbbuf, dmidbuf, doutbuf)[k], (nb_hbm, dmid_hbm, dout_hbm)[k], full_sem.at[k])

    key_step = min(KEY_STEP, seq)
    key_block = max(t, 128)

    def by_prefix(c, body):
        need = lax.div(c * t + t - 1, key_step)
        for k in range(seq // key_step):

            @pl.when(need == k)
            def _():
                body((k + 1) * key_step)

    def scores(c, keys):
        return [
            dot_nt(qkvbuf[rows_of(c), i * hd : (i + 1) * hd], qkvbuf[0:keys, hw + i * hd : hw + (i + 1) * hd])
            for i in range(heads)
        ]

    def causal_softmax(c, keys, raw):
        q_pos = c * t + lax.broadcasted_iota(jnp.int32, (t, keys), 0)
        k_pos = lax.broadcasted_iota(jnp.int32, (t, keys), 1)
        s = jnp.where(k_pos <= q_pos, raw, NEG_BIG / scale)
        e = jnp.exp2((s - jnp.max(s, axis=-1, keepdims=True)) * (scale * LOG2E))
        return e * (1.0 / jnp.sum(e, axis=-1, keepdims=True))

    def fwd_attn(c, first):
        @pl.when(first & (stage == 0))
        def _():
            x_copy(0).wait()

        @pl.when((c == 1) & (stage == 0))
        def _():
            x_copy(1).wait()

        @pl.when(stage > 0)
        def _():
            with jax.named_scope("h_wait"):
                h_all(c).wait_recv()

        @pl.when(first & (stage == 0))
        def _():
            for k in range(slabs + 1):
                weight_copy(k).wait()

        @pl.when(jnp.logical_not(first))
        def _():
            staged_out(0, c).wait()
            staged_out(2, c).wait()

        @pl.when(c >= 2)
        def _():
            rs_drain(0, c)

        slot = lax.rem(c, 2)

        h32 = hbuf[rows_of(c), :].astype(F32)
        na_st[...] = (h32 * rms_inverse(h32) * gain_a).astype(BF16)
        staged_out(0, c).start()
        wide = 3 * hw
        tile = tile_of(wide, 384)
        for j in range(wide // tile):
            cols = slice(j * tile, (j + 1) * tile)
            qkvbuf[rows_of(c), cols] = dot_nn(na_st[...], wqkv[:, cols]).astype(BF16)

        def attend(keys):
            probs = [causal_softmax(c, keys, raw).astype(BF16) for raw in scores(c, keys)]
            for i in range(heads):
                v = qkvbuf[0:keys, 2 * hw + i * hd : 2 * hw + (i + 1) * hd]
                at_st[:, i * hd : (i + 1) * hd] = dot_nn(probs[i], v).astype(BF16)

        by_prefix(c, attend)
        staged_out(2, c).start()
        tile = tile_of(d_model)
        for j in range(d_model // tile):
            cols = slice(j * tile, (j + 1) * tile)
            rs_s[0, slot, :, cols] = dot_nn(at_st[...], wout[:, cols]).astype(BF16)
        rs_start(0, c)

    def fwd_mid(c, first):
        @pl.when(jnp.logical_not(first))
        def _():
            ag_drain(0, nbbuf)

        mid = rs_sum(0, c) + hbuf[quarter(c, me), :].astype(F32)
        midq[c] = mid
        nbbuf[quarter(c, me), :] = (mid * rms_inverse(mid) * gain_b).astype(BF16)
        ag_start(0, nbbuf, c)

    def fwd_mlp(c, first):
        @pl.when(first & (stage == 0))
        def _():
            weight_copy(slabs + 1).wait()
            weight_copy(slabs + 2).wait()

        @pl.when(jnp.logical_not(first))
        def _():
            staged_out(1, c).wait()

        @pl.when(c >= 2)
        def _():
            rs_drain(1, c)

        slot = lax.rem(c, 2)

        ag_wait(0, nbbuf, c)
        full_out(0, c).start()
        tile = tile_of(ff)
        for j in range(ff // tile):
            cols = slice(j * tile, (j + 1) * tile)
            u = dot_nn(nbbuf[rows_of(c), :], wup[:, cols])
            upbuf[rows_of(c), cols] = u
            z_st[:, cols] = gelu_tanh(u).astype(BF16)
        staged_out(1, c).start()
        tile = tile_of(d_model)
        for j in range(d_model // tile):
            cols = slice(j * tile, (j + 1) * tile)
            rs_s[1, slot, :, cols] = dot_nn(z_st[...], wdown[:, cols]).astype(BF16)
        rs_start(1, c)

    def fwd_end(c, first):
        h_out = (midq[c] + rs_sum(1, c)).astype(BF16)

        @pl.when(stage < last)
        def _():
            @pl.when(jnp.logical_not(first))
            def _():
                h_all(c).wait_send()

            hsend[...] = h_out
            for d in far_first:
                h_copy(c, lax.rem(me + d, n_model)).start()

        @pl.when(stage == last)
        def _():
            @pl.when(first)
            def _():
                y_all().wait()

            @pl.when(jnp.logical_not(first))
            def _():
                peer_d_all(c).wait_send()

            diff = h_out.astype(F32) - yq[pl.ds(pl.multiple_of(c * tq, tq), tq), :].astype(F32)
            lossacc[...] += fold_rows(diff * diff)
            doutbuf[quarter(c, me), :] = (diff * (1.0 / elem_count)).astype(BF16)
            for d in order:
                peer_d_copy(c, lax.rem(me + d, n_model)).start()

    def pipeline(phases, chunk_of):
        deepest = max(lag for _, lag, _ in phases)

        def body(i, carry):
            for phase, lag, name in phases:
                j = i - lag

                @pl.when((j >= 0) & (j < n))
                def _():
                    with jax.named_scope(name):
                        phase(chunk_of(j), j == 0)

            return carry

        lax.fori_loop(0, n + deepest, body, 0)

    def flip_weights():
        for w, w_t in ((wdown, wdown_t), (wup, wup_t), (wout, wout_t), (wqkv, wqkv_t)):
            depth = tile_of(w.shape[0], 256)
            for r in range(w.shape[0] // depth):
                w_t[:, r * depth : (r + 1) * depth] = w[r * depth : (r + 1) * depth, :].T

    @pl.when(stage > 0)
    def _():
        for k in range(slabs + 3):
            weight_copy(k).wait()
        flip_weights()

    pipeline(
        [(fwd_attn, 0, "fwd_attn"), (fwd_mlp, 1, "fwd_mlp"), (fwd_mid, 0, "fwd_mid"), (fwd_end, 1, "fwd_end")],
        lambda j: j,
    )

    @pl.when(stage == 0)
    def _():
        flip_weights()

    dkacc[...] = jnp.zeros_like(dkacc)
    dvacc[...] = jnp.zeros_like(dvacc)

    for c in range(min(n, 2)):
        rs_drain(0, c)
        rs_drain(1, c)
    ag_drain(0, nbbuf)
    staged_out(0, 0).wait()
    staged_out(1, 0).wait()
    staged_out(2, 0).wait()

    @pl.when(stage < last)
    def _():
        h_all(0).wait_send()

    @pl.when(stage == last)
    def _():
        peer_d_all(0).wait_send()
        total = lossacc[:, 0:128]
        for j in range(1, d_model // 128):
            total = total + lossacc[:, j * 128 : (j + 1) * 128]
        lossbuf[...] = total

    def rms_backward(v, gain, d_norm, k):
        inv = rms_inverse(v)
        normed = v * inv
        gacc[k] += fold_rows(d_norm * normed)
        d_normed = d_norm * gain
        return inv * (d_normed - normed * jnp.mean(d_normed * normed, axis=-1, keepdims=True))

    def bwd_mlp(c, first):
        @pl.when(stage < last)
        def _():
            with jax.named_scope("d_wait"):
                d_all(c).wait_recv()

        @pl.when(stage == last)
        def _():
            peer_d_all(c).wait_recv()

        full_out(2, c).start()

        @pl.when(jnp.logical_not(first))
        def _():
            staged_out(3, c).wait()

        @pl.when(c < n - 2)
        def _():
            rs_drain(2, c)

        slot = lax.rem(c, 2)

        tile = tile_of(ff)
        for j in range(ff // tile):
            cols = slice(j * tile, (j + 1) * tile)
            d_gelu = dot_nn(doutbuf[rows_of(c), :], wdown_t[:, cols])
            dup_st[:, cols] = (d_gelu * gelu_slope(upbuf[rows_of(c), cols])).astype(BF16)
        staged_out(3, c).start()
        tile = tile_of(d_model)
        for j in range(d_model // tile):
            cols = slice(j * tile, (j + 1) * tile)
            rs_s[2, slot, :, cols] = dot_nn(dup_st[...], wup_t[:, cols]).astype(BF16)
        rs_start(2, c)

    def bwd_mid(c, first):
        @pl.when(jnp.logical_not(first))
        def _():
            ag_drain(1, dmidbuf)

        d_norm = rs_sum(2, c)
        d_mid = doutbuf[quarter(c, me), :].astype(F32) + rms_backward(midq[c], gain_b, d_norm, 1)
        dmidq[lax.rem(c, 4)] = d_mid
        dmidbuf[quarter(c, me), :] = d_mid.astype(BF16)
        ag_start(1, dmidbuf, c)

    def bwd_attn(c, first):
        ag_wait(1, dmidbuf, c)
        full_out(1, c).start()

        @pl.when(jnp.logical_not(first))
        def _():
            staged_out(4, c).wait()

        @pl.when((c < n - 2) & (stage > 0))
        def _():
            rs_drain(3, c)

        slot = lax.rem(c, 2)

        d_attn = dot_nn(dmidbuf[rows_of(c), :], wout_t[...]).astype(BF16)
        at_st[...] = d_attn

        def attend(keys):
            raws = scores(c, keys)
            d_probs = [
                dot_nt(at_st[:, i * hd : (i + 1) * hd], qkvbuf[0:keys, 2 * hw + i * hd : 2 * hw + (i + 1) * hd])
                for i in range(heads)
            ]
            probs, d_scores = [], []
            for raw, dp in zip(raws, d_probs):
                p = causal_softmax(c, keys, raw)
                probs.append(p.astype(BF16))
                d_scores.append((p * (dp - jnp.sum(p * dp, axis=-1, keepdims=True)) * scale).astype(BF16))
            for i in range(heads):
                cols = slice(i * hd, (i + 1) * hd)
                ds_st[i, :, 0:keys] = d_scores[i]
                pr_st[i, :, 0:keys] = probs[i]
                dqkv_st[:, cols] = dot_nn(d_scores[i], qkvbuf[0:keys, hw + i * hd : hw + (i + 1) * hd]).astype(BF16)

        by_prefix(c, attend)
        near_keys = pl.ds(pl.multiple_of(lax.div(c * t, key_block) * key_block, key_block), key_block)
        for i in range(heads):
            cols = slice(i * hd, (i + 1) * hd)
            dkacc[near_keys, cols] += dot_tn(ds_st[i, :, near_keys], qkvbuf[rows_of(c), cols])
            dvacc[near_keys, cols] += dot_tn(pr_st[i, :, near_keys], at_st[:, cols])
        dqkv_st[:, hw : 2 * hw] = dkacc[rows_of(c), :].astype(BF16)
        dqkv_st[:, 2 * hw : 3 * hw] = dvacc[rows_of(c), :].astype(BF16)
        staged_out(4, c).start()
        tile = tile_of(d_model)

        @pl.when(stage > 0)
        def _():
            for j in range(d_model // tile):
                cols = slice(j * tile, (j + 1) * tile)
                rs_s[3, slot, :, cols] = dot_nn(dqkv_st[...], wqkv_t[:, cols]).astype(BF16)
            rs_start(3, c)

        @pl.when(stage == 0)
        def _():
            h32 = hbuf[rows_of(c), :].astype(F32)
            normed = h32 * rms_inverse(h32)
            for j in range(d_model // tile):
                cols = slice(j * tile, (j + 1) * tile)
                gacc[0, :, cols] += fold_rows(dot_nn(dqkv_st[...], wqkv_t[:, cols]) * normed[:, cols])

        def older(keys):
            for i in range(heads):
                cols = slice(i * hd, (i + 1) * hd)
                ds_st[i, :, near_keys] = jnp.zeros((t, key_block), BF16)
                pr_st[i, :, near_keys] = jnp.zeros((t, key_block), BF16)
            for i in range(heads):
                cols = slice(i * hd, (i + 1) * hd)
                dkacc[0:keys, cols] += dot_tn(ds_st[i, :, 0:keys], qkvbuf[rows_of(c), cols])
                dvacc[0:keys, cols] += dot_tn(pr_st[i, :, 0:keys], at_st[:, cols])

        by_prefix(c, older)

    def loss_copy():
        return remote(lossbuf, lossbuf, loss_sem.at[0], loss_sem.at[1], {"stage": down_stage})

    def bwd_end(c, first):
        @pl.when(stage > 0)
        def _():
            h32 = hbuf[quarter(c, me), :].astype(F32)
            d_in = dmidq[lax.rem(c, 4)] + rms_backward(h32, gain_a, rs_sum(3, c), 0)

            @pl.when(jnp.logical_not(first))
            def _():
                d_all(c).wait_send()

            dsend[...] = d_in.astype(BF16)
            for d in far_first:
                d_copy(c, lax.rem(me + d, n_model)).start()

        @pl.when(first)
        def _():
            @pl.when(stage < last)
            def _():
                loss_copy().wait_recv()

            @pl.when(stage > 0)
            def _():
                loss_copy().start()

    pipeline(
        [(bwd_mlp, 0, "bwd_mlp"), (bwd_attn, 1, "bwd_attn"), (bwd_mid, 0, "bwd_mid"), (bwd_end, 1, "bwd_end")],
        lambda j: n - 1 - j,
    )

    fin_s[...] = jnp.zeros_like(fin_s)
    fin_s[0:1, :] = jnp.sum(gacc[0], axis=0, keepdims=True)
    fin_s[1:2, :] = jnp.sum(gacc[1], axis=0, keepdims=True)
    fin_s[2:3, 0:128] = jnp.sum(lossbuf[...], axis=0, keepdims=True)

    def fin_copy(d, peer):
        return remote(fin_s, fin_r.at[d - 1], fin_ssem.at[0], fin_rsem.at[0], {"model": peer})

    for d in order:
        fin_copy(d, lax.rem(me + d, n_model)).start()

    for c in range(min(n, 2)):
        rs_drain(2, c)
    ag_drain(1, dmidbuf)
    staged_out(3, 0).wait()
    staged_out(4, 0).wait()
    for k in range(3):
        full_all(k).wait()

    @pl.when(stage > 0)
    def _():
        for c in range(min(n, 2)):
            rs_drain(3, c)
        d_all(0).wait_send()
        loss_copy().wait_send()

    fin_all = remote(fin_r, fin_r, fin_ssem.at[0], fin_rsem.at[0], {"model": 0})
    fin_all.wait_recv()
    parts = [jnp.where(me == 0, fin_s[...], 0.0)]
    for m in range(n_model):
        term = jnp.where(me == m, fin_s[...], 0.0)
        for d in range(1, n_model):
            term = term + jnp.where(lax.rem(m + d, n_model) == me, fin_r[d - 1], 0.0)
        parts.append(term)
    total = parts[1]
    for m in range(1, n_model):
        total = total + parts[m + 1]
    small_ref[0:2, :] = total[0:2, :]
    loss = jnp.sum(total[2:3, :], axis=-1, keepdims=True) * (0.5 / elem_count)
    small_ref[2:8, :] = jnp.broadcast_to(loss, (6, d_model))
    fin_all.wait_send()


def run_step(cfg, x, y, wqkv, wout, wup, wdown, gain):
    n, t, tq, n_model, seq = cfg["n"], cfg["t"], cfg["tq"], cfg["n_model"], cfg["seq"]
    d_model, ff, hw = cfg["d_model"], cfg["ff"], cfg["heads"] * cfg["hd"]
    dma = pltpu.SemaphoreType.DMA
    near = max(n_model - 1, 1)
    act = lambda width: jax.ShapeDtypeStruct((seq, width), BF16)
    any_spec = pl.BlockSpec(memory_space=pl.ANY)
    vmem_spec = pl.BlockSpec(memory_space=pltpu.VMEM)
    scratch = [
        pltpu.VMEM((d_model, 3 * hw), BF16),
        pltpu.VMEM((hw, d_model), BF16),
        pltpu.VMEM((d_model, ff), BF16),
        pltpu.VMEM((ff, d_model), BF16),
        pltpu.VMEM((3 * hw, d_model), BF16),
        pltpu.VMEM((d_model, hw), BF16),
        pltpu.VMEM((ff, d_model), BF16),
        pltpu.VMEM((d_model, ff), BF16),
        pltpu.VMEM((seq, d_model), BF16),
        pltpu.VMEM((seq, d_model), BF16),
        pltpu.VMEM((seq, d_model), BF16),
        pltpu.VMEM((seq, d_model), BF16),
        pltpu.VMEM((seq, 3 * hw), BF16),
        pltpu.VMEM((seq, ff), F32),
        pltpu.VMEM((n, tq, d_model), F32),
        pltpu.VMEM((n * tq, d_model), BF16),
        pltpu.VMEM((seq, hw), F32),
        pltpu.VMEM((seq, hw), F32),
        pltpu.VMEM((4, 2, near, tq, d_model), BF16),
        pltpu.VMEM((4, 2, t, d_model), BF16),
        pltpu.VMEM((t, d_model), BF16),
        pltpu.VMEM((t, ff), BF16),
        pltpu.VMEM((t, hw), BF16),
        pltpu.VMEM((t, ff), BF16),
        pltpu.VMEM((t, 3 * hw), BF16),
        pltpu.VMEM((cfg["heads"], t, seq), BF16),
        pltpu.VMEM((cfg["heads"], t, seq), BF16),
        pltpu.VMEM((tq, d_model), BF16),
        pltpu.VMEM((tq, d_model), BF16),
        pltpu.VMEM((4, tq, d_model), F32),
        pltpu.VMEM((8, d_model), F32),
        pltpu.VMEM((2, 8, d_model), F32),
        pltpu.VMEM((8, 128), F32),
        pltpu.VMEM((8, d_model), F32),
        pltpu.VMEM((near, 8, d_model), F32),
        dma((3 * cfg["heads"] + 3,)),
        dma((2,)),
        dma((1,)),
        dma((n,)),
        dma((1,)),
        dma((n,)),
        dma((1,)),
        dma((4, 2)),
        dma((4, 2)),
        dma((2, 2)),
        dma((2,)),
        dma((5,)),
        dma((3,)),
        dma((2,)),
        dma((1,)),
        dma((1,)),
    ]
    return pl.pallas_call(
        functools.partial(step_kernel, cfg),
        name="pipeline_step",
        out_shape=(
            act(d_model), act(d_model), act(hw), act(ff), act(3 * hw), act(d_model), act(ff), act(d_model),
            jax.ShapeDtypeStruct((8, d_model), F32),
        ),
        in_specs=[any_spec] * 6 + [vmem_spec],
        out_specs=[any_spec] * 8 + [vmem_spec],
        scratch_shapes=scratch,
        compiler_params=pltpu.CompilerParams(
            collective_id=0, has_side_effects=True, vmem_limit_bytes=VMEM_BYTES
        ),
    )(x, y, wqkv, wout, wup, wdown, gain)


def grads_kernel(nj, bm, *refs):
    ins, small = refs[: 2 * nj], refs[2 * nj]
    outs, loss_ref, gain_ref = refs[2 * nj + 1 : 3 * nj + 1], refs[3 * nj + 1], refs[3 * nj + 2]
    scratch = refs[3 * nj + 3 :]
    bufs, stages, in_sem, out_sem = scratch[: 2 * nj], scratch[2 * nj : 3 * nj], scratch[-2], scratch[-1]

    def load(k):
        return pltpu.make_async_copy(ins[k], bufs[k], in_sem.at[k])

    for k in range(2 * nj):
        load(k).start()
    loss_ref[...] = small[2:3, 0:1]
    gain_ref[...] = small[0:2, :]
    for j in range(nj):
        load(2 * j).wait()
        load(2 * j + 1).wait()
        a, b, out, stage = bufs[2 * j], bufs[2 * j + 1], outs[j], stages[j]
        rows = a.shape[1]
        step = min(bm, rows)
        blocks = rows // step

        def put(i, slot):
            where = pl.ds(pl.multiple_of(i * step, step), step)
            dst = out.at[:, where] if len(out.shape) == 3 else out.at[where]
            return pltpu.make_async_copy(stage.at[slot], dst, out_sem.at[j, slot])

        def block(i, carry):
            slot = lax.rem(i, 2)

            @pl.when(i >= 2)
            def _():
                put(i, slot).wait()

            acc = dot_tn(a[:, pl.ds(pl.multiple_of(i * step, step), step)], b[...])
            if len(out.shape) == 3:
                lanes = out.shape[2]
                for s in range(out.shape[0]):
                    stage[slot, s] = acc[:, s * lanes : (s + 1) * lanes]
            else:
                stage[slot] = acc
            put(i, slot).start()
            return carry

        lax.fori_loop(0, blocks, block, 0)
    for j in range(nj):
        rows = bufs[2 * j].shape[1]
        step = min(bm, rows)
        for slot in range(min(2, rows // step)):
            out, stage = outs[j], stages[j]
            dst = out.at[:, 0:step] if len(out.shape) == 3 else out.at[0:step]
            pltpu.make_async_copy(stage.at[slot], dst, out_sem.at[j, slot]).wait()


def weight_grads(pairs, out_shapes, small, bm):
    nj = len(pairs)
    flat = [x for pair in pairs for x in pair]
    any_spec = pl.BlockSpec(memory_space=pl.ANY)
    vmem_spec = pl.BlockSpec(memory_space=pltpu.VMEM)
    stages = []
    for (a, _), out in zip(pairs, out_shapes):
        step = min(bm, a.shape[1])
        stages.append(pltpu.VMEM((2,) + out[:-2] + (step, out[-1]), F32))
    outs = [jax.ShapeDtypeStruct(out, F32) for out in out_shapes]
    outs += [jax.ShapeDtypeStruct((1, 1), F32), jax.ShapeDtypeStruct((2, small.shape[1]), F32)]
    return pl.pallas_call(
        functools.partial(grads_kernel, nj, bm),
        name="weight_grads",
        out_shape=outs,
        in_specs=[any_spec] * (2 * nj) + [vmem_spec],
        out_specs=[any_spec] * nj + [vmem_spec] * 2,
        scratch_shapes=[pltpu.VMEM(x.shape, x.dtype) for x in flat]
        + stages
        + [pltpu.SemaphoreType.DMA((2 * nj,)), pltpu.SemaphoreType.DMA((nj, 2))],
        compiler_params=pltpu.CompilerParams(vmem_limit_bytes=VMEM_BYTES),
    )(*flat, small)


def solution(mesh):
    n_stage = mesh.shape["stage"]
    n_model = mesh.shape["model"]

    def device_fn(x_in, y_target, w_qkv, w_out, w_up, w_down, norm_gain):
        n_batch, seq_len, d_model = x_in.shape
        heads, hd, ff = w_qkv.shape[3], w_qkv.shape[4], w_up.shape[2]
        t = min(CHUNK, seq_len)
        cfg = dict(
            n=seq_len // t, t=t, tq=t // n_model, n_model=n_model, n_stage=n_stage, seq=seq_len, d_model=d_model,
            heads=heads, hd=hd, ff=ff, elem_count=n_batch * seq_len * d_model,
        )
        na, nb, at, z, dqkv, dmid, dup, dout, small = run_step(
            cfg, x_in[0], y_target[0], w_qkv[0].transpose(1, 2, 0, 3).reshape(3 * heads, d_model, hd), w_out[0].reshape(heads * hd, d_model),
            w_up[0], w_down[0], norm_gain[0],
        )
        g_out, g_up, g_down, g_qkv, loss, g_gain = weight_grads(
            [(at, dmid), (nb, dup), (z, dout), (na, dqkv)],
            [(heads * hd, d_model), (d_model, ff), (ff, d_model), (3 * heads, d_model, hd)],
            small,
            tile_of(d_model, GRAD_ROWS),
        )
        grad_qkv = g_qkv.reshape(3, heads, d_model, hd).transpose(2, 0, 1, 3)[None]
        return loss.reshape(1), grad_qkv, g_out.reshape(1, heads, hd, d_model), g_up[None], g_down[None], g_gain[None]

    act_spec = P("data", None, None)
    weight_specs = (
        P("stage", None, None, "model", None),
        P("stage", "model", None, None),
        P("stage", None, "model"),
        P("stage", "model", None),
        P("stage", None, None),
    )
    grad_specs = (
        P(("data", "stage"), None, None, "model", None),
        P(("data", "stage"), "model", None, None),
        P(("data", "stage"), None, "model"),
        P(("data", "stage"), "model", None),
        P(("data", "stage"), None, None),
    )
    return jax.shard_map(
        device_fn,
        mesh=mesh,
        in_specs=(act_spec, act_spec) + weight_specs,
        out_specs=(P("data"),) + grad_specs,
        check_vma=False,
    )
```

```python
import functools
import math

import jax
import jax.numpy as jnp
from jax import lax
from jax.experimental import pallas as pl
from jax.experimental.pallas import tpu as pltpu
from jax.sharding import PartitionSpec as P

NORM_EPS = 1e-6
NEG_BIG = -1e30
CHUNK = 64
KEY_STEP = 256
GRAD_ROWS = 768
LOG2E = 1.4426950408889634
F32 = jnp.float32
BF16 = jnp.bfloat16
MESH_ID = pl.DeviceIdType.MESH
GELU_A = math.sqrt(2.0 / math.pi)
GELU_B = 0.044715
VMEM_BYTES = 67043328


def dot_nn(a, b):
    return lax.dot_general(a, b, (((1,), (0,)), ((), ())), preferred_element_type=F32)


def dot_nt(a, b):
    return lax.dot_general(a, b, (((1,), (1,)), ((), ())), preferred_element_type=F32)


def dot_tn(a, b):
    return lax.dot_general(a, b, (((0,), (0,)), ((), ())), preferred_element_type=F32)


def rms_inverse(v):
    return lax.rsqrt(jnp.mean(v * v, axis=-1, keepdims=True) + NORM_EPS)


def gelu_tanh(u):
    return u * (0.5 * (1.0 + jnp.tanh(GELU_A * (u + GELU_B * (u * u * u)))))


def gelu_slope(u):
    t = jnp.tanh(GELU_A * (u + GELU_B * (u * u * u)))
    return 0.5 * (1.0 + t) + (0.5 * u) * (1.0 - t * t) * (GELU_A * (1.0 + (3.0 * GELU_B) * (u * u)))


def tile_of(width, top=512):
    for tile in (top, 512, 384, 256, 128):
        if width % tile == 0:
            return tile
    return width


def fold_rows(v):
    total = v[0:8]
    for r in range(8, v.shape[0], 8):
        total = total + v[r : r + 8]
    return total


def step_kernel(cfg, *refs):
    n, t, tq, n_model, n_stage = cfg["n"], cfg["t"], cfg["tq"], cfg["n_model"], cfg["n_stage"]
    seq, d_model, heads, hd, ff = cfg["seq"], cfg["d_model"], cfg["heads"], cfg["hd"], cfg["ff"]
    hw = heads * hd
    elem_count = cfg["elem_count"]
    scale = hd**-0.5
    (
        x_hbm, y_hbm, wqkv_hbm, wout_hbm, wup_hbm, wdown_hbm, gain_ref,
        na_hbm, nb_hbm, at_hbm, z_hbm, dqkv_hbm, dmid_hbm, dup_hbm, dout_hbm, small_hbm,
        wqkv, wout, wup, wdown, wqkv_t, wout_t, wup_t, wdown_t, hbuf, nbbuf, doutbuf, dmidbuf, qkvbuf, upbuf, midq, yq, dkacc, dvacc,
        rs_r, rs_s, na_st, z_st, at_st, dup_st, dqkv_st, ds_st, pr_st, hsend, dsend, dmidq,
        lossacc, gacc, lossbuf, fin_s, fin_r,
        w_sem, x_sem, y_sem, h_rsem, h_ssem, d_rsem, d_ssem, rs_rsem, rs_ssem, ag_rsem, ag_ssem,
        out_sem, full_sem, loss_sem, fin_rsem, fin_ssem,
    ) = refs
    me = lax.axis_index("model")
    stage = lax.axis_index("stage")
    last = n_stage - 1
    order = [d for d in (2, 1, 3) if d < n_model] if n_model > 2 else list(range(1, n_model))

    odd = lax.rem(me, 2)
    send_order = [2, 3 - 2 * odd, 1 + 2 * odd] if n_model == 4 else order

    far_first = [2, 3 - 2 * odd, 1 + 2 * odd, 0] if n_model == 4 else list(range(n_model))

    def remote(src, dst, ssem, rsem, where):
        return pltpu.make_async_remote_copy(
            src_ref=src, dst_ref=dst, send_sem=ssem, recv_sem=rsem, device_id=where, device_id_type=MESH_ID
        )

    def rows_of(c):
        return pl.ds(pl.multiple_of(c * t, t), t)

    def quarter(c, m):
        return pl.ds(pl.multiple_of(c * t + m * tq, tq), tq)

    own = pl.ds(pl.multiple_of(me * tq, tq), tq)

    slabs = 3 * heads

    def weight_copy(k):
        if k < slabs:
            return pltpu.make_async_copy(wqkv_hbm.at[k], wqkv.at[:, pl.ds(k * hd, hd)], w_sem.at[k])
        src = (wout_hbm, wup_hbm, wdown_hbm)[k - slabs]
        dst = (wout, wup, wdown)[k - slabs]
        return pltpu.make_async_copy(src, dst, w_sem.at[k])

    def x_copy(k):
        rows = pl.ds(0, t) if k == 0 else pl.ds(t, seq - t)
        return pltpu.make_async_copy(x_hbm.at[rows], hbuf.at[rows], x_sem.at[k])

    def y_copy(c):
        return pltpu.make_async_copy(y_hbm.at[quarter(c, me)], yq.at[pl.ds(c * tq, tq)], y_sem.at[0])

    def y_all():
        return pltpu.make_async_copy(y_hbm.at[pl.ds(0, n * tq)], yq, y_sem.at[0])

    @pl.when(stage == 0)
    def _():
        x_copy(0).start()

    for k in range(slabs + 3):
        weight_copy(k).start()

    @pl.when(stage == 0)
    def _():
        x_copy(1).start()

    @pl.when(stage == last)
    def _():
        for c in range(n):
            y_copy(c).start()

    barrier = pltpu.get_barrier_semaphore()
    up_stage = lax.rem(stage + 1, n_stage)
    down_stage = lax.rem(stage + n_stage - 1, n_stage)
    greet = [{"model": lax.rem(me + d, n_model)} for d in range(1, n_model)]
    greet += [{"stage": up_stage, "model": m} for m in range(n_model)]
    if n_stage > 2:
        greet += [{"stage": down_stage, "model": m} for m in range(n_model)]
    for where in greet:
        pl.semaphore_signal(barrier, inc=1, device_id=where, device_id_type=MESH_ID)

    qkvbuf[:, 2 * hw : 3 * hw] = jnp.zeros((seq, hw), BF16)
    lossacc[...] = jnp.zeros_like(lossacc)
    gacc[...] = jnp.zeros_like(gacc)
    pl.semaphore_wait(barrier, len(greet))

    gains = gain_ref[...].astype(F32)
    gain_a = gains[0:1, :]
    gain_b = gains[1:2, :]

    others = n_model - 1

    def rs_copy(p, c, d, peer):
        slot = lax.rem(c, 2)
        return remote(
            rs_s.at[p, slot, pl.ds(pl.multiple_of(peer * tq, tq), tq)], rs_r.at[p, slot, d - 1],
            rs_ssem.at[p, slot], rs_rsem.at[p, slot], {"model": peer},
        )

    def rs_all(p, c):
        slot = lax.rem(c, 2)
        return remote(rs_r.at[p, slot], rs_r.at[p, slot], rs_ssem.at[p, slot], rs_rsem.at[p, slot], {"model": 0})

    def rs_start(p, c):
        for d in send_order:
            rs_copy(p, c, d, lax.rem(me + d, n_model)).start()

    def rs_drain(p, c):
        rs_all(p, c).wait_send()

    def rs_sum(p, c):
        with jax.named_scope(f"rs_wait{p}"):
            rs_all(p, c).wait_recv()
        total = rs_s[p, lax.rem(c, 2), own, :].astype(F32)
        for d in range(1, n_model):
            total = total + rs_r[p, lax.rem(c, 2), d - 1].astype(F32)
        return total

    def ag_copy(p, buf, c, peer):
        slot = lax.rem(c, 2)
        return remote(
            buf.at[quarter(c, me)], buf.at[quarter(c, me)], ag_ssem.at[p], ag_rsem.at[p, slot], {"model": peer}
        )

    def ag_all(p, buf, c):
        rows = pl.ds(0, others * tq)
        return remote(buf.at[rows], buf.at[rows], ag_ssem.at[p], ag_rsem.at[p, lax.rem(c, 2)], {"model": 0})

    def ag_start(p, buf, c):
        for d in send_order:
            ag_copy(p, buf, c, lax.rem(me + d, n_model)).start()

    def ag_drain(p, buf):
        ag_all(p, buf, 0).wait_send()

    def ag_wait(p, buf, c):
        with jax.named_scope(f"ag_wait{p}"):
            ag_all(p, buf, c).wait_recv()

    def h_copy(c, m):
        return remote(
            hsend, hbuf.at[quarter(c, me)], h_ssem.at[0], h_rsem.at[c], {"stage": up_stage, "model": m}
        )

    def h_all(c):
        return remote(hbuf.at[rows_of(c)], hbuf.at[rows_of(c)], h_ssem.at[0], h_rsem.at[c], {"model": 0})

    def d_copy(c, m):
        return remote(
            dsend, doutbuf.at[quarter(c, me)], d_ssem.at[0], d_rsem.at[c], {"stage": down_stage, "model": m}
        )

    def d_all(c):
        return remote(doutbuf.at[rows_of(c)], doutbuf.at[rows_of(c)], d_ssem.at[0], d_rsem.at[c], {"model": 0})

    def peer_d_copy(c, peer):
        return remote(
            doutbuf.at[quarter(c, me)], doutbuf.at[quarter(c, me)], d_ssem.at[0], d_rsem.at[c], {"model": peer}
        )

    def peer_d_all(c):
        rows = pl.ds(0, others * tq)
        return remote(doutbuf.at[rows], doutbuf.at[rows], d_ssem.at[0], d_rsem.at[c], {"model": 0})

    def staged_out(k, c):
        src = (na_st, z_st, at_st, dup_st, dqkv_st)[k]
        dst = (na_hbm, z_hbm, at_hbm, dup_hbm, dqkv_hbm)[k]
        return pltpu.make_async_copy(src, dst.at[rows_of(c)], out_sem.at[k])

    def full_out(k, c):
        src = (nbbuf, dmidbuf, doutbuf)[k]
        dst = (nb_hbm, dmid_hbm, dout_hbm)[k]
        return pltpu.make_async_copy(src.at[rows_of(c)], dst.at[rows_of(c)], full_sem.at[k])

    def full_all(k):
        return pltpu.make_async_copy((nbbuf, dmidbuf, doutbuf)[k], (nb_hbm, dmid_hbm, dout_hbm)[k], full_sem.at[k])

    key_step = min(KEY_STEP, seq)
    key_block = max(t, 128)

    def by_prefix(c, body):
        need = lax.div(c * t + t - 1, key_step)
        for k in range(seq // key_step):

            @pl.when(need == k)
            def _():
                body((k + 1) * key_step)

    def scores(c, keys):
        return [
            dot_nt(qkvbuf[rows_of(c), i * hd : (i + 1) * hd], qkvbuf[0:keys, hw + i * hd : hw + (i + 1) * hd])
            for i in range(heads)
        ]

    def causal_softmax(c, keys, raw):
        q_pos = c * t + lax.broadcasted_iota(jnp.int32, (t, keys), 0)
        k_pos = lax.broadcasted_iota(jnp.int32, (t, keys), 1)
        s = jnp.where(k_pos <= q_pos, raw, NEG_BIG / scale)
        e = jnp.exp2((s - jnp.max(s, axis=-1, keepdims=True)) * (scale * LOG2E))
        return e * (1.0 / jnp.sum(e, axis=-1, keepdims=True))

    def fwd_attn(c, first):
        @pl.when(first & (stage == 0))
        def _():
            x_copy(0).wait()

        @pl.when((c == 1) & (stage == 0))
        def _():
            x_copy(1).wait()

        @pl.when(stage > 0)
        def _():
            with jax.named_scope("h_wait"):
                h_all(c).wait_recv()

        @pl.when(first & (stage == 0))
        def _():
            for k in range(slabs + 1):
                weight_copy(k).wait()

        @pl.when(jnp.logical_not(first))
        def _():
            staged_out(0, c).wait()
            staged_out(2, c).wait()

        @pl.when(c >= 2)
        def _():
            rs_drain(0, c)

        slot = lax.rem(c, 2)

        h32 = hbuf[rows_of(c), :].astype(F32)
        na_st[...] = (h32 * rms_inverse(h32) * gain_a).astype(BF16)
        staged_out(0, c).start()
        wide = 3 * hw
        tile = tile_of(wide, 384)
        for j in range(wide // tile):
            cols = slice(j * tile, (j + 1) * tile)
            qkvbuf[rows_of(c), cols] = dot_nn(na_st[...], wqkv[:, cols]).astype(BF16)

        def attend(keys):
            probs = [causal_softmax(c, keys, raw).astype(BF16) for raw in scores(c, keys)]
            for i in range(heads):
                v = qkvbuf[0:keys, 2 * hw + i * hd : 2 * hw + (i + 1) * hd]
                at_st[:, i * hd : (i + 1) * hd] = dot_nn(probs[i], v).astype(BF16)

        by_prefix(c, attend)
        staged_out(2, c).start()
        tile = tile_of(d_model)
        for j in range(d_model // tile):
            cols = slice(j * tile, (j + 1) * tile)
            rs_s[0, slot, :, cols] = dot_nn(at_st[...], wout[:, cols]).astype(BF16)
        rs_start(0, c)

    def fwd_mid(c, first):
        @pl.when(jnp.logical_not(first))
        def _():
            ag_drain(0, nbbuf)

        mid = rs_sum(0, c) + hbuf[quarter(c, me), :].astype(F32)
        midq[c] = mid
        nbbuf[quarter(c, me), :] = (mid * rms_inverse(mid) * gain_b).astype(BF16)
        ag_start(0, nbbuf, c)

    def fwd_mlp(c, first):
        @pl.when(first & (stage == 0))
        def _():
            weight_copy(slabs + 1).wait()
            weight_copy(slabs + 2).wait()

        @pl.when(jnp.logical_not(first))
        def _():
            staged_out(1, c).wait()

        @pl.when(c >= 2)
        def _():
            rs_drain(1, c)

        slot = lax.rem(c, 2)

        ag_wait(0, nbbuf, c)
        full_out(0, c).start()
        tile = tile_of(ff)
        for j in range(ff // tile):
            cols = slice(j * tile, (j + 1) * tile)
            u = dot_nn(nbbuf[rows_of(c), :], wup[:, cols])
            upbuf[rows_of(c), cols] = u
            z_st[:, cols] = gelu_tanh(u).astype(BF16)
        staged_out(1, c).start()
        tile = tile_of(d_model)
        for j in range(d_model // tile):
            cols = slice(j * tile, (j + 1) * tile)
            rs_s[1, slot, :, cols] = dot_nn(z_st[...], wdown[:, cols]).astype(BF16)
        rs_start(1, c)

    def fwd_end(c, first):
        h_out = (midq[c] + rs_sum(1, c)).astype(BF16)

        @pl.when(stage < last)
        def _():
            @pl.when(jnp.logical_not(first))
            def _():
                h_all(c).wait_send()

            hsend[...] = h_out
            for d in far_first:
                h_copy(c, lax.rem(me + d, n_model)).start()

        @pl.when(stage == last)
        def _():
            @pl.when(first)
            def _():
                y_all().wait()

            @pl.when(jnp.logical_not(first))
            def _():
                peer_d_all(c).wait_send()

            diff = h_out.astype(F32) - yq[pl.ds(pl.multiple_of(c * tq, tq), tq), :].astype(F32)
            lossacc[...] += fold_rows(diff * diff)
            doutbuf[quarter(c, me), :] = (diff * (1.0 / elem_count)).astype(BF16)
            for d in order:
                peer_d_copy(c, lax.rem(me + d, n_model)).start()

    def pipeline(phases, chunk_of):
        deepest = max(p[1] for p in phases)

        def body(i, carry):
            for phase, lag, name, *cond in phases:
                j = i - lag
                ok = (j >= 0) & (j < n)
                if cond:
                    ok = ok & cond[0]

                @pl.when(ok)
                def _():
                    with jax.named_scope(name):
                        phase(chunk_of(j), j == 0)

            return carry

        lax.fori_loop(0, n + deepest, body, 0)

    def flip_weights():
        for w, w_t in ((wdown, wdown_t), (wup, wup_t), (wout, wout_t), (wqkv, wqkv_t)):
            depth = tile_of(w.shape[0], 256)
            for r in range(w.shape[0] // depth):
                w_t[:, r * depth : (r + 1) * depth] = w[r * depth : (r + 1) * depth, :].T

    @pl.when(stage > 0)
    def _():
        for k in range(slabs + 3):
            weight_copy(k).wait()
        flip_weights()

    pipeline(
        [(fwd_attn, 0, "fwd_attn"), (fwd_end, 2, "fwd_end", lax.rem(stage, 2) == 0), (fwd_mlp, 1, "fwd_mlp"), (fwd_mid, 0, "fwd_mid"), (fwd_end, 1, "fwd_end", lax.rem(stage, 2) == 1)],
        lambda j: j,
    )

    @pl.when(stage == 0)
    def _():
        flip_weights()

    dkacc[...] = jnp.zeros_like(dkacc)
    dvacc[...] = jnp.zeros_like(dvacc)

    for c in range(min(n, 2)):
        rs_drain(0, c)
        rs_drain(1, c)
    ag_drain(0, nbbuf)
    staged_out(0, 0).wait()
    staged_out(1, 0).wait()
    staged_out(2, 0).wait()

    @pl.when(stage < last)
    def _():
        h_all(0).wait_send()

    @pl.when(stage == last)
    def _():
        peer_d_all(0).wait_send()
        total = lossacc[:, 0:128]
        for j in range(1, d_model // 128):
            total = total + lossacc[:, j * 128 : (j + 1) * 128]
        lossbuf[...] = total

    def rms_backward(v, gain, k, d_norm_of):
        inv = rms_inverse(v)
        normed = v * inv
        scaled = gain * inv
        d_norm = d_norm_of()
        gacc[k] += fold_rows(d_norm * normed)
        d_normed = d_norm * gain
        return d_norm * scaled - normed * (inv * jnp.mean(d_normed * normed, axis=-1, keepdims=True))

    def bwd_mlp(c, first):
        @pl.when(stage < last)
        def _():
            with jax.named_scope("d_wait"):
                d_all(c).wait_recv()

        @pl.when(stage == last)
        def _():
            peer_d_all(c).wait_recv()

        full_out(2, c).start()

        @pl.when(jnp.logical_not(first))
        def _():
            staged_out(3, c).wait()

        @pl.when(c < n - 2)
        def _():
            rs_drain(2, c)

        slot = lax.rem(c, 2)

        tile = tile_of(ff)
        for j in range(ff // tile):
            cols = slice(j * tile, (j + 1) * tile)
            d_gelu = dot_nn(doutbuf[rows_of(c), :], wdown_t[:, cols])
            dup_st[:, cols] = (d_gelu * gelu_slope(upbuf[rows_of(c), cols])).astype(BF16)
        staged_out(3, c).start()
        tile = tile_of(d_model)
        for j in range(d_model // tile):
            cols = slice(j * tile, (j + 1) * tile)
            rs_s[2, slot, :, cols] = dot_nn(dup_st[...], wup_t[:, cols]).astype(BF16)
        rs_start(2, c)

    def bwd_mid(c, first):
        @pl.when(jnp.logical_not(first))
        def _():
            ag_drain(1, dmidbuf)

        d_out = doutbuf[quarter(c, me), :].astype(F32)
        d_mid = d_out + rms_backward(midq[c], gain_b, 1, lambda: rs_sum(2, c))
        dmidq[lax.rem(c, 4)] = d_mid
        dmidbuf[quarter(c, me), :] = d_mid.astype(BF16)
        ag_start(1, dmidbuf, c)

    def bwd_attn(c, first):
        ag_wait(1, dmidbuf, c)
        full_out(1, c).start()

        @pl.when(jnp.logical_not(first))
        def _():
            staged_out(4, c).wait()

        @pl.when((c < n - 2) & (stage > 0))
        def _():
            rs_drain(3, c)

        slot = lax.rem(c, 2)

        d_attn = dot_nn(dmidbuf[rows_of(c), :], wout_t[...]).astype(BF16)
        at_st[...] = d_attn

        def attend(keys):
            raws = scores(c, keys)
            d_probs = [
                dot_nt(at_st[:, i * hd : (i + 1) * hd], qkvbuf[0:keys, 2 * hw + i * hd : 2 * hw + (i + 1) * hd])
                for i in range(heads)
            ]
            probs, d_scores = [], []
            for raw, dp in zip(raws, d_probs):
                p = causal_softmax(c, keys, raw)
                probs.append(p.astype(BF16))
                d_scores.append((p * (dp - jnp.sum(p * dp, axis=-1, keepdims=True)) * scale).astype(BF16))
            for i in range(heads):
                cols = slice(i * hd, (i + 1) * hd)
                ds_st[i, :, 0:keys] = d_scores[i]
                pr_st[i, :, 0:keys] = probs[i]
                dqkv_st[:, cols] = dot_nn(d_scores[i], qkvbuf[0:keys, hw + i * hd : hw + (i + 1) * hd]).astype(BF16)

        by_prefix(c, attend)
        near_keys = pl.ds(pl.multiple_of(lax.div(c * t, key_block) * key_block, key_block), key_block)
        for i in range(heads):
            cols = slice(i * hd, (i + 1) * hd)
            dkacc[near_keys, cols] += dot_tn(ds_st[i, :, near_keys], qkvbuf[rows_of(c), cols])
            dvacc[near_keys, cols] += dot_tn(pr_st[i, :, near_keys], at_st[:, cols])
        dqkv_st[:, hw : 2 * hw] = dkacc[rows_of(c), :].astype(BF16)
        dqkv_st[:, 2 * hw : 3 * hw] = dvacc[rows_of(c), :].astype(BF16)
        staged_out(4, c).start()
        tile = tile_of(d_model)

        @pl.when(stage > 0)
        def _():
            for j in range(d_model // tile):
                cols = slice(j * tile, (j + 1) * tile)
                rs_s[3, slot, :, cols] = dot_nn(dqkv_st[...], wqkv_t[:, cols]).astype(BF16)
            rs_start(3, c)

        @pl.when(stage == 0)
        def _():
            h32 = hbuf[rows_of(c), :].astype(F32)
            normed = h32 * rms_inverse(h32)
            for j in range(d_model // tile):
                cols = slice(j * tile, (j + 1) * tile)
                gacc[0, :, cols] += fold_rows(dot_nn(dqkv_st[...], wqkv_t[:, cols]) * normed[:, cols])

        def older(keys):
            for i in range(heads):
                cols = slice(i * hd, (i + 1) * hd)
                ds_st[i, :, near_keys] = jnp.zeros((t, key_block), BF16)
                pr_st[i, :, near_keys] = jnp.zeros((t, key_block), BF16)
            for i in range(heads):
                cols = slice(i * hd, (i + 1) * hd)
                dkacc[0:keys, cols] += dot_tn(ds_st[i, :, 0:keys], qkvbuf[rows_of(c), cols])
                dvacc[0:keys, cols] += dot_tn(pr_st[i, :, 0:keys], at_st[:, cols])

        @pl.when(c * t >= key_block)
        def _():
            by_prefix(c, older)

    def loss_copy():
        return remote(lossbuf, lossbuf, loss_sem.at[0], loss_sem.at[1], {"stage": down_stage})

    def bwd_end(c, first):
        @pl.when(stage > 0)
        def _():
            h32 = hbuf[quarter(c, me), :].astype(F32)
            d_in = dmidq[lax.rem(c, 4)] + rms_backward(h32, gain_a, 0, lambda: rs_sum(3, c))

            @pl.when(jnp.logical_not(first))
            def _():
                d_all(c).wait_send()

            dsend[...] = d_in.astype(BF16)
            for d in far_first:
                d_copy(c, lax.rem(me + d, n_model)).start()

        @pl.when(first)
        def _():
            @pl.when(stage < last)
            def _():
                loss_copy().wait_recv()

            @pl.when(stage > 0)
            def _():
                loss_copy().start()

    pipeline(
        [(bwd_mlp, 0, "bwd_mlp"), (bwd_end, 2, "bwd_end", lax.rem(stage, 2) == 0), (bwd_attn, 1, "bwd_attn"), (bwd_mid, 0, "bwd_mid"), (bwd_end, 1, "bwd_end", lax.rem(stage, 2) == 1)],
        lambda j: n - 1 - j,
    )

    fin_s[...] = jnp.zeros_like(fin_s)
    fin_s[0:1, :] = jnp.sum(gacc[0], axis=0, keepdims=True)
    fin_s[1:2, :] = jnp.sum(gacc[1], axis=0, keepdims=True)
    fin_s[2:3, 0:128] = jnp.sum(lossbuf[...], axis=0, keepdims=True)

    def fin_copy(d, peer):
        return remote(fin_s, fin_r.at[d - 1], fin_ssem.at[0], fin_rsem.at[0], {"model": peer})

    for d in order:
        fin_copy(d, lax.rem(me + d, n_model)).start()

    for c in range(min(n, 2)):
        rs_drain(2, c)
    ag_drain(1, dmidbuf)
    staged_out(3, 0).wait()
    staged_out(4, 0).wait()
    for k in range(3):
        full_all(k).wait()

    @pl.when(stage > 0)
    def _():
        for c in range(min(n, 2)):
            rs_drain(3, c)
        d_all(0).wait_send()
        loss_copy().wait_send()

    fin_all = remote(fin_r, fin_r, fin_ssem.at[0], fin_rsem.at[0], {"model": 0})
    fin_all.wait_recv()
    fin_all.wait_send()
    parts = [jnp.where(me == 0, fin_s[...], 0.0)]
    for m in range(n_model):
        term = jnp.where(me == m, fin_s[...], 0.0)
        for d in range(1, n_model):
            term = term + jnp.where(lax.rem(m + d, n_model) == me, fin_r[d - 1], 0.0)
        parts.append(term)
    total = parts[1]
    for m in range(1, n_model):
        total = total + parts[m + 1]
    fin_s[0:2, :] = total[0:2, :]
    loss = jnp.sum(total[2:3, :], axis=-1, keepdims=True) * (0.5 / elem_count)
    fin_s[2:8, :] = jnp.broadcast_to(loss, (6, d_model))
    small_out = pltpu.make_async_copy(fin_s, small_hbm, out_sem.at[0])
    small_out.start()
    small_out.wait()


def run_step(cfg, x, y, wqkv, wout, wup, wdown, gain):
    n, t, tq, n_model, seq = cfg["n"], cfg["t"], cfg["tq"], cfg["n_model"], cfg["seq"]
    d_model, ff, hw = cfg["d_model"], cfg["ff"], cfg["heads"] * cfg["hd"]
    dma = pltpu.SemaphoreType.DMA
    near = max(n_model - 1, 1)
    act = lambda width: jax.ShapeDtypeStruct((seq, width), BF16)
    any_spec = pl.BlockSpec(memory_space=pl.ANY)
    vmem_spec = pl.BlockSpec(memory_space=pltpu.VMEM)
    scratch = [
        pltpu.VMEM((d_model, 3 * hw), BF16),
        pltpu.VMEM((hw, d_model), BF16),
        pltpu.VMEM((d_model, ff), BF16),
        pltpu.VMEM((ff, d_model), BF16),
        pltpu.VMEM((3 * hw, d_model), BF16),
        pltpu.VMEM((d_model, hw), BF16),
        pltpu.VMEM((ff, d_model), BF16),
        pltpu.VMEM((d_model, ff), BF16),
        pltpu.VMEM((seq, d_model), BF16),
        pltpu.VMEM((seq, d_model), BF16),
        pltpu.VMEM((seq, d_model), BF16),
        pltpu.VMEM((seq, d_model), BF16),
        pltpu.VMEM((seq, 3 * hw), BF16),
        pltpu.VMEM((seq, ff), F32),
        pltpu.VMEM((n, tq, d_model), F32),
        pltpu.VMEM((n * tq, d_model), BF16),
        pltpu.VMEM((seq, hw), F32),
        pltpu.VMEM((seq, hw), F32),
        pltpu.VMEM((4, 2, near, tq, d_model), BF16),
        pltpu.VMEM((4, 2, t, d_model), BF16),
        pltpu.VMEM((t, d_model), BF16),
        pltpu.VMEM((t, ff), BF16),
        pltpu.VMEM((t, hw), BF16),
        pltpu.VMEM((t, ff), BF16),
        pltpu.VMEM((t, 3 * hw), BF16),
        pltpu.VMEM((cfg["heads"], t, seq), BF16),
        pltpu.VMEM((cfg["heads"], t, seq), BF16),
        pltpu.VMEM((tq, d_model), BF16),
        pltpu.VMEM((tq, d_model), BF16),
        pltpu.VMEM((4, tq, d_model), F32),
        pltpu.VMEM((8, d_model), F32),
        pltpu.VMEM((2, 8, d_model), F32),
        pltpu.VMEM((8, 128), F32),
        pltpu.VMEM((8, d_model), F32),
        pltpu.VMEM((near, 8, d_model), F32),
        dma((3 * cfg["heads"] + 3,)),
        dma((2,)),
        dma((1,)),
        dma((n,)),
        dma((1,)),
        dma((n,)),
        dma((1,)),
        dma((4, 2)),
        dma((4, 2)),
        dma((2, 2)),
        dma((2,)),
        dma((5,)),
        dma((3,)),
        dma((2,)),
        dma((1,)),
        dma((1,)),
    ]
    return pl.pallas_call(
        functools.partial(step_kernel, cfg),
        name="pipeline_step",
        out_shape=(
            act(d_model), act(d_model), act(hw), act(ff), act(3 * hw), act(d_model), act(ff), act(d_model),
            jax.ShapeDtypeStruct((8, d_model), F32),
        ),
        in_specs=[any_spec] * 6 + [vmem_spec],
        out_specs=[any_spec] * 9,
        scratch_shapes=scratch,
        compiler_params=pltpu.CompilerParams(
            collective_id=0, has_side_effects=True, vmem_limit_bytes=VMEM_BYTES
        ),
    )(x, y, wqkv, wout, wup, wdown, gain)


def grads_kernel(nj, bm, *refs):
    ins, small = refs[: 2 * nj], refs[2 * nj]
    outs, loss_hbm, gain_hbm = refs[2 * nj + 1 : 3 * nj + 1], refs[3 * nj + 1], refs[3 * nj + 2]
    scratch = refs[3 * nj + 3 :]
    bufs, stages = scratch[: 2 * nj], scratch[2 * nj : 3 * nj]
    small_buf, loss_buf, gain_buf, in_sem, out_sem, small_sem = scratch[3 * nj :]

    def load(k):
        return pltpu.make_async_copy(ins[k], bufs[k], in_sem.at[k])

    for k in range(2 * nj):
        load(k).start()
    small_in = pltpu.make_async_copy(small, small_buf, small_sem.at[0])
    small_in.start()
    for j in range(nj):
        load(2 * j).wait()
        load(2 * j + 1).wait()
        a, b, out, stage = bufs[2 * j], bufs[2 * j + 1], outs[j], stages[j]
        rows = a.shape[1]
        step = min(bm, rows)
        blocks = rows // step

        def put(i, slot):
            where = pl.ds(pl.multiple_of(i * step, step), step)
            dst = out.at[:, where] if len(out.shape) == 3 else out.at[where]
            return pltpu.make_async_copy(stage.at[slot], dst, out_sem.at[j, slot])

        def block(i, carry):
            slot = lax.rem(i, 2)

            @pl.when(i >= 2)
            def _():
                put(i, slot).wait()

            acc = dot_tn(a[:, pl.ds(pl.multiple_of(i * step, step), step)], b[...])
            if len(out.shape) == 3:
                lanes = out.shape[2]
                for s in range(out.shape[0]):
                    stage[slot, s] = acc[:, s * lanes : (s + 1) * lanes]
            else:
                stage[slot] = acc
            put(i, slot).start()
            return carry

        lax.fori_loop(0, blocks, block, 0)
    small_in.wait()
    loss_buf[...] = small_buf[2:3, 0:1]
    gain_buf[...] = small_buf[0:2, :]
    loss_out = pltpu.make_async_copy(loss_buf, loss_hbm, small_sem.at[0])
    gain_out = pltpu.make_async_copy(gain_buf, gain_hbm, small_sem.at[1])
    loss_out.start()
    gain_out.start()
    for j in range(nj):
        rows = bufs[2 * j].shape[1]
        step = min(bm, rows)
        for slot in range(min(2, rows // step)):
            out, stage = outs[j], stages[j]
            dst = out.at[:, 0:step] if len(out.shape) == 3 else out.at[0:step]
            pltpu.make_async_copy(stage.at[slot], dst, out_sem.at[j, slot]).wait()
    loss_out.wait()
    gain_out.wait()


def weight_grads(pairs, out_shapes, small, bm):
    nj = len(pairs)
    flat = [x for pair in pairs for x in pair]
    any_spec = pl.BlockSpec(memory_space=pl.ANY)
    stages = []
    for (a, _), out in zip(pairs, out_shapes):
        step = min(bm, a.shape[1])
        stages.append(pltpu.VMEM((2,) + out[:-2] + (step, out[-1]), F32))
    outs = [jax.ShapeDtypeStruct(out, F32) for out in out_shapes]
    outs += [jax.ShapeDtypeStruct((1, 1), F32), jax.ShapeDtypeStruct((2, small.shape[1]), F32)]
    return pl.pallas_call(
        functools.partial(grads_kernel, nj, bm),
        name="weight_grads",
        out_shape=outs,
        in_specs=[any_spec] * (2 * nj + 1),
        out_specs=[any_spec] * (nj + 2),
        scratch_shapes=[pltpu.VMEM(x.shape, x.dtype) for x in flat]
        + stages
        + [pltpu.VMEM(small.shape, F32), pltpu.VMEM((1, 1), F32), pltpu.VMEM((2, small.shape[1]), F32)]
        + [pltpu.SemaphoreType.DMA((2 * nj,)), pltpu.SemaphoreType.DMA((nj, 2)), pltpu.SemaphoreType.DMA((2,))],
        compiler_params=pltpu.CompilerParams(vmem_limit_bytes=VMEM_BYTES),
    )(*flat, small)


def solution(mesh):
    n_stage = mesh.shape["stage"]
    n_model = mesh.shape["model"]

    def device_fn(x_in, y_target, w_qkv, w_out, w_up, w_down, norm_gain):
        n_batch, seq_len, d_model = x_in.shape
        heads, hd, ff = w_qkv.shape[3], w_qkv.shape[4], w_up.shape[2]
        t = min(CHUNK, seq_len)
        cfg = dict(
            n=seq_len // t, t=t, tq=t // n_model, n_model=n_model, n_stage=n_stage, seq=seq_len, d_model=d_model,
            heads=heads, hd=hd, ff=ff, elem_count=n_batch * seq_len * d_model,
        )
        na, nb, at, z, dqkv, dmid, dup, dout, small = run_step(
            cfg, x_in[0], y_target[0], w_qkv[0].transpose(1, 2, 0, 3).reshape(3 * heads, d_model, hd), w_out[0].reshape(heads * hd, d_model),
            w_up[0], w_down[0], norm_gain[0],
        )
        g_out, g_up, g_down, g_qkv, loss, g_gain = weight_grads(
            [(at, dmid), (nb, dup), (z, dout), (na, dqkv)],
            [(heads * hd, d_model), (d_model, ff), (ff, d_model), (3 * heads, d_model, hd)],
            small,
            tile_of(d_model, GRAD_ROWS),
        )
        grad_qkv = g_qkv.reshape(3, heads, d_model, hd).transpose(2, 0, 1, 3)[None]
        return loss.reshape(1), grad_qkv, g_out.reshape(1, heads, hd, d_model), g_up[None], g_down[None], g_gain[None]

    act_spec = P("data", None, None)
    weight_specs = (
        P("stage", None, None, "model", None),
        P("stage", "model", None, None),
        P("stage", None, "model"),
        P("stage", "model", None),
        P("stage", None, None),
    )
    grad_specs = (
        P(("data", "stage"), None, None, "model", None),
        P(("data", "stage"), "model", None, None),
        P(("data", "stage"), None, "model"),
        P(("data", "stage"), "model", None),
        P(("data", "stage"), None, None),
    )
    return jax.shard_map(
        device_fn,
        mesh=mesh,
        in_specs=(act_spec, act_spec) + weight_specs,
        out_specs=(P("data"),) + grad_specs,
        check_vma=False,
    )
```

```python
import functools
import math

import jax
import jax.numpy as jnp
from jax import lax
from jax.experimental import pallas as pl
from jax.experimental.pallas import tpu as pltpu
from jax.sharding import PartitionSpec as P

NORM_EPS = 1e-6
NEG_BIG = -1e30
CHUNK = 64
KEY_STEP = 256
SPREAD_FROM = 4
GRAD_ROWS = 768
LOG2E = 1.4426950408889634
F32 = jnp.float32
BF16 = jnp.bfloat16
MESH_ID = pl.DeviceIdType.MESH
GELU_A = math.sqrt(2.0 / math.pi)
GELU_B = 0.044715
VMEM_BYTES = 67043328


def dot_nn(a, b):
    return lax.dot_general(a, b, (((1,), (0,)), ((), ())), preferred_element_type=F32)


def dot_nt(a, b):
    return lax.dot_general(a, b, (((1,), (1,)), ((), ())), preferred_element_type=F32)


def dot_tn(a, b):
    return lax.dot_general(a, b, (((0,), (0,)), ((), ())), preferred_element_type=F32)


def rms_inverse(v):
    return lax.rsqrt(jnp.mean(v * v, axis=-1, keepdims=True) + NORM_EPS)


def gelu_tanh(u):
    return u * (0.5 * (1.0 + jnp.tanh(GELU_A * (u + GELU_B * (u * u * u)))))


def gelu_slope(u):
    t = jnp.tanh(GELU_A * (u + GELU_B * (u * u * u)))
    return 0.5 * (1.0 + t) + (0.5 * u) * (1.0 - t * t) * (GELU_A * (1.0 + (3.0 * GELU_B) * (u * u)))


def tile_of(width, top=512):
    for tile in (top, 512, 384, 256, 128):
        if width % tile == 0:
            return tile
    return width


def fold_rows(v):
    total = v[0:8]
    for r in range(8, v.shape[0], 8):
        total = total + v[r : r + 8]
    return total


def step_kernel(cfg, *refs):
    n, t, tq, n_model, n_stage = cfg["n"], cfg["t"], cfg["tq"], cfg["n_model"], cfg["n_stage"]
    seq, d_model, heads, hd, ff = cfg["seq"], cfg["d_model"], cfg["heads"], cfg["hd"], cfg["ff"]
    hw = heads * hd
    elem_count = cfg["elem_count"]
    scale = hd**-0.5
    (
        x_hbm, y_hbm, wqkv_hbm, wout_hbm, wup_hbm, wdown_hbm, gain_ref,
        na_hbm, nb_hbm, at_hbm, z_hbm, dqkv_hbm, dmid_hbm, dup_hbm, dout_hbm, small_hbm,
        wqkv, wout, wup, wdown, wqkv_t, wout_t, wup_t, wdown_t, hbuf, nbbuf, doutbuf, dmidbuf, qkvbuf, upbuf, midq, yq, dkacc, dvacc,
        rs_r, rs_s, heads_r, na_st, z_st, at_st, dup_st, dqkv_st, ds_st, pr_st, hsend, dsend, dmidq,
        lossacc, gacc, lossbuf, fin_s, fin_r,
        w_sem, x_sem, y_sem, h_rsem, h_ssem, d_rsem, d_ssem, rs_rsem, rs_ssem, ag_rsem, ag_ssem, wout_sem, heads_sem,
        out_sem, full_sem, loss_sem, fin_rsem, fin_ssem,
    ) = refs
    me = lax.axis_index("model")
    stage = lax.axis_index("stage")
    last = n_stage - 1
    spread = stage >= SPREAD_FROM
    order = [d for d in (2, 1, 3) if d < n_model] if n_model > 2 else list(range(1, n_model))

    odd = lax.rem(me, 2)
    send_order = [2, 3 - 2 * odd, 1 + 2 * odd] if n_model == 4 else order

    far_first = [2, 3 - 2 * odd, 1 + 2 * odd, 0] if n_model == 4 else list(range(n_model))

    def remote(src, dst, ssem, rsem, where):
        return pltpu.make_async_remote_copy(
            src_ref=src, dst_ref=dst, send_sem=ssem, recv_sem=rsem, device_id=where, device_id_type=MESH_ID
        )

    def rows_of(c):
        return pl.ds(pl.multiple_of(c * t, t), t)

    def quarter(c, m):
        return pl.ds(pl.multiple_of(c * t + m * tq, tq), tq)

    own = pl.ds(pl.multiple_of(me * tq, tq), tq)
    own_heads = pl.ds(pl.multiple_of(me * hw, hw), hw)

    slabs = 3 * heads

    def weight_copy(k):
        if k < slabs:
            return pltpu.make_async_copy(wqkv_hbm.at[k], wqkv.at[:, pl.ds(k * hd, hd)], w_sem.at[k])
        src = (wout_hbm, wup_hbm, wdown_hbm)[k - slabs]
        dst = (wout.at[own_heads], wup, wdown)[k - slabs]
        return pltpu.make_async_copy(src, dst, w_sem.at[k])

    def x_copy(k):
        rows = pl.ds(0, t) if k == 0 else pl.ds(t, seq - t)
        return pltpu.make_async_copy(x_hbm.at[rows], hbuf.at[rows], x_sem.at[k])

    def y_copy(c):
        return pltpu.make_async_copy(y_hbm.at[quarter(c, me)], yq.at[pl.ds(c * tq, tq)], y_sem.at[0])

    def y_all():
        return pltpu.make_async_copy(y_hbm.at[pl.ds(0, n * tq)], yq, y_sem.at[0])

    @pl.when(stage == 0)
    def _():
        x_copy(0).start()

    for k in range(slabs + 3):
        weight_copy(k).start()

    @pl.when(stage == 0)
    def _():
        x_copy(1).start()

    @pl.when(stage == last)
    def _():
        for c in range(n):
            y_copy(c).start()

    barrier = pltpu.get_barrier_semaphore()
    up_stage = lax.rem(stage + 1, n_stage)
    down_stage = lax.rem(stage + n_stage - 1, n_stage)
    greet = [{"model": lax.rem(me + d, n_model)} for d in range(1, n_model)]
    greet += [{"stage": up_stage, "model": m} for m in range(n_model)]
    if n_stage > 2:
        greet += [{"stage": down_stage, "model": m} for m in range(n_model)]
    for where in greet:
        pl.semaphore_signal(barrier, inc=1, device_id=where, device_id_type=MESH_ID)

    qkvbuf[:, 2 * hw : 3 * hw] = jnp.zeros((seq, hw), BF16)
    lossacc[...] = jnp.zeros_like(lossacc)
    gacc[...] = jnp.zeros_like(gacc)
    pl.semaphore_wait(barrier, len(greet))

    gains = gain_ref[...].astype(F32)
    gain_a = gains[0:1, :]
    gain_b = gains[1:2, :]

    others = n_model - 1

    def rs_copy(p, c, d, peer):
        slot = lax.rem(c, 2)
        return remote(
            rs_s.at[p, slot, pl.ds(pl.multiple_of(peer * tq, tq), tq)], rs_r.at[p, slot, d - 1],
            rs_ssem.at[p, slot], rs_rsem.at[p, slot], {"model": peer},
        )

    def rs_all(p, c):
        slot = lax.rem(c, 2)
        return remote(rs_r.at[p, slot], rs_r.at[p, slot], rs_ssem.at[p, slot], rs_rsem.at[p, slot], {"model": 0})

    def rs_start(p, c):
        for d in send_order:
            rs_copy(p, c, d, lax.rem(me + d, n_model)).start()

    def rs_drain(p, c):
        rs_all(p, c).wait_send()

    def rs_sum(p, c):
        with jax.named_scope(f"rs_wait{p}"):
            rs_all(p, c).wait_recv()
        total = rs_s[p, lax.rem(c, 2), own, :].astype(F32)
        for d in range(1, n_model):
            total = total + rs_r[p, lax.rem(c, 2), d - 1].astype(F32)
        return total

    def ag_copy(p, buf, c, peer):
        slot = lax.rem(c, 2)
        return remote(
            buf.at[quarter(c, me)], buf.at[quarter(c, me)], ag_ssem.at[p], ag_rsem.at[p, slot], {"model": peer}
        )

    def ag_all(p, buf, c):
        rows = pl.ds(0, others * tq)
        return remote(buf.at[rows], buf.at[rows], ag_ssem.at[p], ag_rsem.at[p, lax.rem(c, 2)], {"model": 0})

    def ag_start(p, buf, c):
        for d in send_order:
            ag_copy(p, buf, c, lax.rem(me + d, n_model)).start()

    def ag_drain(p, buf):
        ag_all(p, buf, 0).wait_send()

    def ag_wait(p, buf, c):
        with jax.named_scope(f"ag_wait{p}"):
            ag_all(p, buf, c).wait_recv()

    def wout_copy(peer):
        return remote(wout.at[own_heads], wout.at[own_heads], wout_sem.at[0], wout_sem.at[1], {"model": peer})

    def wout_all():
        rows = pl.ds(0, others * hw)
        return remote(wout.at[rows], wout.at[rows], wout_sem.at[0], wout_sem.at[1], {"model": 0})

    def heads_copy(c, peer):
        slot = lax.rem(c, 2)
        return remote(
            at_st.at[pl.ds(pl.multiple_of(peer * tq, tq), tq)], heads_r.at[slot, me],
            heads_sem.at[0], heads_sem.at[1 + slot], {"model": peer},
        )

    def heads_all(c):
        slot = lax.rem(c, 2)
        part = heads_r.at[slot, pl.ds(0, others)]
        return remote(part, part, heads_sem.at[0], heads_sem.at[1 + slot], {"model": 0})

    def h_copy(c, m):
        return remote(
            hsend, hbuf.at[quarter(c, me)], h_ssem.at[0], h_rsem.at[c], {"stage": up_stage, "model": m}
        )

    def h_all(c):
        return remote(hbuf.at[rows_of(c)], hbuf.at[rows_of(c)], h_ssem.at[0], h_rsem.at[c], {"model": 0})

    def d_copy(c, m):
        return remote(
            dsend, doutbuf.at[quarter(c, me)], d_ssem.at[0], d_rsem.at[c], {"stage": down_stage, "model": m}
        )

    def d_all(c):
        return remote(doutbuf.at[rows_of(c)], doutbuf.at[rows_of(c)], d_ssem.at[0], d_rsem.at[c], {"model": 0})

    def peer_d_copy(c, peer):
        return remote(
            doutbuf.at[quarter(c, me)], doutbuf.at[quarter(c, me)], d_ssem.at[0], d_rsem.at[c], {"model": peer}
        )

    def peer_d_all(c):
        rows = pl.ds(0, others * tq)
        return remote(doutbuf.at[rows], doutbuf.at[rows], d_ssem.at[0], d_rsem.at[c], {"model": 0})

    def staged_out(k, c):
        src = (na_st, z_st, at_st, dup_st, dqkv_st)[k]
        dst = (na_hbm, z_hbm, at_hbm, dup_hbm, dqkv_hbm)[k]
        return pltpu.make_async_copy(src, dst.at[rows_of(c)], out_sem.at[k])

    def full_out(k, c):
        src = (nbbuf, dmidbuf, doutbuf)[k]
        dst = (nb_hbm, dmid_hbm, dout_hbm)[k]
        return pltpu.make_async_copy(src.at[rows_of(c)], dst.at[rows_of(c)], full_sem.at[k])

    def full_all(k):
        return pltpu.make_async_copy((nbbuf, dmidbuf, doutbuf)[k], (nb_hbm, dmid_hbm, dout_hbm)[k], full_sem.at[k])

    key_step = min(KEY_STEP, seq)
    key_block = max(t, 128)

    def by_prefix(c, body):
        need = lax.div(c * t + t - 1, key_step)
        for k in range(seq // key_step):

            @pl.when(need == k)
            def _():
                body((k + 1) * key_step)

    def scores(c, keys):
        return [
            dot_nt(qkvbuf[rows_of(c), i * hd : (i + 1) * hd], qkvbuf[0:keys, hw + i * hd : hw + (i + 1) * hd])
            for i in range(heads)
        ]

    def causal_softmax(c, keys, raw):
        q_pos = c * t + lax.broadcasted_iota(jnp.int32, (t, keys), 0)
        k_pos = lax.broadcasted_iota(jnp.int32, (t, keys), 1)
        s = jnp.where(k_pos <= q_pos, raw, NEG_BIG / scale)
        e = jnp.exp2((s - jnp.max(s, axis=-1, keepdims=True)) * (scale * LOG2E))
        return e * (1.0 / jnp.sum(e, axis=-1, keepdims=True))

    def fwd_attn(c, first):
        @pl.when(first & (stage == 0))
        def _():
            x_copy(0).wait()

        @pl.when((c == 1) & (stage == 0))
        def _():
            x_copy(1).wait()

        @pl.when(stage > 0)
        def _():
            with jax.named_scope("h_wait"):
                h_all(c).wait_recv()

        @pl.when(first & (stage == 0))
        def _():
            for k in range(slabs + 1):
                weight_copy(k).wait()

        @pl.when(jnp.logical_not(first))
        def _():
            staged_out(0, c).wait()
            staged_out(2, c).wait()

        @pl.when((c >= 2) & jnp.logical_not(spread))
        def _():
            rs_drain(0, c)

        @pl.when((c >= 1) & spread)
        def _():
            heads_all(c).wait_send()

        slot = lax.rem(c, 2)

        h32 = hbuf[rows_of(c), :].astype(F32)
        na_st[...] = (h32 * rms_inverse(h32) * gain_a).astype(BF16)
        staged_out(0, c).start()
        wide = 3 * hw
        tile = tile_of(wide, 384)
        for j in range(wide // tile):
            cols = slice(j * tile, (j + 1) * tile)
            qkvbuf[rows_of(c), cols] = dot_nn(na_st[...], wqkv[:, cols]).astype(BF16)

        def attend(keys):
            probs = [causal_softmax(c, keys, raw).astype(BF16) for raw in scores(c, keys)]
            for i in range(heads):
                v = qkvbuf[0:keys, 2 * hw + i * hd : 2 * hw + (i + 1) * hd]
                at_st[:, i * hd : (i + 1) * hd] = dot_nn(probs[i], v).astype(BF16)

        by_prefix(c, attend)
        staged_out(2, c).start()

        @pl.when(jnp.logical_not(spread))
        def _():
            tile = tile_of(d_model)
            for j in range(d_model // tile):
                cols = slice(j * tile, (j + 1) * tile)
                rs_s[0, lax.rem(c, 2), :, cols] = dot_nn(at_st[...], wout[own_heads, cols]).astype(BF16)
            rs_start(0, c)

        @pl.when(spread)
        def _():
            for d in send_order:
                heads_copy(c, lax.rem(me + d, n_model)).start()
            heads_r[lax.rem(c, 2), me] = at_st[own, :]

    def fwd_mid(c, first):
        @pl.when(jnp.logical_not(first))
        def _():
            ag_drain(0, nbbuf)

        @pl.when(jnp.logical_not(spread))
        def _():
            midq[c] = rs_sum(0, c) + hbuf[quarter(c, me), :].astype(F32)

        @pl.when(first & spread)
        def _():
            wout_all().wait_recv()

        @pl.when(spread)
        def _():
            heads_all(c).wait_recv()
            attn = jnp.concatenate([heads_r[lax.rem(c, 2), m] for m in range(n_model)], axis=-1)
            midq[c] = dot_nn(attn, wout[...]) + hbuf[quarter(c, me), :].astype(F32)

        mid = midq[c]
        nbbuf[quarter(c, me), :] = (mid * rms_inverse(mid) * gain_b).astype(BF16)
        ag_start(0, nbbuf, c)

    def fwd_mlp(c, first):
        @pl.when(first & (stage == 0))
        def _():
            weight_copy(slabs + 1).wait()
            weight_copy(slabs + 2).wait()

        @pl.when(jnp.logical_not(first))
        def _():
            staged_out(1, c).wait()

        @pl.when(c >= 2)
        def _():
            rs_drain(1, c)

        slot = lax.rem(c, 2)

        ag_wait(0, nbbuf, c)
        full_out(0, c).start()
        tile = tile_of(ff)
        for j in range(ff // tile):
            cols = slice(j * tile, (j + 1) * tile)
            u = dot_nn(nbbuf[rows_of(c), :], wup[:, cols])
            upbuf[rows_of(c), cols] = u
            z_st[:, cols] = gelu_tanh(u).astype(BF16)
        staged_out(1, c).start()
        tile = tile_of(d_model)
        for j in range(d_model // tile):
            cols = slice(j * tile, (j + 1) * tile)
            rs_s[1, slot, :, cols] = dot_nn(z_st[...], wdown[:, cols]).astype(BF16)
        rs_start(1, c)

    def fwd_end(c, first):
        h_out = (midq[c] + rs_sum(1, c)).astype(BF16)

        @pl.when(stage < last)
        def _():
            @pl.when(jnp.logical_not(first))
            def _():
                h_all(c).wait_send()

            hsend[...] = h_out
            for d in far_first:
                h_copy(c, lax.rem(me + d, n_model)).start()

        @pl.when(stage == last)
        def _():
            @pl.when(first)
            def _():
                y_all().wait()

            @pl.when(jnp.logical_not(first))
            def _():
                peer_d_all(c).wait_send()

            diff = h_out.astype(F32) - yq[pl.ds(pl.multiple_of(c * tq, tq), tq), :].astype(F32)
            lossacc[...] += fold_rows(diff * diff)
            doutbuf[quarter(c, me), :] = (diff * (1.0 / elem_count)).astype(BF16)
            for d in order:
                peer_d_copy(c, lax.rem(me + d, n_model)).start()

    def pipeline(phases, chunk_of):
        deepest = max(p[1] for p in phases)

        def body(i, carry):
            for phase, lag, name, *cond in phases:
                j = i - lag
                ok = (j >= 0) & (j < n)
                if cond:
                    ok = ok & cond[0]

                @pl.when(ok)
                def _():
                    with jax.named_scope(name):
                        phase(chunk_of(j), j == 0)

            return carry

        lax.fori_loop(0, n + deepest, body, 0)

    def flip_weights():
        for w, w_t in ((wdown, wdown_t), (wup, wup_t), (wout.at[own_heads], wout_t), (wqkv, wqkv_t)):
            depth = tile_of(w.shape[0], 256)
            for r in range(w.shape[0] // depth):
                w_t[:, r * depth : (r + 1) * depth] = w[r * depth : (r + 1) * depth, :].T

    @pl.when(stage > 0)
    def _():
        for k in range(slabs + 3):
            weight_copy(k).wait()

        @pl.when(spread)
        def _():
            for d in send_order:
                wout_copy(lax.rem(me + d, n_model)).start()

        flip_weights()

    pipeline(
        [(fwd_attn, 0, "fwd_attn"), (fwd_end, 2, "fwd_end", lax.rem(stage, 2) == 0), (fwd_mlp, 1, "fwd_mlp"), (fwd_mid, 0, "fwd_mid"), (fwd_end, 1, "fwd_end", lax.rem(stage, 2) == 1)],
        lambda j: j,
    )

    @pl.when(stage == 0)
    def _():
        flip_weights()

    dkacc[...] = jnp.zeros_like(dkacc)
    dvacc[...] = jnp.zeros_like(dvacc)

    @pl.when(jnp.logical_not(spread))
    def _():
        for c in range(min(n, 2)):
            rs_drain(0, c)

    @pl.when(spread)
    def _():
        heads_all(0).wait_send()
        wout_all().wait_send()

    for c in range(min(n, 2)):
        rs_drain(1, c)
    ag_drain(0, nbbuf)
    staged_out(0, 0).wait()
    staged_out(1, 0).wait()
    staged_out(2, 0).wait()

    @pl.when(stage < last)
    def _():
        h_all(0).wait_send()

    @pl.when(stage == last)
    def _():
        peer_d_all(0).wait_send()
        total = lossacc[:, 0:128]
        for j in range(1, d_model // 128):
            total = total + lossacc[:, j * 128 : (j + 1) * 128]
        lossbuf[...] = total

    def rms_backward(v, gain, k, d_norm_of):
        inv = rms_inverse(v)
        normed = v * inv
        scaled = gain * inv
        d_norm = d_norm_of()
        gacc[k] += fold_rows(d_norm * normed)
        d_normed = d_norm * gain
        return d_norm * scaled - normed * (inv * jnp.mean(d_normed * normed, axis=-1, keepdims=True))

    def bwd_mlp(c, first):
        @pl.when(stage < last)
        def _():
            with jax.named_scope("d_wait"):
                d_all(c).wait_recv()

        @pl.when(stage == last)
        def _():
            peer_d_all(c).wait_recv()

        full_out(2, c).start()

        @pl.when(jnp.logical_not(first))
        def _():
            staged_out(3, c).wait()

        @pl.when(c < n - 2)
        def _():
            rs_drain(2, c)

        slot = lax.rem(c, 2)

        tile = tile_of(ff)
        for j in range(ff // tile):
            cols = slice(j * tile, (j + 1) * tile)
            d_gelu = dot_nn(doutbuf[rows_of(c), :], wdown_t[:, cols])
            dup_st[:, cols] = (d_gelu * gelu_slope(upbuf[rows_of(c), cols])).astype(BF16)
        staged_out(3, c).start()
        tile = tile_of(d_model)
        for j in range(d_model // tile):
            cols = slice(j * tile, (j + 1) * tile)
            rs_s[2, slot, :, cols] = dot_nn(dup_st[...], wup_t[:, cols]).astype(BF16)
        rs_start(2, c)

    def bwd_mid(c, first):
        @pl.when(jnp.logical_not(first))
        def _():
            ag_drain(1, dmidbuf)

        d_out = doutbuf[quarter(c, me), :].astype(F32)
        d_mid = d_out + rms_backward(midq[c], gain_b, 1, lambda: rs_sum(2, c))
        dmidq[lax.rem(c, 4)] = d_mid
        dmidbuf[quarter(c, me), :] = d_mid.astype(BF16)
        ag_start(1, dmidbuf, c)

    def bwd_attn(c, first):
        ag_wait(1, dmidbuf, c)
        full_out(1, c).start()

        @pl.when(jnp.logical_not(first))
        def _():
            staged_out(4, c).wait()

        @pl.when((c < n - 2) & (stage > 0))
        def _():
            rs_drain(3, c)

        slot = lax.rem(c, 2)

        d_attn = dot_nn(dmidbuf[rows_of(c), :], wout_t[...]).astype(BF16)
        at_st[...] = d_attn

        def attend(keys):
            raws = scores(c, keys)
            d_probs = [
                dot_nt(at_st[:, i * hd : (i + 1) * hd], qkvbuf[0:keys, 2 * hw + i * hd : 2 * hw + (i + 1) * hd])
                for i in range(heads)
            ]
            probs, d_scores = [], []
            for raw, dp in zip(raws, d_probs):
                p = causal_softmax(c, keys, raw)
                probs.append(p.astype(BF16))
                d_scores.append((p * (dp - jnp.sum(p * dp, axis=-1, keepdims=True)) * scale).astype(BF16))
            for i in range(heads):
                cols = slice(i * hd, (i + 1) * hd)
                ds_st[i, :, 0:keys] = d_scores[i]
                pr_st[i, :, 0:keys] = probs[i]
                dqkv_st[:, cols] = dot_nn(d_scores[i], qkvbuf[0:keys, hw + i * hd : hw + (i + 1) * hd]).astype(BF16)

        by_prefix(c, attend)
        near_keys = pl.ds(pl.multiple_of(lax.div(c * t, key_block) * key_block, key_block), key_block)
        for i in range(heads):
            cols = slice(i * hd, (i + 1) * hd)
            dkacc[near_keys, cols] += dot_tn(ds_st[i, :, near_keys], qkvbuf[rows_of(c), cols])
            dvacc[near_keys, cols] += dot_tn(pr_st[i, :, near_keys], at_st[:, cols])
        dqkv_st[:, hw : 2 * hw] = dkacc[rows_of(c), :].astype(BF16)
        dqkv_st[:, 2 * hw : 3 * hw] = dvacc[rows_of(c), :].astype(BF16)
        staged_out(4, c).start()
        tile = tile_of(d_model)

        @pl.when(stage > 0)
        def _():
            for j in range(d_model // tile):
                cols = slice(j * tile, (j + 1) * tile)
                rs_s[3, slot, :, cols] = dot_nn(dqkv_st[...], wqkv_t[:, cols]).astype(BF16)
            rs_start(3, c)

        @pl.when(stage == 0)
        def _():
            h32 = hbuf[rows_of(c), :].astype(F32)
            normed = h32 * rms_inverse(h32)
            for j in range(d_model // tile):
                cols = slice(j * tile, (j + 1) * tile)
                gacc[0, :, cols] += fold_rows(dot_nn(dqkv_st[...], wqkv_t[:, cols]) * normed[:, cols])

        def older(keys):
            for i in range(heads):
                cols = slice(i * hd, (i + 1) * hd)
                ds_st[i, :, near_keys] = jnp.zeros((t, key_block), BF16)
                pr_st[i, :, near_keys] = jnp.zeros((t, key_block), BF16)
            for i in range(heads):
                cols = slice(i * hd, (i + 1) * hd)
                dkacc[0:keys, cols] += dot_tn(ds_st[i, :, 0:keys], qkvbuf[rows_of(c), cols])
                dvacc[0:keys, cols] += dot_tn(pr_st[i, :, 0:keys], at_st[:, cols])

        @pl.when(c * t >= key_block)
        def _():
            by_prefix(c, older)

    def loss_copy():
        return remote(lossbuf, lossbuf, loss_sem.at[0], loss_sem.at[1], {"stage": down_stage})

    def bwd_end(c, first):
        @pl.when(stage > 0)
        def _():
            h32 = hbuf[quarter(c, me), :].astype(F32)
            d_in = dmidq[lax.rem(c, 4)] + rms_backward(h32, gain_a, 0, lambda: rs_sum(3, c))

            @pl.when(jnp.logical_not(first))
            def _():
                d_all(c).wait_send()

            dsend[...] = d_in.astype(BF16)
            for d in far_first:
                d_copy(c, lax.rem(me + d, n_model)).start()

        @pl.when(first)
        def _():
            @pl.when(stage < last)
            def _():
                loss_copy().wait_recv()

            @pl.when(stage > 0)
            def _():
                loss_copy().start()

    pipeline(
        [(bwd_mlp, 0, "bwd_mlp"), (bwd_end, 2, "bwd_end", lax.rem(stage, 2) == 0), (bwd_attn, 1, "bwd_attn"), (bwd_mid, 0, "bwd_mid"), (bwd_end, 1, "bwd_end", lax.rem(stage, 2) == 1)],
        lambda j: n - 1 - j,
    )

    fin_s[...] = jnp.zeros_like(fin_s)
    fin_s[0:1, :] = jnp.sum(gacc[0], axis=0, keepdims=True)
    fin_s[1:2, :] = jnp.sum(gacc[1], axis=0, keepdims=True)
    fin_s[2:3, 0:128] = jnp.sum(lossbuf[...], axis=0, keepdims=True)

    def fin_copy(d, peer):
        return remote(fin_s, fin_r.at[d - 1], fin_ssem.at[0], fin_rsem.at[0], {"model": peer})

    for d in order:
        fin_copy(d, lax.rem(me + d, n_model)).start()

    for c in range(min(n, 2)):
        rs_drain(2, c)
    ag_drain(1, dmidbuf)
    staged_out(3, 0).wait()
    staged_out(4, 0).wait()
    for k in range(3):
        full_all(k).wait()

    @pl.when(stage > 0)
    def _():
        for c in range(min(n, 2)):
            rs_drain(3, c)
        d_all(0).wait_send()
        loss_copy().wait_send()

    fin_all = remote(fin_r, fin_r, fin_ssem.at[0], fin_rsem.at[0], {"model": 0})
    fin_all.wait_recv()
    fin_all.wait_send()
    parts = [jnp.where(me == 0, fin_s[...], 0.0)]
    for m in range(n_model):
        term = jnp.where(me == m, fin_s[...], 0.0)
        for d in range(1, n_model):
            term = term + jnp.where(lax.rem(m + d, n_model) == me, fin_r[d - 1], 0.0)
        parts.append(term)
    total = parts[1]
    for m in range(1, n_model):
        total = total + parts[m + 1]
    fin_s[0:2, :] = total[0:2, :]
    loss = jnp.sum(total[2:3, :], axis=-1, keepdims=True) * (0.5 / elem_count)
    fin_s[2:8, :] = jnp.broadcast_to(loss, (6, d_model))
    small_out = pltpu.make_async_copy(fin_s, small_hbm, out_sem.at[0])
    small_out.start()
    small_out.wait()


def run_step(cfg, x, y, wqkv, wout, wup, wdown, gain):
    n, t, tq, n_model, seq = cfg["n"], cfg["t"], cfg["tq"], cfg["n_model"], cfg["seq"]
    d_model, ff, hw = cfg["d_model"], cfg["ff"], cfg["heads"] * cfg["hd"]
    dma = pltpu.SemaphoreType.DMA
    near = max(n_model - 1, 1)
    act = lambda width: jax.ShapeDtypeStruct((seq, width), BF16)
    any_spec = pl.BlockSpec(memory_space=pl.ANY)
    vmem_spec = pl.BlockSpec(memory_space=pltpu.VMEM)
    scratch = [
        pltpu.VMEM((d_model, 3 * hw), BF16),
        pltpu.VMEM((n_model * hw, d_model), BF16),
        pltpu.VMEM((d_model, ff), BF16),
        pltpu.VMEM((ff, d_model), BF16),
        pltpu.VMEM((3 * hw, d_model), BF16),
        pltpu.VMEM((d_model, hw), BF16),
        pltpu.VMEM((ff, d_model), BF16),
        pltpu.VMEM((d_model, ff), BF16),
        pltpu.VMEM((seq, d_model), BF16),
        pltpu.VMEM((seq, d_model), BF16),
        pltpu.VMEM((seq, d_model), BF16),
        pltpu.VMEM((seq, d_model), BF16),
        pltpu.VMEM((seq, 3 * hw), BF16),
        pltpu.VMEM((seq, ff), F32),
        pltpu.VMEM((n, tq, d_model), F32),
        pltpu.VMEM((n * tq, d_model), BF16),
        pltpu.VMEM((seq, hw), F32),
        pltpu.VMEM((seq, hw), F32),
        pltpu.VMEM((4, 2, near, tq, d_model), BF16),
        pltpu.VMEM((4, 2, t, d_model), BF16),
        pltpu.VMEM((2, n_model, tq, hw), BF16),
        pltpu.VMEM((t, d_model), BF16),
        pltpu.VMEM((t, ff), BF16),
        pltpu.VMEM((t, hw), BF16),
        pltpu.VMEM((t, ff), BF16),
        pltpu.VMEM((t, 3 * hw), BF16),
        pltpu.VMEM((cfg["heads"], t, seq), BF16),
        pltpu.VMEM((cfg["heads"], t, seq), BF16),
        pltpu.VMEM((tq, d_model), BF16),
        pltpu.VMEM((tq, d_model), BF16),
        pltpu.VMEM((4, tq, d_model), F32),
        pltpu.VMEM((8, d_model), F32),
        pltpu.VMEM((2, 8, d_model), F32),
        pltpu.VMEM((8, 128), F32),
        pltpu.VMEM((8, d_model), F32),
        pltpu.VMEM((near, 8, d_model), F32),
        dma((3 * cfg["heads"] + 3,)),
        dma((2,)),
        dma((1,)),
        dma((n,)),
        dma((1,)),
        dma((n,)),
        dma((1,)),
        dma((4, 2)),
        dma((4, 2)),
        dma((2, 2)),
        dma((2,)),
        dma((2,)),
        dma((3,)),
        dma((5,)),
        dma((3,)),
        dma((2,)),
        dma((1,)),
        dma((1,)),
    ]
    return pl.pallas_call(
        functools.partial(step_kernel, cfg),
        name="pipeline_step",
        out_shape=(
            act(d_model), act(d_model), act(hw), act(ff), act(3 * hw), act(d_model), act(ff), act(d_model),
            jax.ShapeDtypeStruct((8, d_model), F32),
        ),
        in_specs=[any_spec] * 6 + [vmem_spec],
        out_specs=[any_spec] * 9,
        scratch_shapes=scratch,
        compiler_params=pltpu.CompilerParams(
            collective_id=0, has_side_effects=True, vmem_limit_bytes=VMEM_BYTES
        ),
    )(x, y, wqkv, wout, wup, wdown, gain)


def grads_kernel(nj, bm, *refs):
    ins, small = refs[: 2 * nj], refs[2 * nj]
    outs, loss_hbm, gain_hbm = refs[2 * nj + 1 : 3 * nj + 1], refs[3 * nj + 1], refs[3 * nj + 2]
    scratch = refs[3 * nj + 3 :]
    bufs, stages = scratch[: 2 * nj], scratch[2 * nj : 3 * nj]
    small_buf, loss_buf, gain_buf, in_sem, out_sem, small_sem = scratch[3 * nj :]

    def load(k):
        return pltpu.make_async_copy(ins[k], bufs[k], in_sem.at[k])

    for k in range(2 * nj):
        load(k).start()
    small_in = pltpu.make_async_copy(small, small_buf, small_sem.at[0])
    small_in.start()
    for j in range(nj):
        load(2 * j).wait()
        load(2 * j + 1).wait()
        a, b, out, stage = bufs[2 * j], bufs[2 * j + 1], outs[j], stages[j]
        rows = a.shape[1]
        step = min(bm, rows)
        blocks = rows // step

        def put(i, slot):
            where = pl.ds(pl.multiple_of(i * step, step), step)
            dst = out.at[:, where] if len(out.shape) == 3 else out.at[where]
            return pltpu.make_async_copy(stage.at[slot], dst, out_sem.at[j, slot])

        def block(i, carry):
            slot = lax.rem(i, 2)

            @pl.when(i >= 2)
            def _():
                put(i, slot).wait()

            acc = dot_tn(a[:, pl.ds(pl.multiple_of(i * step, step), step)], b[...])
            if len(out.shape) == 3:
                lanes = out.shape[2]
                for s in range(out.shape[0]):
                    stage[slot, s] = acc[:, s * lanes : (s + 1) * lanes]
            else:
                stage[slot] = acc
            put(i, slot).start()
            return carry

        lax.fori_loop(0, blocks, block, 0)
    small_in.wait()
    loss_buf[...] = small_buf[2:3, 0:1]
    gain_buf[...] = small_buf[0:2, :]
    loss_out = pltpu.make_async_copy(loss_buf, loss_hbm, small_sem.at[0])
    gain_out = pltpu.make_async_copy(gain_buf, gain_hbm, small_sem.at[1])
    loss_out.start()
    gain_out.start()
    for j in range(nj):
        rows = bufs[2 * j].shape[1]
        step = min(bm, rows)
        for slot in range(min(2, rows // step)):
            out, stage = outs[j], stages[j]
            dst = out.at[:, 0:step] if len(out.shape) == 3 else out.at[0:step]
            pltpu.make_async_copy(stage.at[slot], dst, out_sem.at[j, slot]).wait()
    loss_out.wait()
    gain_out.wait()


def weight_grads(pairs, out_shapes, small, bm):
    nj = len(pairs)
    flat = [x for pair in pairs for x in pair]
    any_spec = pl.BlockSpec(memory_space=pl.ANY)
    stages = []
    for (a, _), out in zip(pairs, out_shapes):
        step = min(bm, a.shape[1])
        stages.append(pltpu.VMEM((2,) + out[:-2] + (step, out[-1]), F32))
    outs = [jax.ShapeDtypeStruct(out, F32) for out in out_shapes]
    outs += [jax.ShapeDtypeStruct((1, 1), F32), jax.ShapeDtypeStruct((2, small.shape[1]), F32)]
    return pl.pallas_call(
        functools.partial(grads_kernel, nj, bm),
        name="weight_grads",
        out_shape=outs,
        in_specs=[any_spec] * (2 * nj + 1),
        out_specs=[any_spec] * (nj + 2),
        scratch_shapes=[pltpu.VMEM(x.shape, x.dtype) for x in flat]
        + stages
        + [pltpu.VMEM(small.shape, F32), pltpu.VMEM((1, 1), F32), pltpu.VMEM((2, small.shape[1]), F32)]
        + [pltpu.SemaphoreType.DMA((2 * nj,)), pltpu.SemaphoreType.DMA((nj, 2)), pltpu.SemaphoreType.DMA((2,))],
        compiler_params=pltpu.CompilerParams(vmem_limit_bytes=VMEM_BYTES),
    )(*flat, small)


def solution(mesh):
    n_stage = mesh.shape["stage"]
    n_model = mesh.shape["model"]

    def device_fn(x_in, y_target, w_qkv, w_out, w_up, w_down, norm_gain):
        n_batch, seq_len, d_model = x_in.shape
        heads, hd, ff = w_qkv.shape[3], w_qkv.shape[4], w_up.shape[2]
        t = min(CHUNK, seq_len)
        cfg = dict(
            n=seq_len // t, t=t, tq=t // n_model, n_model=n_model, n_stage=n_stage, seq=seq_len, d_model=d_model,
            heads=heads, hd=hd, ff=ff, elem_count=n_batch * seq_len * d_model,
        )
        na, nb, at, z, dqkv, dmid, dup, dout, small = run_step(
            cfg, x_in[0], y_target[0], w_qkv[0].transpose(1, 2, 0, 3).reshape(3 * heads, d_model, hd), w_out[0].reshape(heads * hd, d_model),
            w_up[0], w_down[0], norm_gain[0],
        )
        g_out, g_up, g_down, g_qkv, loss, g_gain = weight_grads(
            [(at, dmid), (nb, dup), (z, dout), (na, dqkv)],
            [(heads * hd, d_model), (d_model, ff), (ff, d_model), (3 * heads, d_model, hd)],
            small,
            tile_of(d_model, GRAD_ROWS),
        )
        grad_qkv = g_qkv.reshape(3, heads, d_model, hd).transpose(2, 0, 1, 3)[None]
        return loss.reshape(1), grad_qkv, g_out.reshape(1, heads, hd, d_model), g_up[None], g_down[None], g_gain[None]

    act_spec = P("data", None, None)
    weight_specs = (
        P("stage", None, None, "model", None),
        P("stage", "model", None, None),
        P("stage", None, "model"),
        P("stage", "model", None),
        P("stage", None, None),
    )
    grad_specs = (
        P(("data", "stage"), None, None, "model", None),
        P(("data", "stage"), "model", None, None),
        P(("data", "stage"), None, "model"),
        P(("data", "stage"), "model", None),
        P(("data", "stage"), None, None),
    )
    return jax.shard_map(
        device_fn,
        mesh=mesh,
        in_specs=(act_spec, act_spec) + weight_specs,
        out_specs=(P("data"),) + grad_specs,
        check_vma=False,
    )
```

```python
import functools
import math

import jax
import jax.numpy as jnp
from jax import lax
from jax.experimental import pallas as pl
from jax.experimental.pallas import tpu as pltpu
from jax.sharding import PartitionSpec as P

NORM_EPS = 1e-6
NEG_BIG = -1e30
CHUNK = 64
KEY_STEP = 256
SPREAD_FROM = 3
GRAD_ROWS = 768
LOG2E = 1.4426950408889634
F32 = jnp.float32
BF16 = jnp.bfloat16
MESH_ID = pl.DeviceIdType.MESH
GELU_A = math.sqrt(2.0 / math.pi)
GELU_B = 0.044715
VMEM_BYTES = 67043328


def dot_nn(a, b):
    return lax.dot_general(a, b, (((1,), (0,)), ((), ())), preferred_element_type=F32)


def dot_nt(a, b):
    return lax.dot_general(a, b, (((1,), (1,)), ((), ())), preferred_element_type=F32)


def dot_tn(a, b):
    return lax.dot_general(a, b, (((0,), (0,)), ((), ())), preferred_element_type=F32)


def rms_inverse(v):
    return lax.rsqrt(jnp.mean(v * v, axis=-1, keepdims=True) + NORM_EPS)


def gelu_tanh(u):
    return u * (0.5 * (1.0 + jnp.tanh(GELU_A * (u + GELU_B * (u * u * u)))))


def gelu_slope(u):
    t = jnp.tanh(GELU_A * (u + GELU_B * (u * u * u)))
    return 0.5 * (1.0 + t) + (0.5 * u) * (1.0 - t * t) * (GELU_A * (1.0 + (3.0 * GELU_B) * (u * u)))


def tile_of(width, top=512):
    for tile in (top, 512, 384, 256, 128):
        if width % tile == 0:
            return tile
    return width


def fold_rows(v):
    total = v[0:8]
    for r in range(8, v.shape[0], 8):
        total = total + v[r : r + 8]
    return total


def step_kernel(cfg, *refs):
    n, t, tq, n_model, n_stage = cfg["n"], cfg["t"], cfg["tq"], cfg["n_model"], cfg["n_stage"]
    seq, d_model, heads, hd, ff = cfg["seq"], cfg["d_model"], cfg["heads"], cfg["hd"], cfg["ff"]
    hw = heads * hd
    elem_count = cfg["elem_count"]
    scale = hd**-0.5
    (
        x_hbm, y_hbm, wqkv_hbm, wout_hbm, wup_hbm, wdown_hbm, gain_ref,
        na_hbm, nb_hbm, at_hbm, z_hbm, dqkv_hbm, dmid_hbm, dup_hbm, dout_hbm, small_hbm,
        wqkv, wout, wup, wdown, wqkv_t, wout_t, wup_t, wdown_t, hbuf, nbbuf, doutbuf, dmidbuf, qkvbuf, upbuf, midq, yq, dkacc, dvacc,
        rs_r, rs_s, heads_r, na_st, z_st, at_st, dup_st, dqkv_st, ds_st, pr_st, hsend, dsend, dmidq,
        lossacc, gacc, lossbuf, fin_s, fin_r,
        w_sem, x_sem, y_sem, h_rsem, h_ssem, d_rsem, d_ssem, rs_rsem, rs_ssem, ag_rsem, ag_ssem, wout_sem, heads_sem,
        out_sem, full_sem, loss_sem, fin_rsem, fin_ssem,
    ) = refs
    me = lax.axis_index("model")
    stage = lax.axis_index("stage")
    last = n_stage - 1
    spread = stage >= SPREAD_FROM
    order = [d for d in (2, 1, 3) if d < n_model] if n_model > 2 else list(range(1, n_model))

    odd = lax.rem(me, 2)
    send_order = [2, 3 - 2 * odd, 1 + 2 * odd] if n_model == 4 else order

    far_first = [2, 3 - 2 * odd, 1 + 2 * odd, 0] if n_model == 4 else list(range(n_model))

    def remote(src, dst, ssem, rsem, where):
        return pltpu.make_async_remote_copy(
            src_ref=src, dst_ref=dst, send_sem=ssem, recv_sem=rsem, device_id=where, device_id_type=MESH_ID
        )

    def rows_of(c):
        return pl.ds(pl.multiple_of(c * t, t), t)

    def quarter(c, m):
        return pl.ds(pl.multiple_of(c * t + m * tq, tq), tq)

    own = pl.ds(pl.multiple_of(me * tq, tq), tq)
    own_heads = pl.ds(pl.multiple_of(me * hw, hw), hw)

    slabs = 3 * heads

    def weight_copy(k):
        if k < slabs:
            return pltpu.make_async_copy(wqkv_hbm.at[k], wqkv.at[:, pl.ds(k * hd, hd)], w_sem.at[k])
        src = (wout_hbm, wup_hbm, wdown_hbm)[k - slabs]
        dst = (wout.at[own_heads], wup, wdown)[k - slabs]
        return pltpu.make_async_copy(src, dst, w_sem.at[k])

    def x_copy(k):
        rows = pl.ds(0, t) if k == 0 else pl.ds(t, seq - t)
        return pltpu.make_async_copy(x_hbm.at[rows], hbuf.at[rows], x_sem.at[k])

    def y_copy(c):
        return pltpu.make_async_copy(y_hbm.at[quarter(c, me)], yq.at[pl.ds(c * tq, tq)], y_sem.at[0])

    def y_all():
        return pltpu.make_async_copy(y_hbm.at[pl.ds(0, n * tq)], yq, y_sem.at[0])

    @pl.when(stage == 0)
    def _():
        x_copy(0).start()

    for k in range(slabs + 3):
        weight_copy(k).start()

    @pl.when(stage == 0)
    def _():
        x_copy(1).start()

    @pl.when(stage == last)
    def _():
        for c in range(n):
            y_copy(c).start()

    barrier = pltpu.get_barrier_semaphore()
    up_stage = lax.rem(stage + 1, n_stage)
    down_stage = lax.rem(stage + n_stage - 1, n_stage)
    greet = [{"model": lax.rem(me + d, n_model)} for d in range(1, n_model)]
    greet += [{"stage": up_stage, "model": m} for m in range(n_model)]
    if n_stage > 2:
        greet += [{"stage": down_stage, "model": m} for m in range(n_model)]
    for where in greet:
        pl.semaphore_signal(barrier, inc=1, device_id=where, device_id_type=MESH_ID)

    qkvbuf[:, 2 * hw : 3 * hw] = jnp.zeros((seq, hw), BF16)
    lossacc[...] = jnp.zeros_like(lossacc)
    gacc[...] = jnp.zeros_like(gacc)
    pl.semaphore_wait(barrier, len(greet))

    gains = gain_ref[...].astype(F32)
    gain_a = gains[0:1, :]
    gain_b = gains[1:2, :]

    others = n_model - 1

    def rs_copy(p, c, d, peer):
        slot = lax.rem(c, 2)
        return remote(
            rs_s.at[p, slot, pl.ds(pl.multiple_of(peer * tq, tq), tq)], rs_r.at[p, slot, d - 1],
            rs_ssem.at[p, slot], rs_rsem.at[p, slot], {"model": peer},
        )

    def rs_all(p, c):
        slot = lax.rem(c, 2)
        return remote(rs_r.at[p, slot], rs_r.at[p, slot], rs_ssem.at[p, slot], rs_rsem.at[p, slot], {"model": 0})

    def rs_start(p, c):
        for d in send_order:
            rs_copy(p, c, d, lax.rem(me + d, n_model)).start()

    def rs_drain(p, c):
        rs_all(p, c).wait_send()

    def rs_sum(p, c):
        with jax.named_scope(f"rs_wait{p}"):
            rs_all(p, c).wait_recv()
        total = rs_s[p, lax.rem(c, 2), own, :].astype(F32)
        for d in range(1, n_model):
            total = total + rs_r[p, lax.rem(c, 2), d - 1].astype(F32)
        return total

    def ag_copy(p, buf, c, peer):
        slot = lax.rem(c, 2)
        return remote(
            buf.at[quarter(c, me)], buf.at[quarter(c, me)], ag_ssem.at[p], ag_rsem.at[p, slot], {"model": peer}
        )

    def ag_all(p, buf, c):
        rows = pl.ds(0, others * tq)
        return remote(buf.at[rows], buf.at[rows], ag_ssem.at[p], ag_rsem.at[p, lax.rem(c, 2)], {"model": 0})

    def ag_start(p, buf, c):
        for d in send_order:
            ag_copy(p, buf, c, lax.rem(me + d, n_model)).start()

    def ag_drain(p, buf):
        ag_all(p, buf, 0).wait_send()

    def ag_wait(p, buf, c):
        with jax.named_scope(f"ag_wait{p}"):
            ag_all(p, buf, c).wait_recv()

    def wout_copy(peer):
        return remote(wout.at[own_heads], wout.at[own_heads], wout_sem.at[0], wout_sem.at[1], {"model": peer})

    def wout_all():
        rows = pl.ds(0, others * hw)
        return remote(wout.at[rows], wout.at[rows], wout_sem.at[0], wout_sem.at[1], {"model": 0})

    def heads_copy(c, peer):
        slot = lax.rem(c, 2)
        return remote(
            at_st.at[pl.ds(pl.multiple_of(peer * tq, tq), tq)], heads_r.at[slot, me],
            heads_sem.at[0], heads_sem.at[1 + slot], {"model": peer},
        )

    def heads_all(c):
        slot = lax.rem(c, 2)
        part = heads_r.at[slot, pl.ds(0, others)]
        return remote(part, part, heads_sem.at[0], heads_sem.at[1 + slot], {"model": 0})

    def h_copy(c, m):
        return remote(
            hsend, hbuf.at[quarter(c, me)], h_ssem.at[0], h_rsem.at[c], {"stage": up_stage, "model": m}
        )

    def h_all(c):
        return remote(hbuf.at[rows_of(c)], hbuf.at[rows_of(c)], h_ssem.at[0], h_rsem.at[c], {"model": 0})

    def d_copy(c, m):
        return remote(
            dsend, doutbuf.at[quarter(c, me)], d_ssem.at[0], d_rsem.at[c], {"stage": down_stage, "model": m}
        )

    def d_all(c):
        return remote(doutbuf.at[rows_of(c)], doutbuf.at[rows_of(c)], d_ssem.at[0], d_rsem.at[c], {"model": 0})

    def peer_d_copy(c, peer):
        return remote(
            doutbuf.at[quarter(c, me)], doutbuf.at[quarter(c, me)], d_ssem.at[0], d_rsem.at[c], {"model": peer}
        )

    def peer_d_all(c):
        rows = pl.ds(0, others * tq)
        return remote(doutbuf.at[rows], doutbuf.at[rows], d_ssem.at[0], d_rsem.at[c], {"model": 0})

    def staged_out(k, c):
        src = (na_st, z_st, at_st, dup_st, dqkv_st)[k]
        dst = (na_hbm, z_hbm, at_hbm, dup_hbm, dqkv_hbm)[k]
        return pltpu.make_async_copy(src, dst.at[rows_of(c)], out_sem.at[k])

    def full_out(k, c):
        src = (nbbuf, dmidbuf, doutbuf)[k]
        dst = (nb_hbm, dmid_hbm, dout_hbm)[k]
        return pltpu.make_async_copy(src.at[rows_of(c)], dst.at[rows_of(c)], full_sem.at[k])

    def full_all(k):
        return pltpu.make_async_copy((nbbuf, dmidbuf, doutbuf)[k], (nb_hbm, dmid_hbm, dout_hbm)[k], full_sem.at[k])

    key_step = min(KEY_STEP, seq)
    key_block = max(t, 128)

    def by_prefix(c, body):
        need = lax.div(c * t + t - 1, key_step)
        for k in range(seq // key_step):

            @pl.when(need == k)
            def _():
                body((k + 1) * key_step)

    def scores(c, keys):
        return [
            dot_nt(qkvbuf[rows_of(c), i * hd : (i + 1) * hd], qkvbuf[0:keys, hw + i * hd : hw + (i + 1) * hd])
            for i in range(heads)
        ]

    def causal_softmax(c, keys, raw):
        q_pos = c * t + lax.broadcasted_iota(jnp.int32, (t, keys), 0)
        k_pos = lax.broadcasted_iota(jnp.int32, (t, keys), 1)
        s = jnp.where(k_pos <= q_pos, raw, NEG_BIG / scale)
        e = jnp.exp2((s - jnp.max(s, axis=-1, keepdims=True)) * (scale * LOG2E))
        return e * (1.0 / jnp.sum(e, axis=-1, keepdims=True))

    def fwd_attn(c, first):
        @pl.when(first & (stage == 0))
        def _():
            x_copy(0).wait()

        @pl.when((c == 1) & (stage == 0))
        def _():
            x_copy(1).wait()

        @pl.when(stage > 0)
        def _():
            with jax.named_scope("h_wait"):
                h_all(c).wait_recv()

        @pl.when(first & (stage == 0))
        def _():
            for k in range(slabs + 1):
                weight_copy(k).wait()

        @pl.when(jnp.logical_not(first))
        def _():
            staged_out(0, c).wait()
            staged_out(2, c).wait()

        @pl.when((c >= 2) & jnp.logical_not(spread))
        def _():
            rs_drain(0, c)

        @pl.when((c >= 1) & spread)
        def _():
            heads_all(c).wait_send()

        slot = lax.rem(c, 2)

        h32 = hbuf[rows_of(c), :].astype(F32)
        na_st[...] = (h32 * rms_inverse(h32) * gain_a).astype(BF16)
        staged_out(0, c).start()
        wide = 3 * hw
        tile = tile_of(wide, 384)
        for j in range(wide // tile):
            cols = slice(j * tile, (j + 1) * tile)
            qkvbuf[rows_of(c), cols] = dot_nn(na_st[...], wqkv[:, cols]).astype(BF16)

        def attend(keys):
            probs = [causal_softmax(c, keys, raw).astype(BF16) for raw in scores(c, keys)]
            for i in range(heads):
                v = qkvbuf[0:keys, 2 * hw + i * hd : 2 * hw + (i + 1) * hd]
                at_st[:, i * hd : (i + 1) * hd] = dot_nn(probs[i], v).astype(BF16)

        by_prefix(c, attend)
        staged_out(2, c).start()

        @pl.when(jnp.logical_not(spread))
        def _():
            tile = tile_of(d_model)
            for j in range(d_model // tile):
                cols = slice(j * tile, (j + 1) * tile)
                rs_s[0, lax.rem(c, 2), :, cols] = dot_nn(at_st[...], wout[own_heads, cols]).astype(BF16)
            rs_start(0, c)

        @pl.when(spread)
        def _():
            for d in send_order:
                heads_copy(c, lax.rem(me + d, n_model)).start()
            heads_r[lax.rem(c, 2), me] = at_st[own, :]

    def fwd_mid(c, first):
        @pl.when(jnp.logical_not(first))
        def _():
            ag_drain(0, nbbuf)

        @pl.when(jnp.logical_not(spread))
        def _():
            midq[c] = rs_sum(0, c) + hbuf[quarter(c, me), :].astype(F32)

        @pl.when(first & spread)
        def _():
            wout_all().wait_recv()

        @pl.when(spread)
        def _():
            heads_all(c).wait_recv()
            attn = jnp.concatenate([heads_r[lax.rem(c, 2), m] for m in range(n_model)], axis=-1)
            midq[c] = dot_nn(attn, wout[...]) + hbuf[quarter(c, me), :].astype(F32)

        mid = midq[c]
        nbbuf[quarter(c, me), :] = (mid * rms_inverse(mid) * gain_b).astype(BF16)
        ag_start(0, nbbuf, c)

    def fwd_mlp(c, first):
        @pl.when(first & (stage == 0))
        def _():
            weight_copy(slabs + 1).wait()
            weight_copy(slabs + 2).wait()

        @pl.when(jnp.logical_not(first))
        def _():
            staged_out(1, c).wait()

        @pl.when(c >= 2)
        def _():
            rs_drain(1, c)

        slot = lax.rem(c, 2)

        ag_wait(0, nbbuf, c)
        full_out(0, c).start()
        tile = tile_of(ff)
        for j in range(ff // tile):
            cols = slice(j * tile, (j + 1) * tile)
            u = dot_nn(nbbuf[rows_of(c), :], wup[:, cols])
            upbuf[rows_of(c), cols] = u
            z_st[:, cols] = gelu_tanh(u).astype(BF16)
        staged_out(1, c).start()
        tile = tile_of(d_model)
        for j in range(d_model // tile):
            cols = slice(j * tile, (j + 1) * tile)
            rs_s[1, slot, :, cols] = dot_nn(z_st[...], wdown[:, cols]).astype(BF16)
        rs_start(1, c)

    def fwd_end(c, first):
        h_out = (midq[c] + rs_sum(1, c)).astype(BF16)

        @pl.when(stage < last)
        def _():
            @pl.when(jnp.logical_not(first))
            def _():
                h_all(c).wait_send()

            hsend[...] = h_out
            for d in far_first:
                h_copy(c, lax.rem(me + d, n_model)).start()

        @pl.when(stage == last)
        def _():
            @pl.when(first)
            def _():
                y_all().wait()

            @pl.when(jnp.logical_not(first))
            def _():
                peer_d_all(c).wait_send()

            diff = h_out.astype(F32) - yq[pl.ds(pl.multiple_of(c * tq, tq), tq), :].astype(F32)
            lossacc[...] += fold_rows(diff * diff)
            doutbuf[quarter(c, me), :] = (diff * (1.0 / elem_count)).astype(BF16)
            for d in order:
                peer_d_copy(c, lax.rem(me + d, n_model)).start()

    def pipeline(phases, chunk_of):
        deepest = max(p[1] for p in phases)

        def body(i, carry):
            for phase, lag, name, *cond in phases:
                j = i - lag
                ok = (j >= 0) & (j < n)
                if cond:
                    ok = ok & cond[0]

                @pl.when(ok)
                def _():
                    with jax.named_scope(name):
                        phase(chunk_of(j), j == 0)

            return carry

        lax.fori_loop(0, n + deepest, body, 0)

    def flip_weights():
        for w, w_t in ((wdown, wdown_t), (wup, wup_t), (wout.at[own_heads], wout_t), (wqkv, wqkv_t)):
            depth = tile_of(w.shape[0], 256)
            for r in range(w.shape[0] // depth):
                w_t[:, r * depth : (r + 1) * depth] = w[r * depth : (r + 1) * depth, :].T

    @pl.when(stage > 0)
    def _():
        for k in range(slabs + 3):
            weight_copy(k).wait()

        @pl.when(spread)
        def _():
            for d in send_order:
                wout_copy(lax.rem(me + d, n_model)).start()

        flip_weights()

    pipeline(
        [(fwd_attn, 0, "fwd_attn"), (fwd_end, 2, "fwd_end", (lax.rem(stage, 2) == 0) | (stage >= SPREAD_FROM)), (fwd_mlp, 1, "fwd_mlp"), (fwd_mid, 0, "fwd_mid"), (fwd_end, 1, "fwd_end", jnp.logical_not((lax.rem(stage, 2) == 0) | (stage >= SPREAD_FROM)))],
        lambda j: j,
    )

    @pl.when(stage == 0)
    def _():
        flip_weights()

    dkacc[...] = jnp.zeros_like(dkacc)
    dvacc[...] = jnp.zeros_like(dvacc)

    @pl.when(jnp.logical_not(spread))
    def _():
        for c in range(min(n, 2)):
            rs_drain(0, c)

    @pl.when(spread)
    def _():
        heads_all(0).wait_send()
        wout_all().wait_send()

    for c in range(min(n, 2)):
        rs_drain(1, c)
    ag_drain(0, nbbuf)
    staged_out(0, 0).wait()
    staged_out(1, 0).wait()
    staged_out(2, 0).wait()

    @pl.when(stage < last)
    def _():
        h_all(0).wait_send()

    @pl.when(stage == last)
    def _():
        peer_d_all(0).wait_send()
        total = lossacc[:, 0:128]
        for j in range(1, d_model // 128):
            total = total + lossacc[:, j * 128 : (j + 1) * 128]
        lossbuf[...] = total

    def rms_backward(v, gain, k, d_norm_of):
        inv = rms_inverse(v)
        normed = v * inv
        scaled = gain * inv
        d_norm = d_norm_of()
        gacc[k] += fold_rows(d_norm * normed)
        d_normed = d_norm * gain
        return d_norm * scaled - normed * (inv * jnp.mean(d_normed * normed, axis=-1, keepdims=True))

    def bwd_mlp(c, first):
        @pl.when(stage < last)
        def _():
            with jax.named_scope("d_wait"):
                d_all(c).wait_recv()

        @pl.when(stage == last)
        def _():
            peer_d_all(c).wait_recv()

        full_out(2, c).start()

        @pl.when(jnp.logical_not(first))
        def _():
            staged_out(3, c).wait()

        @pl.when(c < n - 2)
        def _():
            rs_drain(2, c)

        slot = lax.rem(c, 2)

        tile = tile_of(ff)
        for j in range(ff // tile):
            cols = slice(j * tile, (j + 1) * tile)
            d_gelu = dot_nn(doutbuf[rows_of(c), :], wdown_t[:, cols])
            dup_st[:, cols] = (d_gelu * gelu_slope(upbuf[rows_of(c), cols])).astype(BF16)
        staged_out(3, c).start()
        tile = tile_of(d_model)
        for j in range(d_model // tile):
            cols = slice(j * tile, (j + 1) * tile)
            rs_s[2, slot, :, cols] = dot_nn(dup_st[...], wup_t[:, cols]).astype(BF16)
        rs_start(2, c)

    def bwd_mid(c, first):
        @pl.when(jnp.logical_not(first))
        def _():
            ag_drain(1, dmidbuf)

        d_out = doutbuf[quarter(c, me), :].astype(F32)
        d_mid = d_out + rms_backward(midq[c], gain_b, 1, lambda: rs_sum(2, c))
        dmidq[lax.rem(c, 4)] = d_mid
        dmidbuf[quarter(c, me), :] = d_mid.astype(BF16)
        ag_start(1, dmidbuf, c)

    def bwd_attn(c, first):
        ag_wait(1, dmidbuf, c)
        full_out(1, c).start()

        @pl.when(jnp.logical_not(first))
        def _():
            staged_out(4, c).wait()

        @pl.when((c < n - 2) & (stage > 0))
        def _():
            rs_drain(3, c)

        slot = lax.rem(c, 2)

        d_attn = dot_nn(dmidbuf[rows_of(c), :], wout_t[...]).astype(BF16)
        at_st[...] = d_attn

        def attend(keys):
            raws = scores(c, keys)
            d_probs = [
                dot_nt(at_st[:, i * hd : (i + 1) * hd], qkvbuf[0:keys, 2 * hw + i * hd : 2 * hw + (i + 1) * hd])
                for i in range(heads)
            ]
            probs, d_scores = [], []
            for raw, dp in zip(raws, d_probs):
                p = causal_softmax(c, keys, raw)
                probs.append(p.astype(BF16))
                d_scores.append((p * (dp - jnp.sum(p * dp, axis=-1, keepdims=True)) * scale).astype(BF16))
            for i in range(heads):
                cols = slice(i * hd, (i + 1) * hd)
                ds_st[i, :, 0:keys] = d_scores[i]
                pr_st[i, :, 0:keys] = probs[i]
                dqkv_st[:, cols] = dot_nn(d_scores[i], qkvbuf[0:keys, hw + i * hd : hw + (i + 1) * hd]).astype(BF16)

        by_prefix(c, attend)
        near_keys = pl.ds(pl.multiple_of(lax.div(c * t, key_block) * key_block, key_block), key_block)
        for i in range(heads):
            cols = slice(i * hd, (i + 1) * hd)
            dkacc[near_keys, cols] += dot_tn(ds_st[i, :, near_keys], qkvbuf[rows_of(c), cols])
            dvacc[near_keys, cols] += dot_tn(pr_st[i, :, near_keys], at_st[:, cols])
        dqkv_st[:, hw : 2 * hw] = dkacc[rows_of(c), :].astype(BF16)
        dqkv_st[:, 2 * hw : 3 * hw] = dvacc[rows_of(c), :].astype(BF16)
        staged_out(4, c).start()
        tile = tile_of(d_model)

        @pl.when(stage > 0)
        def _():
            for j in range(d_model // tile):
                cols = slice(j * tile, (j + 1) * tile)
                rs_s[3, slot, :, cols] = dot_nn(dqkv_st[...], wqkv_t[:, cols]).astype(BF16)
            rs_start(3, c)

        @pl.when(stage == 0)
        def _():
            h32 = hbuf[rows_of(c), :].astype(F32)
            normed = h32 * rms_inverse(h32)
            for j in range(d_model // tile):
                cols = slice(j * tile, (j + 1) * tile)
                gacc[0, :, cols] += fold_rows(dot_nn(dqkv_st[...], wqkv_t[:, cols]) * normed[:, cols])

        def older(keys):
            for i in range(heads):
                cols = slice(i * hd, (i + 1) * hd)
                ds_st[i, :, near_keys] = jnp.zeros((t, key_block), BF16)
                pr_st[i, :, near_keys] = jnp.zeros((t, key_block), BF16)
            for i in range(heads):
                cols = slice(i * hd, (i + 1) * hd)
                dkacc[0:keys, cols] += dot_tn(ds_st[i, :, 0:keys], qkvbuf[rows_of(c), cols])
                dvacc[0:keys, cols] += dot_tn(pr_st[i, :, 0:keys], at_st[:, cols])

        @pl.when(c * t >= key_block)
        def _():
            by_prefix(c, older)

    def loss_copy():
        return remote(lossbuf, lossbuf, loss_sem.at[0], loss_sem.at[1], {"stage": down_stage})

    def bwd_end(c, first):
        @pl.when(stage > 0)
        def _():
            h32 = hbuf[quarter(c, me), :].astype(F32)
            d_in = dmidq[lax.rem(c, 4)] + rms_backward(h32, gain_a, 0, lambda: rs_sum(3, c))

            @pl.when(jnp.logical_not(first))
            def _():
                d_all(c).wait_send()

            dsend[...] = d_in.astype(BF16)
            for d in far_first:
                d_copy(c, lax.rem(me + d, n_model)).start()

        @pl.when(first)
        def _():
            @pl.when(stage < last)
            def _():
                loss_copy().wait_recv()

            @pl.when(stage > 0)
            def _():
                loss_copy().start()

    pipeline(
        [(bwd_mlp, 0, "bwd_mlp"), (bwd_end, 2, "bwd_end", lax.rem(stage, 2) == 0), (bwd_attn, 1, "bwd_attn"), (bwd_mid, 0, "bwd_mid"), (bwd_end, 1, "bwd_end", lax.rem(stage, 2) == 1)],
        lambda j: n - 1 - j,
    )

    fin_s[...] = jnp.zeros_like(fin_s)
    fin_s[0:1, :] = jnp.sum(gacc[0], axis=0, keepdims=True)
    fin_s[1:2, :] = jnp.sum(gacc[1], axis=0, keepdims=True)
    fin_s[2:3, 0:128] = jnp.sum(lossbuf[...], axis=0, keepdims=True)

    def fin_copy(d, peer):
        return remote(fin_s, fin_r.at[d - 1], fin_ssem.at[0], fin_rsem.at[0], {"model": peer})

    for d in order:
        fin_copy(d, lax.rem(me + d, n_model)).start()

    for c in range(min(n, 2)):
        rs_drain(2, c)
    ag_drain(1, dmidbuf)
    staged_out(3, 0).wait()
    staged_out(4, 0).wait()
    for k in range(3):
        full_all(k).wait()

    @pl.when(stage > 0)
    def _():
        for c in range(min(n, 2)):
            rs_drain(3, c)
        d_all(0).wait_send()
        loss_copy().wait_send()

    fin_all = remote(fin_r, fin_r, fin_ssem.at[0], fin_rsem.at[0], {"model": 0})
    fin_all.wait_recv()
    fin_all.wait_send()
    parts = [jnp.where(me == 0, fin_s[...], 0.0)]
    for m in range(n_model):
        term = jnp.where(me == m, fin_s[...], 0.0)
        for d in range(1, n_model):
            term = term + jnp.where(lax.rem(m + d, n_model) == me, fin_r[d - 1], 0.0)
        parts.append(term)
    total = parts[1]
    for m in range(1, n_model):
        total = total + parts[m + 1]
    fin_s[0:2, :] = total[0:2, :]
    loss = jnp.sum(total[2:3, :], axis=-1, keepdims=True) * (0.5 / elem_count)
    fin_s[2:8, :] = jnp.broadcast_to(loss, (6, d_model))
    small_out = pltpu.make_async_copy(fin_s, small_hbm, out_sem.at[0])
    small_out.start()
    small_out.wait()


def run_step(cfg, x, y, wqkv, wout, wup, wdown, gain):
    n, t, tq, n_model, seq = cfg["n"], cfg["t"], cfg["tq"], cfg["n_model"], cfg["seq"]
    d_model, ff, hw = cfg["d_model"], cfg["ff"], cfg["heads"] * cfg["hd"]
    dma = pltpu.SemaphoreType.DMA
    near = max(n_model - 1, 1)
    act = lambda width: jax.ShapeDtypeStruct((seq, width), BF16)
    any_spec = pl.BlockSpec(memory_space=pl.ANY)
    vmem_spec = pl.BlockSpec(memory_space=pltpu.VMEM)
    scratch = [
        pltpu.VMEM((d_model, 3 * hw), BF16),
        pltpu.VMEM((n_model * hw, d_model), BF16),
        pltpu.VMEM((d_model, ff), BF16),
        pltpu.VMEM((ff, d_model), BF16),
        pltpu.VMEM((3 * hw, d_model), BF16),
        pltpu.VMEM((d_model, hw), BF16),
        pltpu.VMEM((ff, d_model), BF16),
        pltpu.VMEM((d_model, ff), BF16),
        pltpu.VMEM((seq, d_model), BF16),
        pltpu.VMEM((seq, d_model), BF16),
        pltpu.VMEM((seq, d_model), BF16),
        pltpu.VMEM((seq, d_model), BF16),
        pltpu.VMEM((seq, 3 * hw), BF16),
        pltpu.VMEM((seq, ff), F32),
        pltpu.VMEM((n, tq, d_model), F32),
        pltpu.VMEM((n * tq, d_model), BF16),
        pltpu.VMEM((seq, hw), F32),
        pltpu.VMEM((seq, hw), F32),
        pltpu.VMEM((4, 2, near, tq, d_model), BF16),
        pltpu.VMEM((4, 2, t, d_model), BF16),
        pltpu.VMEM((2, n_model, tq, hw), BF16),
        pltpu.VMEM((t, d_model), BF16),
        pltpu.VMEM((t, ff), BF16),
        pltpu.VMEM((t, hw), BF16),
        pltpu.VMEM((t, ff), BF16),
        pltpu.VMEM((t, 3 * hw), BF16),
        pltpu.VMEM((cfg["heads"], t, seq), BF16),
        pltpu.VMEM((cfg["heads"], t, seq), BF16),
        pltpu.VMEM((tq, d_model), BF16),
        pltpu.VMEM((tq, d_model), BF16),
        pltpu.VMEM((4, tq, d_model), F32),
        pltpu.VMEM((8, d_model), F32),
        pltpu.VMEM((2, 8, d_model), F32),
        pltpu.VMEM((8, 128), F32),
        pltpu.VMEM((8, d_model), F32),
        pltpu.VMEM((near, 8, d_model), F32),
        dma((3 * cfg["heads"] + 3,)),
        dma((2,)),
        dma((1,)),
        dma((n,)),
        dma((1,)),
        dma((n,)),
        dma((1,)),
        dma((4, 2)),
        dma((4, 2)),
        dma((2, 2)),
        dma((2,)),
        dma((2,)),
        dma((3,)),
        dma((5,)),
        dma((3,)),
        dma((2,)),
        dma((1,)),
        dma((1,)),
    ]
    return pl.pallas_call(
        functools.partial(step_kernel, cfg),
        name="pipeline_step",
        out_shape=(
            act(d_model), act(d_model), act(hw), act(ff), act(3 * hw), act(d_model), act(ff), act(d_model),
            jax.ShapeDtypeStruct((8, d_model), F32),
        ),
        in_specs=[any_spec] * 6 + [vmem_spec],
        out_specs=[any_spec] * 9,
        scratch_shapes=scratch,
        compiler_params=pltpu.CompilerParams(
            collective_id=0, has_side_effects=True, vmem_limit_bytes=VMEM_BYTES
        ),
    )(x, y, wqkv, wout, wup, wdown, gain)


def grads_kernel(nj, bm, *refs):
    ins, small = refs[: 2 * nj], refs[2 * nj]
    outs, loss_hbm, gain_hbm = refs[2 * nj + 1 : 3 * nj + 1], refs[3 * nj + 1], refs[3 * nj + 2]
    scratch = refs[3 * nj + 3 :]
    bufs, stages = scratch[: 2 * nj], scratch[2 * nj : 3 * nj]
    small_buf, loss_buf, gain_buf, in_sem, out_sem, small_sem = scratch[3 * nj :]

    def load(k):
        return pltpu.make_async_copy(ins[k], bufs[k], in_sem.at[k])

    for k in range(2 * nj):
        load(k).start()
    small_in = pltpu.make_async_copy(small, small_buf, small_sem.at[0])
    small_in.start()
    for j in range(nj):
        load(2 * j).wait()
        load(2 * j + 1).wait()
        a, b, out, stage = bufs[2 * j], bufs[2 * j + 1], outs[j], stages[j]
        rows = a.shape[1]
        step = min(bm, rows)
        blocks = rows // step

        def put(i, slot):
            where = pl.ds(pl.multiple_of(i * step, step), step)
            dst = out.at[:, where] if len(out.shape) == 3 else out.at[where]
            return pltpu.make_async_copy(stage.at[slot], dst, out_sem.at[j, slot])

        def block(i, carry):
            slot = lax.rem(i, 2)

            @pl.when(i >= 2)
            def _():
                put(i, slot).wait()

            acc = dot_tn(a[:, pl.ds(pl.multiple_of(i * step, step), step)], b[...])
            if len(out.shape) == 3:
                lanes = out.shape[2]
                for s in range(out.shape[0]):
                    stage[slot, s] = acc[:, s * lanes : (s + 1) * lanes]
            else:
                stage[slot] = acc
            put(i, slot).start()
            return carry

        lax.fori_loop(0, blocks, block, 0)
    small_in.wait()
    loss_buf[...] = small_buf[2:3, 0:1]
    gain_buf[...] = small_buf[0:2, :]
    loss_out = pltpu.make_async_copy(loss_buf, loss_hbm, small_sem.at[0])
    gain_out = pltpu.make_async_copy(gain_buf, gain_hbm, small_sem.at[1])
    loss_out.start()
    gain_out.start()
    for j in range(nj):
        rows = bufs[2 * j].shape[1]
        step = min(bm, rows)
        for slot in range(min(2, rows // step)):
            out, stage = outs[j], stages[j]
            dst = out.at[:, 0:step] if len(out.shape) == 3 else out.at[0:step]
            pltpu.make_async_copy(stage.at[slot], dst, out_sem.at[j, slot]).wait()
    loss_out.wait()
    gain_out.wait()


def weight_grads(pairs, out_shapes, small, bm):
    nj = len(pairs)
    flat = [x for pair in pairs for x in pair]
    any_spec = pl.BlockSpec(memory_space=pl.ANY)
    stages = []
    for (a, _), out in zip(pairs, out_shapes):
        step = min(bm, a.shape[1])
        stages.append(pltpu.VMEM((2,) + out[:-2] + (step, out[-1]), F32))
    outs = [jax.ShapeDtypeStruct(out, F32) for out in out_shapes]
    outs += [jax.ShapeDtypeStruct((1, 1), F32), jax.ShapeDtypeStruct((2, small.shape[1]), F32)]
    return pl.pallas_call(
        functools.partial(grads_kernel, nj, bm),
        name="weight_grads",
        out_shape=outs,
        in_specs=[any_spec] * (2 * nj + 1),
        out_specs=[any_spec] * (nj + 2),
        scratch_shapes=[pltpu.VMEM(x.shape, x.dtype) for x in flat]
        + stages
        + [pltpu.VMEM(small.shape, F32), pltpu.VMEM((1, 1), F32), pltpu.VMEM((2, small.shape[1]), F32)]
        + [pltpu.SemaphoreType.DMA((2 * nj,)), pltpu.SemaphoreType.DMA((nj, 2)), pltpu.SemaphoreType.DMA((2,))],
        compiler_params=pltpu.CompilerParams(vmem_limit_bytes=VMEM_BYTES),
    )(*flat, small)


def solution(mesh):
    n_stage = mesh.shape["stage"]
    n_model = mesh.shape["model"]

    def device_fn(x_in, y_target, w_qkv, w_out, w_up, w_down, norm_gain):
        n_batch, seq_len, d_model = x_in.shape
        heads, hd, ff = w_qkv.shape[3], w_qkv.shape[4], w_up.shape[2]
        t = min(CHUNK, seq_len)
        cfg = dict(
            n=seq_len // t, t=t, tq=t // n_model, n_model=n_model, n_stage=n_stage, seq=seq_len, d_model=d_model,
            heads=heads, hd=hd, ff=ff, elem_count=n_batch * seq_len * d_model,
        )
        na, nb, at, z, dqkv, dmid, dup, dout, small = run_step(
            cfg, x_in[0], y_target[0], w_qkv[0].transpose(1, 2, 0, 3).reshape(3 * heads, d_model, hd), w_out[0].reshape(heads * hd, d_model),
            w_up[0], w_down[0], norm_gain[0],
        )
        g_out, g_up, g_down, g_qkv, loss, g_gain = weight_grads(
            [(at, dmid), (nb, dup), (z, dout), (na, dqkv)],
            [(heads * hd, d_model), (d_model, ff), (ff, d_model), (3 * heads, d_model, hd)],
            small,
            tile_of(d_model, GRAD_ROWS),
        )
        grad_qkv = g_qkv.reshape(3, heads, d_model, hd).transpose(2, 0, 1, 3)[None]
        return loss.reshape(1), grad_qkv, g_out.reshape(1, heads, hd, d_model), g_up[None], g_down[None], g_gain[None]

    act_spec = P("data", None, None)
    weight_specs = (
        P("stage", None, None, "model", None),
        P("stage", "model", None, None),
        P("stage", None, "model"),
        P("stage", "model", None),
        P("stage", None, None),
    )
    grad_specs = (
        P(("data", "stage"), None, None, "model", None),
        P(("data", "stage"), "model", None, None),
        P(("data", "stage"), None, "model"),
        P(("data", "stage"), "model", None),
        P(("data", "stage"), None, None),
    )
    return jax.shard_map(
        device_fn,
        mesh=mesh,
        in_specs=(act_spec, act_spec) + weight_specs,
        out_specs=(P("data"),) + grad_specs,
        check_vma=False,
    )
```
